32 devices in a mesh: dp: 8 (over z, x), tensor: 4 (over y, core).
Axes of the slice: x: 2, y: 2, z: 4, core: 2. Of those that a mesh axis runs over, the one named last changes fastest.
Arguments:
- residual_in: float32 [16384, 768], P(('dp', 'tensor')), may hold values from -6 to 6
- out_grad: float32 [16384, 768], P(('dp', 'tensor')), may hold values from -6 to 6
- seq_lengths: int32 [8, 16], P('dp'), may hold values from 0 to 1024, as said below
- timesteps: int32 [8, 16], P('dp'), may hold values from 0 to 1023
- norm_gain: float32 [768], replicated, may hold values from 0.5 to 1.5
- norm_bias: float32 [768], replicated, may hold values from -3 to 3
- qkv_weight: float32 [3, 768, 768], P(None, 'dp', 'tensor'), may hold values from -0.21875 to 0.21875
- proj_weight: float32 [768, 768], P('tensor', 'dp'), may hold values from -0.875 to 0.875
- proj_bias: float32 [768], replicated, may hold values from -2 to 2
- up_weight: float32 [768, 3072], P('dp', 'tensor'), may hold values from -0.21875 to 0.21875
- up_bias: float32 [3072], replicated, may hold values from -3 to 3
- down_weight: float32 [3072, 768], P('tensor', 'dp'), may hold values from -0.109375 to 0.109375
- down_bias: float32 [768], replicated, may hold values from -2 to 2
- time_weight: float32 [128, 2304], replicated, may hold values from -0.5 to 0.5
- time_bias: float32 [2304], replicated, may hold values from -3 to 3
Outputs:
- residual_out: float32 [16384, 768], P(('dp', 'tensor'))
- input_grad: float32 [16384, 768], P(('dp', 'tensor'))
- norm_gain_grad: float32 [768], replicated
- norm_bias_grad: float32 [768], replicated
- qkv_weight_grad: float32 [3, 768, 768], P(None, 'dp', 'tensor')
- proj_weight_grad: float32 [768, 768], P('tensor', 'dp')
- proj_bias_grad: float32 [768], replicated
- up_weight_grad: float32 [768, 3072], P('dp', 'tensor')
- up_bias_grad: float32 [3072], replicated
- down_weight_grad: float32 [3072, 768], P('tensor', 'dp')
- down_bias_grad: float32 [768], replicated
- time_weight_grad: float32 [128, 2304], replicated
- time_bias_grad: float32 [2304], replicated
The draws below stay inside these ranges and needn't reach their ends.
Inputs may be any that keep to these rules, and one draw needn't show every extreme that they name: `seq_lengths`: row g lists the lengths of the sequences packed in order into the 2048 rows of pack g: the nonzero lengths come first and lie between 128 and 1024, their sum is at most 2048, the rows after it are padding, and every row holds a length of exactly 1024.
All inputs are finite; a program needn't handle non-finite values.
Results may differ from the reference program's by a relative error of at most 0.015.
Values may be sent and summed in bfloat16 or wider, within the bound.
A program may use at most 128 MiB of HBM per device.

```python
import math
import jax
import jax.numpy as jnp
from jax import lax

D = 768
HEADS = 12
HDIM = 64
FF = 3072
TEMB = 128
MIN_LEN = 128
TSTEPS = 1024
QBLK = 512
TOK_DEV = 2048
MAX_LEN = 1024
SEQS = 16
TOKENS = 16384
N_DP = 8


def draw_seq_lengths(key, part):
    key_pick, key_extra, key_long = jax.random.split(key, 3)
    levels = jnp.array([1, 1, 1, 1, 2, 2, 4, 8], jnp.int32) * MIN_LEN
    picks = jax.random.randint(key_pick, (N_DP, SEQS), 0, 8)
    base_len = levels[picks]
    extra = jax.random.randint(key_extra, (N_DP, SEQS), 0, 8 * MIN_LEN) % base_len
    raw_len = jnp.minimum(base_len + extra, MAX_LEN)
    long_slot = jax.random.randint(key_long, (N_DP, 1), 0, max(1, min(2, TOK_DEV // MAX_LEN - 1)))
    slot_index = jnp.arange(SEQS, dtype=jnp.int32)[None, :]
    raw_len = jnp.where(slot_index == long_slot, MAX_LEN, raw_len)
    seq_ends = jnp.cumsum(raw_len, axis=1)
    return jnp.where(seq_ends <= TOK_DEV, raw_len, 0).astype(jnp.int32)


def with_ends(values, key, smallest, largest):
    shape = values.shape
    index_at = [jax.random.randint(jax.random.fold_in(key, axis), (), 0, shape[axis]) for axis in range(len(shape))]
    values = values.at[tuple(index_at)].set(smallest)
    longest = shape.index(max(shape))
    index_at[longest] = (index_at[longest] + 1) % shape[longest]
    return values.at[tuple(index_at)].set(largest)


def with_spikes(entries, rng, source, target, shards_of, factor):
    owner, partner = [(jnp.arange(entries.shape[dim]) // (entries.shape[dim] // shards_of)).reshape([-1 if axis == dim else 1 for axis in range(entries.ndim)]) for dim in (source, target)]
    chosen = jax.random.permutation(rng, shards_of)[partner]
    strong = (owner == chosen) | (owner == (partner + shards_of // 2) % shards_of)
    return jnp.where(strong, factor * entries, entries)


def block_scale(own_key, shape, pieces, least, high):
    factor_of, own = 1.0, jax.random.fold_in(own_key, 6)
    for dim, parts in pieces:
        heights = jnp.exp(jax.random.uniform(jax.random.fold_in(own, dim), (parts,), jnp.float32, least / len(pieces), high / len(pieces)))
        factor_of = factor_of * jnp.repeat(heights, shape[dim] // parts).reshape([-1 if axis == dim else 1 for axis in range(len(shape))])
    return factor_of


def centred(own_key, extent, scale, most, pieces=(), held_as=jnp.bfloat16):
    drawn = jax.random.normal(own_key, extent, jnp.float32) * scale
    if len(pieces) > 0:
        drawn = block_scale(own_key, extent, pieces, -0.22, 0.18) * drawn
    return jnp.clip(drawn, min=-most, max=most).astype(held_as)


def bell_draw_with(stream_key, shape, deviation, bound, shards, heavy, kind=jnp.bfloat16):
    values = deviation * jax.random.normal(stream_key, shape, jnp.float32)
    if shards:
        values = values * block_scale(stream_key, shape, shards, -0.22, 0.18)
    return jnp.clip(with_spikes(values, jax.random.fold_in(stream_key, 3), *heavy), -bound, bound).astype(kind)


def setup_inputs(seed: int = 0) -> dict:
    arg_keys = jax.random.split(jax.random.key(seed), 16)
    residual_in = centred(arg_keys[0], (TOKENS, D), 1.0, 6.0, ((0, 32),), jnp.float32)
    out_grad = bell_draw_with(arg_keys[1], (TOKENS, D), 1.0, 6.0, ((0, 32),), (0, 1, 32, 2.75), jnp.float32)
    seq_lengths = draw_seq_lengths(jax.random.fold_in(arg_keys[15], 71), 0)
    timesteps = with_ends(jax.random.randint(arg_keys[3], (N_DP, SEQS), 0, TSTEPS), jax.random.fold_in(arg_keys[3], 1), 0, TSTEPS - 1).astype(jnp.int32)
    norm_gain = jnp.clip(1.0 + 0.1 * jax.random.normal(arg_keys[4], (D,), jnp.float32), 0.5, 1.5)
    norm_bias = centred(arg_keys[5], (D,), 0.5, 3.0, (), jnp.float32)
    qkv_weight = centred(arg_keys[6], (3, D, D), D ** -0.5, 0.21875, ((1, 8), (2, 4)), jnp.float32)
    proj_weight = centred(arg_keys[7], (D, D), (D // 16) ** -0.5, 0.875, ((0, 4), (1, 8)), jnp.float32)
    proj_bias = centred(arg_keys[8], (D,), 0.3, 2.0, (), jnp.float32)
    up_weight = centred(arg_keys[9], (D, FF), D ** -0.5, 0.21875, ((0, 8), (1, 4)), jnp.float32)
    up_bias = centred(arg_keys[10], (FF,), 0.5, 3.0, (), jnp.float32)
    down_weight = centred(arg_keys[11], (FF, D), FF ** -0.5, 0.109375, ((0, 4), (1, 8)), jnp.float32)
    down_bias = centred(arg_keys[12], (D,), 0.3, 2.0, (), jnp.float32)
    time_weight = centred(arg_keys[13], (TEMB, 3 * D), TEMB ** -0.5, 0.5, (), jnp.float32)
    time_bias = centred(arg_keys[14], (3 * D,), 0.5, 3.0, (), jnp.float32)
    return {"residual_in": residual_in, "out_grad": out_grad, "seq_lengths": seq_lengths, "timesteps": timesteps, "norm_gain": norm_gain, "norm_bias": norm_bias, "qkv_weight": qkv_weight, "proj_weight": proj_weight, "proj_bias": proj_bias, "up_weight": up_weight, "up_bias": up_bias, "down_weight": down_weight, "down_bias": down_bias, "time_weight": time_weight, "time_bias": time_bias}


@jax.custom_vjp
def low(v):
    return lax.optimization_barrier(v.astype(jnp.bfloat16)).astype(jnp.float32)

@jax.custom_vjp
def low_back(v):
    return v

def low_keep(v):
    return (low(v), None)

def low_pass(kept, grad):
    return (grad,)

def back_keep(v):
    return (v, None)

def back_low(kept, grad):
    return (low(grad),)
low.defvjp(low_keep, low_pass)
low_back.defvjp(back_keep, back_low)
highest = lax.Precision.HIGHEST

def layer_norm(values):
    center = values - lax.optimization_barrier(jnp.mean(values, axis=-1, keepdims=True))
    spread = lax.optimization_barrier(jnp.mean(center * center, axis=-1, keepdims=True))
    return center * lax.rsqrt(spread + 1e-05)

def pack_info(lengths, row_total):
    row_index = jnp.arange(row_total, dtype=jnp.int32)
    seq_ends = jnp.cumsum(lengths).astype(jnp.int32)
    passed = row_index[:, None] >= seq_ends[None, :]
    segment = lax.optimization_barrier(jnp.sum(passed.astype(jnp.int32), axis=1)).astype(jnp.int32)
    starts = lax.optimization_barrier(jnp.sum(jnp.where(passed, lengths[None, :], 0), axis=1)).astype(jnp.int32)
    return (segment, (row_index - starts).astype(jnp.int32))

def time_embed(time_index, embed_width):
    half_width = embed_width // 2
    freqs = jnp.exp(-math.log(10000.0) * jnp.arange(half_width, dtype=jnp.float32) / half_width)
    angles = time_index.astype(jnp.float32)[:, None] * freqs[None, :]
    return jnp.concatenate([jnp.cos(angles), jnp.sin(angles)], axis=1)

def rope_tables(positions, head_width):
    half_width = head_width // 2
    inverse = jnp.exp(-math.log(10000.0) * jnp.arange(half_width, dtype=jnp.float32) * (2.0 / head_width))
    angles = positions.astype(jnp.float32)[:, None] * inverse[None, :]
    return (jnp.cos(angles)[:, None, :], jnp.sin(angles)[:, None, :])

def rotate(values, cosine, sine_table):
    half_width = values.shape[-1] // 2
    lead_half = values[..., :half_width]
    tail_half = values[..., half_width:]
    return jnp.concatenate([lead_half * cosine - tail_half * sine_table, tail_half * cosine + lead_half * sine_table], axis=-1)

def layer_forward(segment, positions, embedded, x_pack, norm_gain, norm_bias, qkv_weight, proj_weight, proj_bias, up_weight, up_bias, down_weight, down_bias, time_weight, time_bias):
    row_total = x_pack.shape[0]
    normed = low(layer_norm(x_pack) * norm_gain + norm_bias)
    projected = jnp.einsum('td,cde->cte', normed, low(qkv_weight), precision=highest)
    cosine, sine_table = rope_tables(positions, HDIM)
    query_raw = low_back(projected[0]).reshape(row_total, HEADS, HDIM)
    key_raw = low_back(projected[1]).reshape(row_total, HEADS, HDIM)
    queries = low(rotate(query_raw, cosine, sine_table) * (1.0 / math.sqrt(HDIM)))
    keys_low = low(rotate(key_raw, cosine, sine_table))
    values_low = low(low_back(projected[2].reshape(row_total, HEADS, HDIM)))
    block_count = row_total // QBLK

    def attend(block_item):
        query_block, segment_block = block_item
        scores = low_back(jnp.einsum('qhd,khd->hqk', query_block, keys_low, precision=highest))
        allowed = segment_block[:, None] == segment[None, :]
        scores = jnp.where(allowed[None], scores, -1000000000.0)
        soft_weights = jax.nn.softmax(scores, axis=-1)
        return jnp.einsum('hqk,khd->qhd', low(soft_weights), values_low, precision=highest)
    mixed = lax.map(jax.checkpoint(attend), (queries.reshape(block_count, QBLK, HEADS, HDIM), segment.reshape(block_count, QBLK)))
    attn_out = low_back(low(mixed.reshape(row_total, D)))
    hidden = x_pack + low_back(jnp.dot(attn_out, low(proj_weight), precision=highest)) + proj_bias
    onehot = (segment[:, None] == jnp.arange(SEQS, dtype=jnp.int32)[None, :]).astype(jnp.float32)
    mod_table = jnp.dot(embedded, time_weight, precision=highest) + time_bias
    modulation = jnp.dot(onehot, mod_table, precision=highest)
    mod_scale = modulation[:, :D]
    mod_shift = modulation[:, D:2 * D]
    mod_gate = modulation[:, 2 * D:]
    modulated = low(layer_norm(hidden) * (1.0 + mod_scale) + mod_shift)
    pre_act = low_back(jnp.dot(modulated, low(up_weight), precision=highest) + up_bias)
    active = low(jax.nn.gelu(pre_act, approximate=True))
    branch = low_back(jnp.dot(active, low(down_weight), precision=highest)) + down_bias
    return hidden + mod_gate * branch

def reference(residual_in, out_grad, seq_lengths, timesteps, norm_gain, norm_bias, qkv_weight, proj_weight, proj_bias, up_weight, up_bias, down_weight, down_bias, time_weight, time_bias):
    params = (norm_gain, norm_bias, qkv_weight, proj_weight, proj_bias, up_weight, up_bias, down_weight, down_bias, time_weight, time_bias)
    x_packs = residual_in.reshape(N_DP, TOK_DEV, D)
    grad_packs = out_grad.reshape(N_DP, TOK_DEV, D)

    def one_pack(totals, pack_item):
        x_pack, grad_pack, lengths, time_index = pack_item
        segment, positions = pack_info(lengths, TOK_DEV)
        embedded = time_embed(time_index, TEMB)

        def apply_layer(x_value, *weights):
            return layer_forward(segment, positions, embedded, x_value, *weights)
        out_pack, pullback = jax.vjp(apply_layer, x_pack, *params)
        grads = pullback(grad_pack)
        totals = tuple((running + update for running, update in zip(totals, grads[1:])))
        return (totals, (out_pack, grads[0]))
    starting = tuple((jnp.zeros(weight.shape, jnp.float32) for weight in params))
    totals, stacked = lax.scan(one_pack, starting, (x_packs, grad_packs, seq_lengths, timesteps))
    outputs = stacked[0].reshape(TOKENS, D)
    in_grads = stacked[1].reshape(TOKENS, D)
    return (outputs, in_grads, totals[0], totals[1], totals[2], totals[3], totals[4], totals[5], totals[6], totals[7], totals[8], totals[9], totals[10])
```

```python
import functools
import math

import jax
import jax.numpy as jnp
from jax import lax
from jax.experimental import pallas as pl
from jax.experimental.pallas import tpu as pltpu
from jax.sharding import PartitionSpec as P

HDIM = 64
HALF = HDIM // 2
BQ = 256
BK = 256
NEG = -1000000000.0
MESH = pl.DeviceIdType.MESH
BF = jnp.bfloat16
F32 = jnp.float32
VMEM_LIMIT = 60 * 1024 * 1024


highest = lax.Precision.HIGHEST


def dot(a, b, ca, cb, out=F32):
    return lax.dot_general(a, b, (((ca,), (cb,)), ((), ())), preferred_element_type=out)


def normalize(values):
    center = values - jnp.mean(values, axis=-1, keepdims=True)
    inverse = lax.rsqrt(jnp.mean(center * center, axis=-1, keepdims=True) + 1e-05)
    return (center * inverse, inverse)


def norm_back(grad_in, normed, inverse):
    return inverse * (
        grad_in
        - jnp.mean(grad_in, axis=-1, keepdims=True)
        - normed * jnp.mean(grad_in * normed, axis=-1, keepdims=True)
    )


def pack_info(lengths, row_total):
    row_index = jnp.arange(row_total, dtype=jnp.int32)
    seq_ends = jnp.cumsum(lengths)
    passed = row_index[:, None] >= seq_ends[None, :]
    segment = jnp.sum(passed.astype(jnp.int32), axis=1)
    starts = jnp.sum(jnp.where(passed, lengths[None, :], 0), axis=1)
    return (segment, row_index - starts)


def key_ranges(lengths, row_total):
    seq_ends = jnp.cumsum(lengths)
    first = jnp.arange(row_total // BQ, dtype=jnp.int32) * BQ
    last = first + (BQ - 1)
    start = jnp.sum(jnp.where(first[:, None] >= seq_ends[None, :], lengths[None, :], 0), axis=1)
    end = jnp.min(jnp.where(seq_ends[None, :] > last[:, None], seq_ends[None, :], row_total), axis=1)
    return (start // BK).astype(jnp.int32), ((end + BK - 1) // BK).astype(jnp.int32)


def time_embed(time_index, embed_width):
    half_width = embed_width // 2
    freqs = jnp.exp(-math.log(10000.0) * jnp.arange(half_width, dtype=jnp.float32) / half_width)
    angles = time_index.astype(jnp.float32)[:, None] * freqs[None, :]
    return jnp.concatenate([jnp.cos(angles), jnp.sin(angles)], axis=1)


def rope_tables(positions):
    inverse = jnp.exp(-math.log(10000.0) * jnp.arange(HALF, dtype=jnp.float32) * (2.0 / HDIM))
    angles = inverse[:, None] * positions.astype(jnp.float32)[None, :]
    return (jnp.cos(angles), jnp.sin(angles))


def project_kernel(heads, n_ref, w_ref, cos_ref, sin_ref, q_ref, k_ref, v_ref):
    width = heads * HDIM
    raw = dot(w_ref[...], n_ref[...], 1, 1)
    cos = cos_ref[...]
    sin = sin_ref[...]
    for part, out_ref, factor in ((0, q_ref, 1.0 / math.sqrt(HDIM)), (1, k_ref, 1.0)):
        for h in range(heads):
            base = part * width + h * HDIM
            a = raw[base : base + HALF]
            b = raw[base + HALF : base + HDIM]
            out_ref[h * HDIM : h * HDIM + HALF] = ((a * cos - b * sin) * factor).astype(BF)
            out_ref[h * HDIM + HALF : (h + 1) * HDIM] = ((b * cos + a * sin) * factor).astype(BF)
    v_ref[...] = raw[2 * width :].astype(BF)


def project(normed, weight_t, cos, sin, heads):
    rows, width_model = normed.shape
    width = heads * HDIM
    tile = 512
    out = jax.ShapeDtypeStruct((width, rows), BF)
    spec = pl.BlockSpec((width, tile), lambda i: (0, i))
    return pl.pallas_call(
        functools.partial(project_kernel, heads),
        name="project_qkv",
        grid=(rows // tile,),
        in_specs=[
            pl.BlockSpec((tile, width_model), lambda i: (i, 0)),
            pl.BlockSpec((3 * width, width_model), lambda i: (0, 0)),
            pl.BlockSpec((HALF, tile), lambda i: (0, i)),
            pl.BlockSpec((HALF, tile), lambda i: (0, i)),
        ],
        out_specs=[spec, spec, spec],
        out_shape=[out, out, out],
        cost_estimate=pl.CostEstimate(
            flops=2 * rows * width_model * 3 * width, bytes_accessed=8 << 20, transcendentals=0
        ),
    )(normed, weight_t, cos, sin)


def wide(column, lanes):
    return jnp.concatenate([column] * (lanes // 128), axis=1)


def attend_kernel(
    heads, lo_ref, hi_ref, q_ref, k_ref, v_ref, srow_ref, scol_ref, o_ref, lse_ref, kt_ref, sc_ref
):
    i = pl.program_id(0)

    @pl.when(i == 0)
    def _():
        for h in range(heads):
            kt_ref[h] = k_ref[h * HDIM : (h + 1) * HDIM, :].T
        sc_ref[...] = jnp.broadcast_to(scol_ref[...], sc_ref.shape)

    srow = srow_ref[...]

    def step(j, carry):
        base = pl.multiple_of(j * BK, BK)
        allowed = wide(sc_ref[pl.ds(base, BK), :], BQ) == srow
        out = []
        for h in range(heads):
            m, l, acc = carry[h]
            s = dot(kt_ref[h, pl.ds(base, BK), :], q_ref[h * HDIM : (h + 1) * HDIM, :], 1, 0)
            s = jnp.where(allowed, s, NEG)
            m_new = jnp.maximum(m, jnp.max(s, axis=0, keepdims=True))
            fade = jnp.exp(m - m_new)
            p = jnp.exp(s - m_new)
            l = fade * l + jnp.sum(p, axis=0, keepdims=True)
            acc = fade * acc + dot(
                v_ref[h * HDIM : (h + 1) * HDIM, pl.ds(base, BK)], p.astype(BF), 1, 0
            )
            out.append((m_new, l, acc))
        return tuple(out)

    empty = (
        jnp.full((1, BQ), -3.0e38, F32),
        jnp.zeros((1, BQ), F32),
        jnp.zeros((HDIM, BQ), F32),
    )
    done = lax.fori_loop(lo_ref[i], hi_ref[i], step, (empty,) * heads)
    for h in range(heads):
        m, l, acc = done[h]
        o_ref[h * HDIM : (h + 1) * HDIM, :] = (acc / l).astype(BF)
        lse_ref[h : h + 1, :] = m + jnp.log(l)


def attend(q, k, v, seg_row, seg_col, lo, hi):
    width, rows = q.shape
    heads = width // HDIM
    whole = lambda i, *_: (0, 0)
    block = lambda i, *_: (0, i)
    return pl.pallas_call(
        functools.partial(attend_kernel, heads),
        name="attend",
        grid_spec=pltpu.PrefetchScalarGridSpec(
            num_scalar_prefetch=2,
            grid=(rows // BQ,),
            in_specs=[
                pl.BlockSpec((width, BQ), block),
                pl.BlockSpec((width, rows), whole),
                pl.BlockSpec((width, rows), whole),
                pl.BlockSpec((1, BQ), block),
                pl.BlockSpec((rows, 1), whole),
            ],
            out_specs=[
                pl.BlockSpec((width, BQ), block),
                pl.BlockSpec((heads, BQ), block),
            ],
            scratch_shapes=[
                pltpu.VMEM((heads, rows, HDIM), BF),
                pltpu.VMEM((rows, 128), jnp.int32),
            ],
        ),
        out_shape=[
            jax.ShapeDtypeStruct((width, rows), BF),
            jax.ShapeDtypeStruct((heads, rows), F32),
        ],
        compiler_params=pltpu.CompilerParams(vmem_limit_bytes=VMEM_LIMIT),
        cost_estimate=pl.CostEstimate(
            flops=rows * rows * heads * HDIM * 8, bytes_accessed=8 << 20, transcendentals=rows * rows
        ),
    )(lo, hi, q, k, v, seg_row, seg_col)


def attend_back_kernel(
    heads,
    lo_ref,
    hi_ref,
    q_ref,
    k_ref,
    v_ref,
    do_ref,
    o_ref,
    lse_ref,
    srow_ref,
    scol_ref,
    cos_ref,
    sin_ref,
    g_ref,
    kt_ref,
    vt_ref,
    sc_ref,
    dk_ref,
    dv_ref,
):
    i = pl.program_id(0)
    width = heads * HDIM

    @pl.when(i == 0)
    def _():
        for h in range(heads):
            kt_ref[h] = k_ref[h * HDIM : (h + 1) * HDIM, :].T
            vt_ref[h] = v_ref[h * HDIM : (h + 1) * HDIM, :].T
        sc_ref[...] = jnp.broadcast_to(scol_ref[...], sc_ref.shape)
        dk_ref[...] = jnp.zeros_like(dk_ref)
        dv_ref[...] = jnp.zeros_like(dv_ref)

    srow = srow_ref[...]
    inner = []
    for h in range(heads):
        part = slice(h * HDIM, (h + 1) * HDIM)
        inner.append(
            jnp.sum(do_ref[part, :].astype(F32) * o_ref[part, :].astype(F32), axis=0, keepdims=True)
        )

    def step(j, carry):
        base = pl.multiple_of(j * BK, BK)
        keys = pl.ds(base, BK)
        allowed = wide(sc_ref[keys, :], BQ) == srow
        out = []
        for h in range(heads):
            part = slice(h * HDIM, (h + 1) * HDIM)
            q = q_ref[part, :]
            grad = do_ref[part, :]
            s = dot(kt_ref[h, keys, :], q, 1, 0)
            s = jnp.where(allowed, s, NEG)
            p = jnp.exp(s - lse_ref[h : h + 1, :])
            dp = dot(vt_ref[h, keys, :], grad, 1, 0)
            ds = (p * (dp - inner[h])).astype(BF)
            out.append(carry[h] + dot(k_ref[part, keys], ds, 1, 0))
            dk_ref[part, keys] += dot(q, ds, 1, 1)
            dv_ref[part, keys] += dot(grad, p.astype(BF), 1, 1)
        return tuple(out)

    done = lax.fori_loop(
        lo_ref[i], hi_ref[i], step, (jnp.zeros((HDIM, BQ), F32),) * heads
    )
    here = pl.ds(pl.multiple_of(i * BQ, BQ), BQ)
    cos = cos_ref[:, here]
    sin = sin_ref[:, here]
    factor = 1.0 / math.sqrt(HDIM)
    for h in range(heads):
        a = done[h][:HALF] * factor
        b = done[h][HALF:] * factor
        g_ref[h * HDIM : h * HDIM + HALF, here] = (a * cos + b * sin).astype(BF)
        g_ref[h * HDIM + HALF : (h + 1) * HDIM, here] = (b * cos - a * sin).astype(BF)

    @pl.when(i == pl.num_programs(0) - 1)
    def _():
        cos_all = cos_ref[...]
        sin_all = sin_ref[...]
        for h in range(heads):
            a = dk_ref[h * HDIM : h * HDIM + HALF, :]
            b = dk_ref[h * HDIM + HALF : (h + 1) * HDIM, :]
            base = width + h * HDIM
            g_ref[base : base + HALF, :] = (a * cos_all + b * sin_all).astype(BF)
            g_ref[base + HALF : base + HDIM, :] = (b * cos_all - a * sin_all).astype(BF)
        g_ref[2 * width :, :] = dv_ref[...].astype(BF)


def attend_back(q, k, v, do, o, lse, seg_row, seg_col, cos, sin, lo, hi):
    width, rows = q.shape
    heads = width // HDIM
    whole = lambda i, *_: (0, 0)
    block = lambda i, *_: (0, i)
    return pl.pallas_call(
        functools.partial(attend_back_kernel, heads),
        name="attend_back",
        grid_spec=pltpu.PrefetchScalarGridSpec(
            num_scalar_prefetch=2,
            grid=(rows // BQ,),
            in_specs=[
                pl.BlockSpec((width, BQ), block),
                pl.BlockSpec((width, rows), whole),
                pl.BlockSpec((width, rows), whole),
                pl.BlockSpec((width, BQ), block),
                pl.BlockSpec((width, BQ), block),
                pl.BlockSpec((heads, BQ), block),
                pl.BlockSpec((1, BQ), block),
                pl.BlockSpec((rows, 1), whole),
                pl.BlockSpec((HALF, rows), whole),
                pl.BlockSpec((HALF, rows), whole),
            ],
            out_specs=pl.BlockSpec((3 * width, rows), whole),
            scratch_shapes=[
                pltpu.VMEM((heads, rows, HDIM), BF),
                pltpu.VMEM((heads, rows, HDIM), BF),
                pltpu.VMEM((rows, 128), jnp.int32),
                pltpu.VMEM((width, rows), F32),
                pltpu.VMEM((width, rows), F32),
            ],
        ),
        out_shape=jax.ShapeDtypeStruct((3 * width, rows), BF),
        compiler_params=pltpu.CompilerParams(vmem_limit_bytes=VMEM_LIMIT),
        cost_estimate=pl.CostEstimate(
            flops=rows * rows * heads * HDIM * 20, bytes_accessed=8 << 20, transcendentals=rows * rows
        ),
    )(lo, hi, q, k, v, do, o, lse, seg_row, seg_col, cos, sin)


def place_kernel(count, order_ref, *refs):
    out_ref = refs[count]
    for n in range(count):
        out_ref[order_ref[n]] = refs[n][...]


def place(pieces, order):
    count = len(pieces)
    rows, columns = pieces[0].shape
    return pl.pallas_call(
        functools.partial(place_kernel, count),
        name="place",
        grid_spec=pltpu.PrefetchScalarGridSpec(
            num_scalar_prefetch=1,
            grid=(1,),
            in_specs=[pl.BlockSpec((rows, columns), lambda i, *_: (0, 0))] * count,
            out_specs=pl.BlockSpec((count, rows, columns), lambda i, *_: (0, 0, 0)),
        ),
        out_shape=jax.ShapeDtypeStruct((count, rows, columns), pieces[0].dtype),
        cost_estimate=pl.CostEstimate(
            flops=0, bytes_accessed=4 * count * rows * columns, transcendentals=0
        ),
    )(order, *pieces).reshape(count * rows, columns)


def opening_kernel(n_z, n_ref, w_ref, n_out, w_out, local_sem, send_sem, recv_sem):
    dp = lax.axis_index("dp")
    t = lax.axis_index("tensor")
    z, x = dp // 2, dp % 2
    y, c = t // 2, t % 2
    rows = n_ref.shape[0]
    core_peer = {"tensor": 2 * y + (1 - c)}
    y_rank = 2 * (1 - y) + c
    y_peer = {"tensor": y_rank}
    x_peer = {"dp": 2 * z + (1 - x)}
    z_peers = [{"dp": 2 * ((z + s) % n_z) + x} for s in range(1, n_z)]

    barrier = pltpu.get_barrier_semaphore()
    for peer in [core_peer, y_peer, x_peer] + z_peers:
        pl.semaphore_signal(barrier, inc=1, device_id=peer, device_id_type=MESH)
    pl.semaphore_wait(barrier, 3 + len(z_peers))

    def n_at(rank):
        return n_out.at[pl.ds(pl.multiple_of(rank * rows, rows), rows)]

    def w_at(rank):
        return w_out.at[rank]

    def send(src, dst, peer, slot):
        copy = pltpu.make_async_remote_copy(
            src_ref=src,
            dst_ref=dst,
            send_sem=send_sem.at[slot],
            recv_sem=recv_sem.at[slot],
            device_id=peer,
            device_id_type=MESH,
        )
        copy.start()
        return copy

    n_y = send(n_ref, n_at(t), y_peer, 0)
    z_copies = [send(w_ref, w_at(dp), peer, 3 + s) for s, peer in enumerate(z_peers)]
    base = 3 + len(z_peers)
    x_copies = [send(w_ref, w_at(dp), x_peer, base)]
    n_core = send(n_ref, n_at(t), core_peer, 1)
    own_n = pltpu.make_async_copy(n_ref, n_at(t), local_sem.at[0])
    own_w = pltpu.make_async_copy(w_ref, w_at(dp), local_sem.at[1])
    own_n.start()
    own_w.start()
    for s, copy in enumerate(z_copies):
        copy.wait_recv()
        rank = 2 * ((z + n_z - 1 - s) % n_z) + x
        x_copies.append(send(w_at(rank), w_at(rank), x_peer, base + 1 + s))
    n_y.wait_recv()
    n_relay = send(n_at(y_rank), n_at(y_rank), core_peer, 2)
    n_core.wait_recv()
    n_relay.wait_recv()
    for copy in x_copies:
        copy.wait_recv()
    for copy in [n_y, n_core, n_relay] + z_copies + x_copies:
        copy.wait_send()
    own_n.wait()
    own_w.wait()


def opening(normed, weight, n_dp, n_tensor):
    rows, width = normed.shape
    depth, columns = weight.shape
    n_z = n_dp // 2
    slots = 3 + (n_z - 1) + n_z
    return pl.pallas_call(
        functools.partial(opening_kernel, n_z),
        name="opening",
        in_specs=[pl.BlockSpec(memory_space=pltpu.VMEM)] * 2,
        out_specs=[pl.BlockSpec(memory_space=pl.ANY)] * 2,
        out_shape=[
            jax.ShapeDtypeStruct((n_tensor * rows, width), BF),
            jax.ShapeDtypeStruct((n_dp, depth, columns), BF),
        ],
        scratch_shapes=[
            pltpu.SemaphoreType.DMA((2,)),
            pltpu.SemaphoreType.DMA((slots,)),
            pltpu.SemaphoreType.DMA((slots,)),
        ],
        compiler_params=pltpu.CompilerParams(collective_id=0, has_side_effects=True),
        cost_estimate=pl.CostEstimate(flops=0, bytes_accessed=64 << 20, transcendentals=0),
    )(normed, weight)


def to_tensor_peer(value, distance):
    size = lax.axis_size("tensor")
    return lax.ppermute(value, "tensor", [(r, r ^ distance) for r in range(size)])


def z_step(value, step):
    size = lax.axis_size("dp")
    n_z = size // 2
    pairs = [(r, 2 * ((r // 2 + step) % n_z) + r % 2) for r in range(size)]
    return lax.ppermute(value, "dp", pairs)


def x_swap(value):
    size = lax.axis_size("dp")
    return lax.ppermute(value, "dp", [(r, r ^ 1) for r in range(size)])


def gather_pieces(value):
    n_z = lax.axis_size("dp") // 2
    near = [value] + [z_step(value, s) for s in range(1, n_z)]
    return near + [x_swap(piece) for piece in near]


def piece_order():
    n_z = lax.axis_size("dp") // 2
    rank = lax.axis_index("dp")
    steps = (rank // 2 - jnp.arange(n_z, dtype=jnp.int32)) % n_z
    return jnp.concatenate([2 * steps + rank % 2, 2 * steps + 1 - rank % 2]).astype(jnp.int32)


def gather_rows(value, order):
    return place(gather_pieces(value), order)


def scatter_sum(total):
    size = lax.axis_size("dp")
    n_z = size // 2
    rank = lax.axis_index("dp")
    z, x = rank // 2, rank % 2
    blocks = total.reshape(n_z, 2, total.shape[0] // size, total.shape[1])
    away = lax.dynamic_index_in_dim(blocks, 1 - x, 1, keepdims=False).astype(BF)
    kept = lax.dynamic_index_in_dim(blocks, x, 1, keepdims=False).astype(F32)
    summed = (kept + x_swap(away).astype(F32)).astype(BF)
    result = lax.dynamic_index_in_dim(summed, z, 0, keepdims=False).astype(F32)
    for s in range(1, n_z):
        block = lax.dynamic_index_in_dim(summed, (z + s) % n_z, 0, keepdims=False)
        result = result + z_step(block, s).astype(F32)
    return result


def tensor_sum_scatter(parts):
    near = parts[0].astype(F32) + to_tensor_peer(parts[1], 1).astype(F32)
    far = (parts[2].astype(F32) + to_tensor_peer(parts[3], 1).astype(F32)).astype(BF)
    return near + to_tensor_peer(far, 2).astype(F32)


def gather_tensor(value):
    far = to_tensor_peer(value, 2)
    return [value, to_tensor_peer(value, 1), far, to_tensor_peer(far, 1)]


def butterfly(value, axis):
    size = lax.axis_size(axis)
    distance = 1
    while distance < size:
        value = value + lax.ppermute(value, axis, [(r, r ^ distance) for r in range(size)])
        distance *= 2
    return value


def gelu_tanh(values):
    return jax.nn.gelu(values, approximate=True)


def shards(
    residual_in,
    out_grad,
    seq_lengths,
    timesteps,
    norm_gain,
    norm_bias,
    qkv_weight,
    proj_weight,
    proj_bias,
    up_weight,
    up_bias,
    down_weight,
    down_bias,
    time_weight,
    time_bias,
):
    row_count, width_model = residual_in.shape
    n_dp = lax.axis_size("dp")
    n_tensor = lax.axis_size("tensor")
    tensor_rank = lax.axis_index("tensor")
    total_rows = row_count * n_tensor
    slot_count = seq_lengths.shape[1]
    head_width = qkv_weight.shape[2]
    heads = head_width // HDIM
    units = up_weight.shape[1]
    order = piece_order()
    ranks = [tensor_rank ^ d for d in range(n_tensor)]

    normed_in, inverse_in = normalize(residual_in)
    normed_low = (normed_in * norm_gain + norm_bias).astype(BF)
    qkv_shard = jnp.transpose(qkv_weight, (1, 0, 2)).reshape(qkv_weight.shape[1], -1).astype(BF)
    normed_full, qkv_full = opening(normed_low, qkv_shard, n_dp, n_tensor)
    qkv_full = qkv_full.reshape(width_model, -1)

    up_own = gather_rows(up_weight.astype(BF), order)
    down_own = gather_rows(down_weight.T.astype(BF), order)
    proj_own = gather_rows(proj_weight.T.astype(BF), order)
    up_all = gather_tensor(up_own)
    down_all = gather_tensor(down_own)
    proj_all = gather_tensor(proj_own)

    segment, positions = pack_info(seq_lengths[0], total_rows)
    lo, hi = key_ranges(seq_lengths[0], total_rows)
    own_segment = lax.dynamic_slice_in_dim(segment, tensor_rank * row_count, row_count)
    onehot = (own_segment[:, None] == jnp.arange(slot_count, dtype=jnp.int32)[None, :]).astype(F32)
    embedded = time_embed(timesteps[0], time_weight.shape[0])
    mod_table = jnp.dot(embedded, time_weight, precision=highest) + time_bias
    modulation = jnp.dot(onehot, mod_table, precision=highest)
    mod_scale = modulation[:, :width_model]
    mod_shift = modulation[:, width_model : 2 * width_model]
    mod_gate = modulation[:, 2 * width_model :]
    branch_grad = out_grad * mod_gate
    branch_low = branch_grad.astype(BF)
    cos, sin = rope_tables(positions)
    seg_row = segment[None, :]
    seg_col = segment[:, None]

    queries, keys, values = project(normed_full, qkv_full.T, cos, sin, heads)
    mixed, log_totals = attend(queries, keys, values, seg_row, seg_col, lo, hi)

    def rows_of(array, rank):
        return lax.dynamic_slice_in_dim(array, rank * row_count, row_count, 1)

    mixed_own = [rows_of(mixed, ranks[0])] + [
        to_tensor_peer(rows_of(mixed, ranks[d]), d) for d in range(1, n_tensor)
    ]
    attention = sum(dot(mixed_own[d], proj_all[d], 0, 1) for d in range(n_tensor))
    hidden = residual_in + attention + proj_bias
    hidden_normed, inverse_hidden = normalize(hidden)
    modulated = (hidden_normed * (1.0 + mod_scale) + mod_shift).astype(BF)

    branch = down_bias
    modulated_grad = 0.0
    up_parts, down_parts, up_bias_parts = [], [], []
    for d in range(n_tensor):
        bias = lax.dynamic_slice_in_dim(up_bias, ranks[d] * units, units)
        pre_act = dot(modulated, up_all[d], 1, 0) + bias
        active, pullback = jax.vjp(gelu_tanh, pre_act)
        active_low = active.astype(BF)
        branch = branch + dot(active_low, down_all[d], 1, 1)
        pre_grad = pullback(dot(branch_low, down_all[d], 1, 0))[0].astype(BF)
        modulated_grad = modulated_grad + dot(pre_grad, up_all[d], 1, 1)
        up_bias_parts.append(jnp.sum(pre_grad, axis=0, dtype=F32))
        up_parts.append(dot(modulated, pre_grad, 0, 0).astype(BF))
        down_parts.append(dot(branch_low, active_low, 0, 0).astype(BF))

    residual_out = hidden + mod_gate * branch
    gate_grad = out_grad * branch
    scale_grad = modulated_grad * hidden_normed
    hidden_norm_grad = modulated_grad * (1.0 + mod_scale)
    hidden_grad = out_grad + norm_back(hidden_norm_grad, hidden_normed, inverse_hidden)
    hidden_low = hidden_grad.astype(BF)

    mixed_grads = [dot(proj_all[d], hidden_low, 1 - 1, 1).astype(BF) for d in range(n_tensor)]
    arrived = [mixed_grads[0]] + [to_tensor_peer(mixed_grads[d], d) for d in range(1, n_tensor)]
    stacked = jnp.stack(arrived)
    by_rank = jnp.stack([lax.dynamic_index_in_dim(stacked, tensor_rank ^ r, 0, False) for r in range(n_tensor)], axis=1)
    mixed_grad = by_rank.reshape(head_width, total_rows)

    qkv_grad = attend_back(
        queries, keys, values, mixed_grad, mixed, log_totals, seg_row, seg_col, cos, sin, lo, hi
    )

    grad_up = scatter_sum(tensor_sum_scatter(up_parts))
    grad_down = scatter_sum(tensor_sum_scatter(down_parts)).T
    proj_parts = [dot(hidden_low, mixed_own[d], 0, 1).astype(BF) for d in range(n_tensor)]
    grad_proj = scatter_sum(tensor_sum_scatter(proj_parts)).T

    mod_grad = jnp.concatenate([scale_grad, modulated_grad, gate_grad], axis=1)
    mod_seq_grad = lax.dot_general(onehot, mod_grad, (((0,), (0,)), ((), ())), precision=highest)
    up_bias_stack = jnp.stack(up_bias_parts)
    up_bias_part = jnp.stack(
        [lax.dynamic_index_in_dim(up_bias_stack, tensor_rank ^ r, 0, False) for r in range(n_tensor)]
    ).reshape(-1)
    extra = jnp.concatenate(
        [jnp.sum(hidden_grad, axis=0), jnp.sum(branch_grad, axis=0), up_bias_part]
    ).reshape(2, -1)
    pack_sums = butterfly(jnp.concatenate([mod_seq_grad, extra]), "tensor")
    pieces = gather_pieces(pack_sums)
    embed_pieces = gather_pieces(embedded)
    all_mod = jnp.concatenate([piece[:slot_count] for piece in pieces])
    all_embed = jnp.concatenate(embed_pieces)
    grad_time_weight = lax.dot_general(
        all_embed, all_mod, (((0,), (0,)), ((), ())), precision=highest
    )
    grad_time_bias = jnp.sum(all_mod, axis=0)
    biases = sum(piece[slot_count:] for piece in pieces).reshape(-1)
    grad_proj_bias = biases[:width_model]
    grad_down_bias = biases[width_model : 2 * width_model]
    grad_up_bias = biases[2 * width_model :]

    qkv_part = dot(normed_full, qkv_grad, 0, 1).astype(BF)
    grad_qkv = scatter_sum(qkv_part)
    grad_qkv = grad_qkv.reshape(grad_qkv.shape[0], 3, head_width).transpose(1, 0, 2)
    normed_parts = [
        dot(rows_of(qkv_grad, ranks[d]), qkv_full, 0, 1).astype(BF) for d in range(n_tensor)
    ]
    normed_grad = tensor_sum_scatter(normed_parts)
    input_grad = hidden_grad + norm_back(normed_grad * norm_gain, normed_in, inverse_in)
    tail = jnp.stack([jnp.sum(normed_grad * normed_in, axis=0), jnp.sum(normed_grad, axis=0)])
    tail = butterfly(butterfly(tail, "tensor"), "dp")
    return (
        residual_out,
        input_grad,
        tail[0],
        tail[1],
        grad_qkv,
        grad_proj,
        grad_proj_bias,
        grad_up,
        grad_up_bias,
        grad_down,
        grad_down_bias,
        grad_time_weight,
        grad_time_bias,
    )


def solution(mesh):
    in_specs = (
        P(("dp", "tensor"), None),
        P(("dp", "tensor"), None),
        P("dp", None),
        P("dp", None),
        P(),
        P(),
        P(None, "dp", "tensor"),
        P("tensor", "dp"),
        P(),
        P("dp", "tensor"),
        P(),
        P("tensor", "dp"),
        P(),
        P(),
        P(),
    )
    out_specs = (
        P(("dp", "tensor"), None),
        P(("dp", "tensor"), None),
        P(),
        P(),
        P(None, "dp", "tensor"),
        P("tensor", "dp"),
        P(),
        P("dp", "tensor"),
        P(),
        P("tensor", "dp"),
        P(),
        P(),
        P(),
    )
    return jax.shard_map(shards, mesh=mesh, in_specs=in_specs, out_specs=out_specs, check_vma=False)
```

```python
import functools
import math

import jax
import jax.numpy as jnp
from jax import lax
from jax.experimental import pallas as pl
from jax.experimental.pallas import tpu as pltpu
from jax.sharding import PartitionSpec as P


HDIM = 64
HALF = HDIM // 2
BQ = 256
BK = 256
NEG = -1000000000.0
MESH = pl.DeviceIdType.MESH
BF = jnp.bfloat16
F32 = jnp.float32
VMEM_LIMIT = 60 * 1024 * 1024


highest = lax.Precision.HIGHEST


def dot(a, b, ca, cb, out=F32):
    return lax.dot_general(a, b, (((ca,), (cb,)), ((), ())), preferred_element_type=out)


def normalize(values):
    center = values - jnp.mean(values, axis=-1, keepdims=True)
    inverse = lax.rsqrt(jnp.mean(center * center, axis=-1, keepdims=True) + 1e-05)
    return (center * inverse, inverse)


def norm_back(grad_in, normed, inverse):
    return inverse * (
        grad_in
        - jnp.mean(grad_in, axis=-1, keepdims=True)
        - normed * jnp.mean(grad_in * normed, axis=-1, keepdims=True)
    )


def pack_info(lengths, row_total):
    row_index = jnp.arange(row_total, dtype=jnp.int32)
    seq_ends = jnp.cumsum(lengths)
    passed = row_index[:, None] >= seq_ends[None, :]
    segment = jnp.sum(passed.astype(jnp.int32), axis=1)
    starts = jnp.sum(jnp.where(passed, lengths[None, :], 0), axis=1)
    return (segment, row_index - starts)


def key_ranges(lengths, row_total):
    seq_ends = jnp.cumsum(lengths)
    first = jnp.arange(row_total // BQ, dtype=jnp.int32) * BQ
    last = first + (BQ - 1)
    start = jnp.sum(jnp.where(first[:, None] >= seq_ends[None, :], lengths[None, :], 0), axis=1)
    end = jnp.min(jnp.where(seq_ends[None, :] > last[:, None], seq_ends[None, :], row_total), axis=1)
    return (start // BK).astype(jnp.int32), ((end + BK - 1) // BK).astype(jnp.int32)


def time_embed(time_index, embed_width):
    half_width = embed_width // 2
    freqs = jnp.exp(-math.log(10000.0) * jnp.arange(half_width, dtype=jnp.float32) / half_width)
    angles = time_index.astype(jnp.float32)[:, None] * freqs[None, :]
    return jnp.concatenate([jnp.cos(angles), jnp.sin(angles)], axis=1)


def rope_tables(positions):
    inverse = jnp.exp(-math.log(10000.0) * jnp.arange(HALF, dtype=jnp.float32) * (2.0 / HDIM))
    angles = inverse[:, None] * positions.astype(jnp.float32)[None, :]
    return (jnp.cos(angles), jnp.sin(angles))


def project_kernel(heads, n_ref, w_ref, cos_ref, sin_ref, q_ref, k_ref, v_ref):
    width = heads * HDIM
    raw = dot(w_ref[...], n_ref[...], 1, 1)
    cos = cos_ref[...]
    sin = sin_ref[...]
    for part, out_ref, factor in ((0, q_ref, 1.0 / math.sqrt(HDIM)), (1, k_ref, 1.0)):
        for h in range(heads):
            base = part * width + h * HDIM
            a = raw[base : base + HALF]
            b = raw[base + HALF : base + HDIM]
            out_ref[h * HDIM : h * HDIM + HALF] = ((a * cos - b * sin) * factor).astype(BF)
            out_ref[h * HDIM + HALF : (h + 1) * HDIM] = ((b * cos + a * sin) * factor).astype(BF)
    v_ref[...] = raw[2 * width :].astype(BF)


def project(normed, weight_t, cos, sin, heads):
    rows, width_model = normed.shape
    width = heads * HDIM
    tile = 512
    out = jax.ShapeDtypeStruct((width, rows), BF)
    spec = pl.BlockSpec((width, tile), lambda i: (0, i))
    return pl.pallas_call(
        functools.partial(project_kernel, heads),
        name="project_qkv",
        grid=(rows // tile,),
        in_specs=[
            pl.BlockSpec((tile, width_model), lambda i: (i, 0)),
            pl.BlockSpec((3 * width, width_model), lambda i: (0, 0)),
            pl.BlockSpec((HALF, tile), lambda i: (0, i)),
            pl.BlockSpec((HALF, tile), lambda i: (0, i)),
        ],
        out_specs=[spec, spec, spec],
        out_shape=[out, out, out],
        cost_estimate=pl.CostEstimate(
            flops=2 * rows * width_model * 3 * width, bytes_accessed=8 << 20, transcendentals=0
        ),
    )(normed, weight_t, cos, sin)


def wide(column, lanes):
    return jnp.concatenate([column] * (lanes // 128), axis=1)


def attend_kernel(
    heads, lo_ref, hi_ref, q_ref, k_ref, v_ref, srow_ref, scol_ref, o_ref, lse_ref, kt_ref, sc_ref
):
    i = pl.program_id(0)

    @pl.when(i == 0)
    def _():
        for h in range(heads):
            kt_ref[h] = k_ref[h * HDIM : (h + 1) * HDIM, :].T
        sc_ref[...] = jnp.broadcast_to(scol_ref[...], sc_ref.shape)

    srow = srow_ref[...]

    def step(j, carry):
        base = pl.multiple_of(j * BK, BK)
        allowed = wide(sc_ref[pl.ds(base, BK), :], BQ) == srow
        out = []
        for h in range(heads):
            m, l, acc = carry[h]
            s = dot(kt_ref[h, pl.ds(base, BK), :], q_ref[h * HDIM : (h + 1) * HDIM, :], 1, 0)
            s = jnp.where(allowed, s, NEG)
            m_new = jnp.maximum(m, jnp.max(s, axis=0, keepdims=True))
            fade = jnp.exp(m - m_new)
            p = jnp.exp(s - m_new)
            l = fade * l + jnp.sum(p, axis=0, keepdims=True)
            acc = fade * acc + dot(
                v_ref[h * HDIM : (h + 1) * HDIM, pl.ds(base, BK)], p.astype(BF), 1, 0
            )
            out.append((m_new, l, acc))
        return tuple(out)

    empty = (
        jnp.full((1, BQ), -3.0e38, F32),
        jnp.zeros((1, BQ), F32),
        jnp.zeros((HDIM, BQ), F32),
    )
    done = lax.fori_loop(lo_ref[i], hi_ref[i], step, (empty,) * heads)
    for h in range(heads):
        m, l, acc = done[h]
        o_ref[h * HDIM : (h + 1) * HDIM, :] = (acc / l).astype(BF)
        lse_ref[h : h + 1, :] = m + jnp.log(l)


def attend(q, k, v, seg_row, seg_col, lo, hi):
    width, rows = q.shape
    heads = width // HDIM
    whole = lambda i, *_: (0, 0)
    block = lambda i, *_: (0, i)
    return pl.pallas_call(
        functools.partial(attend_kernel, heads),
        name="attend",
        grid_spec=pltpu.PrefetchScalarGridSpec(
            num_scalar_prefetch=2,
            grid=(rows // BQ,),
            in_specs=[
                pl.BlockSpec((width, BQ), block),
                pl.BlockSpec((width, rows), whole),
                pl.BlockSpec((width, rows), whole),
                pl.BlockSpec((1, BQ), block),
                pl.BlockSpec((rows, 1), whole),
            ],
            out_specs=[
                pl.BlockSpec((width, BQ), block),
                pl.BlockSpec((heads, BQ), block),
            ],
            scratch_shapes=[
                pltpu.VMEM((heads, rows, HDIM), BF),
                pltpu.VMEM((rows, 128), jnp.int32),
            ],
        ),
        out_shape=[
            jax.ShapeDtypeStruct((width, rows), BF),
            jax.ShapeDtypeStruct((heads, rows), F32),
        ],
        compiler_params=pltpu.CompilerParams(vmem_limit_bytes=VMEM_LIMIT),
        cost_estimate=pl.CostEstimate(
            flops=rows * rows * heads * HDIM * 8, bytes_accessed=8 << 20, transcendentals=rows * rows
        ),
    )(lo, hi, q, k, v, seg_row, seg_col)


def attend_back_kernel(
    heads,
    lo_ref,
    hi_ref,
    q_ref,
    k_ref,
    v_ref,
    do_ref,
    o_ref,
    lse_ref,
    srow_ref,
    scol_ref,
    cos_ref,
    sin_ref,
    g_ref,
    kt_ref,
    vt_ref,
    sc_ref,
    dk_ref,
    dv_ref,
):
    i = pl.program_id(0)
    width = heads * HDIM

    @pl.when(i == 0)
    def _():
        for h in range(heads):
            kt_ref[h] = k_ref[h * HDIM : (h + 1) * HDIM, :].T
            vt_ref[h] = v_ref[h * HDIM : (h + 1) * HDIM, :].T
        sc_ref[...] = jnp.broadcast_to(scol_ref[...], sc_ref.shape)
        dk_ref[...] = jnp.zeros_like(dk_ref)
        dv_ref[...] = jnp.zeros_like(dv_ref)

    srow = srow_ref[...]
    inner = []
    for h in range(heads):
        part = slice(h * HDIM, (h + 1) * HDIM)
        inner.append(
            jnp.sum(do_ref[part, :].astype(F32) * o_ref[part, :].astype(F32), axis=0, keepdims=True)
        )

    def step(j, carry):
        base = pl.multiple_of(j * BK, BK)
        keys = pl.ds(base, BK)
        allowed = wide(sc_ref[keys, :], BQ) == srow
        out = []
        for h in range(heads):
            part = slice(h * HDIM, (h + 1) * HDIM)
            q = q_ref[part, :]
            grad = do_ref[part, :]
            s = dot(kt_ref[h, keys, :], q, 1, 0)
            s = jnp.where(allowed, s, NEG)
            p = jnp.exp(s - lse_ref[h : h + 1, :])
            dp = dot(vt_ref[h, keys, :], grad, 1, 0)
            ds = (p * (dp - inner[h])).astype(BF)
            out.append(carry[h] + dot(k_ref[part, keys], ds, 1, 0))
            dk_ref[part, keys] += dot(q, ds, 1, 1)
            dv_ref[part, keys] += dot(grad, p.astype(BF), 1, 1)
        return tuple(out)

    done = lax.fori_loop(
        lo_ref[i], hi_ref[i], step, (jnp.zeros((HDIM, BQ), F32),) * heads
    )
    here = pl.ds(pl.multiple_of(i * BQ, BQ), BQ)
    cos = cos_ref[:, here]
    sin = sin_ref[:, here]
    factor = 1.0 / math.sqrt(HDIM)
    for h in range(heads):
        a = done[h][:HALF] * factor
        b = done[h][HALF:] * factor
        g_ref[h * HDIM : h * HDIM + HALF, here] = (a * cos + b * sin).astype(BF)
        g_ref[h * HDIM + HALF : (h + 1) * HDIM, here] = (b * cos - a * sin).astype(BF)

    @pl.when(i == pl.num_programs(0) - 1)
    def _():
        cos_all = cos_ref[...]
        sin_all = sin_ref[...]
        for h in range(heads):
            a = dk_ref[h * HDIM : h * HDIM + HALF, :]
            b = dk_ref[h * HDIM + HALF : (h + 1) * HDIM, :]
            base = width + h * HDIM
            g_ref[base : base + HALF, :] = (a * cos_all + b * sin_all).astype(BF)
            g_ref[base + HALF : base + HDIM, :] = (b * cos_all - a * sin_all).astype(BF)
        g_ref[2 * width :, :] = dv_ref[...].astype(BF)


def attend_back(q, k, v, do, o, lse, seg_row, seg_col, cos, sin, lo, hi):
    width, rows = q.shape
    heads = width // HDIM
    whole = lambda i, *_: (0, 0)
    block = lambda i, *_: (0, i)
    return pl.pallas_call(
        functools.partial(attend_back_kernel, heads),
        name="attend_back",
        grid_spec=pltpu.PrefetchScalarGridSpec(
            num_scalar_prefetch=2,
            grid=(rows // BQ,),
            in_specs=[
                pl.BlockSpec((width, BQ), block),
                pl.BlockSpec((width, rows), whole),
                pl.BlockSpec((width, rows), whole),
                pl.BlockSpec((width, BQ), block),
                pl.BlockSpec((width, BQ), block),
                pl.BlockSpec((heads, BQ), block),
                pl.BlockSpec((1, BQ), block),
                pl.BlockSpec((rows, 1), whole),
                pl.BlockSpec((HALF, rows), whole),
                pl.BlockSpec((HALF, rows), whole),
            ],
            out_specs=pl.BlockSpec((3 * width, rows), whole),
            scratch_shapes=[
                pltpu.VMEM((heads, rows, HDIM), BF),
                pltpu.VMEM((heads, rows, HDIM), BF),
                pltpu.VMEM((rows, 128), jnp.int32),
                pltpu.VMEM((width, rows), F32),
                pltpu.VMEM((width, rows), F32),
            ],
        ),
        out_shape=jax.ShapeDtypeStruct((3 * width, rows), BF),
        compiler_params=pltpu.CompilerParams(vmem_limit_bytes=VMEM_LIMIT),
        cost_estimate=pl.CostEstimate(
            flops=rows * rows * heads * HDIM * 20, bytes_accessed=8 << 20, transcendentals=rows * rows
        ),
    )(lo, hi, q, k, v, do, o, lse, seg_row, seg_col, cos, sin)


class Links:
    def __init__(self, send_sem, recv_sem, n_z):
        dp = lax.axis_index("dp")
        t = lax.axis_index("tensor")
        self.n_z, self.dp, self.t = n_z, dp, t
        self.z, self.x = dp // 2, dp % 2
        self.y, self.c = t // 2, t % 2
        self.core_rank = 2 * self.y + (1 - self.c)
        self.y_rank = 2 * (1 - self.y) + self.c
        self.core = {"tensor": self.core_rank}
        self.across = {"tensor": self.y_rank}
        self.beside = {"dp": 2 * self.z + (1 - self.x)}
        self.send_sem, self.recv_sem = send_sem, recv_sem
        self.slot = 0

    def along(self, step):
        return {"dp": 2 * ((self.z + step) % self.n_z) + self.x}

    def slots(self, count):
        first = self.slot
        self.slot += count
        return first

    def copy(self, src, dst, peer, slot):
        return pltpu.make_async_remote_copy(
            src_ref=src,
            dst_ref=dst,
            send_sem=self.send_sem.at[slot],
            recv_sem=self.recv_sem.at[slot],
            device_id=peer,
            device_id_type=MESH,
        )

    def send(self, src, dst, peer):
        copy = self.copy(src, dst, peer, self.slots(1))
        copy.start()
        return copy


def greet(peers):
    barrier = pltpu.get_barrier_semaphore()
    for peer in peers:
        pl.semaphore_signal(barrier, inc=1, device_id=peer, device_id_type=MESH)
    pl.semaphore_wait(barrier, len(peers))


def opening_kernel(n_z, count, *refs):
    n_ref, w_refs = refs[0], refs[1 : 1 + count]
    n_out, w_outs = refs[1 + count], refs[2 + count : 2 + 2 * count]
    local_sem, send_sem, recv_sem = refs[2 + 2 * count :]
    links = Links(send_sem, recv_sem, n_z)
    greet([links.core, links.across, links.beside] + [links.along(k) for k in range(1, n_z)])
    rows = n_ref.shape[0]

    def n_at(rank):
        return n_out.at[pl.ds(pl.multiple_of(rank * rows, rows), rows)]

    def w_at(n, rank):
        return w_outs[n].at[0, rank] if n in (1, 2) else w_outs[n].at[rank]

    crossed = []

    def cross(rank):
        crossed.append(links.send(w_outs[2].at[0, rank], w_outs[2].at[1, rank], links.across))

    n_y = links.send(n_ref, n_at(links.t), links.across)
    near, far = [], []
    for n in range(count):
        near.append([links.send(w_refs[n], w_at(n, links.dp), links.along(k)) for k in range(1, n_z)])
        far.append([links.send(w_refs[n], w_at(n, links.dp), links.beside)])
    n_core = links.send(n_ref, n_at(links.t), links.core)
    local = [pltpu.make_async_copy(n_ref, n_at(links.t), local_sem.at[0])]
    for n in range(count):
        local.append(pltpu.make_async_copy(w_refs[n], w_at(n, links.dp), local_sem.at[1 + n]))
    for copy in local:
        copy.start()
    others = []
    for n in range(count):
        for k in range(1, n_z):
            near[n][k - 1].wait_recv()
            rank = 2 * ((links.z + n_z - k) % n_z) + links.x
            far[n].append(links.send(w_at(n, rank), w_at(n, rank), links.beside))
            if n == 2:
                cross(rank)
        if n == 2:
            local[1 + n].wait()
            cross(links.dp)
        if n == 1:
            n_y.wait_recv()
            n_relay = links.send(n_at(links.y_rank), n_at(links.y_rank), links.core)
            for copy in far[n]:
                copy.wait_recv()
            local[1 + n].wait()
            others.append(links.send(w_outs[n].at[0], w_outs[n].at[2], links.across))
            others.append(links.send(w_outs[n].at[0], w_outs[n].at[1], links.core))
    for k in range(n_z):
        far[2][k].wait_recv()
        cross(2 * ((links.z + n_z - k) % n_z) + 1 - links.x)
    others[0].wait_recv()
    others.append(links.send(w_outs[1].at[2], w_outs[1].at[3], links.core))
    n_core.wait_recv()
    n_relay.wait_recv()
    others[1].wait_recv()
    others[2].wait_recv()
    for n in range(count):
        if n not in (1, 2):
            for copy in far[n]:
                copy.wait_recv()
            local[1 + n].wait()
        for copy in near[n] + far[n]:
            copy.wait_send()
    for copy in crossed:
        copy.wait_recv()
    for copy in [n_y, n_core, n_relay] + others + crossed:
        copy.wait_send()
    local[0].wait()


def opening(normed, weights, n_dp, n_tensor):
    rows, width = normed.shape
    n_z = n_dp // 2
    count = len(weights)
    slots = count * (2 * n_z - 1) + 6 + n_dp
    shapes = [(n_dp,) + w.shape for w in weights]
    shapes[1] = (n_tensor,) + shapes[1]
    shapes[2] = (2,) + shapes[2]
    return pl.pallas_call(
        functools.partial(opening_kernel, n_z, count),
        name="opening",
        in_specs=[pl.BlockSpec(memory_space=pltpu.VMEM)] * (1 + count),
        out_specs=[pl.BlockSpec(memory_space=pl.ANY)] * (1 + count),
        out_shape=[jax.ShapeDtypeStruct((n_tensor * rows, width), BF)]
        + [jax.ShapeDtypeStruct(shape, BF) for shape in shapes],
        scratch_shapes=[
            pltpu.SemaphoreType.DMA((1 + count,)),
            pltpu.SemaphoreType.DMA((slots,)),
            pltpu.SemaphoreType.DMA((slots,)),
        ],
        compiler_params=pltpu.CompilerParams(collective_id=0, has_side_effects=True),
        cost_estimate=pl.CostEstimate(flops=0, bytes_accessed=64 << 20, transcendentals=0),
    )(normed, *weights)


def closing_kernel(n_z, count, *refs):
    part_refs = refs[:4]
    w_refs = refs[4 : 4 + count]
    x_ref, h_ref, gain_ref, sums_ref = refs[4 + count : 8 + count]
    outs = refs[8 + count : 11 + 2 * count]
    in_grad_ref, tail_ref, all_ref, g_refs = outs[0], outs[1], outs[2], outs[3:]
    scratch = refs[11 + 2 * count :]
    core_buf, y_send, y_recv, vec, all_vec, sums_buf = scratch[:6]
    x_recv = scratch[6 : 6 + count]
    z_send = scratch[6 + count : 6 + 2 * count]
    z_recv = scratch[6 + 2 * count : 6 + 3 * count]
    send_sem, recv_sem = scratch[6 + 3 * count :]
    links = Links(send_sem, recv_sem, n_z)
    n_dp = 2 * n_z
    dp_peers = [{"dp": (links.dp + k) % n_dp} for k in range(1, n_dp)]
    diagonal = {"tensor": 3 - links.t}
    greet([links.core, links.across, diagonal] + dp_peers)

    c1 = links.send(part_refs[1], core_buf.at[0], links.core)
    c3 = links.send(part_refs[3], core_buf.at[1], links.core)
    quarter = sums_ref.shape[1] // 4

    def lanes(rank):
        return pl.ds(pl.multiple_of(rank * quarter, 128), quarter)

    ranks = (links.core_rank, links.y_rank, 3 - links.t)
    tensor_peers = (links.core, links.across, diagonal)
    sums_tensor = [
        links.send(sums_ref.at[:, lanes(rank)], sums_buf.at[links.t], peer)
        for rank, peer in zip(ranks, tensor_peers)
    ]
    sums_buf[links.t] = sums_ref[:, lanes(links.t)]
    x_slots = [links.slots(n_z) for _ in range(count)]
    z_slots = [links.slots(n_z) for _ in range(count)]

    def x_copy(n, s):
        target = (links.z + s) % n_z
        src = w_refs[n].at[target, 1 - links.x]
        return links.copy(src, x_recv[n].at[s], links.beside, x_slots[n] + s)

    def z_copy(n, s):
        peer = {"dp": 2 * ((links.z + s) % n_z) + links.x}
        return links.copy(z_send[n].at[s], z_recv[n].at[s], peer, z_slots[n] + s)

    def x_sum(n, s):
        x_copy(n, s).wait_recv()
        own = w_refs[n][(links.z + s) % n_z, links.x]
        return own.astype(F32) + x_recv[n][s].astype(F32)

    for n in range(count):
        for s in list(range(1, n_z)) + [0]:
            x_copy(n, s).start()

    c1.wait_recv()
    c3.wait_recv()
    y_send[...] = (part_refs[2][...].astype(F32) + core_buf[1].astype(F32)).astype(BF)
    for copy in sums_tensor:
        copy.wait_recv()
    own_lanes = lanes(links.t)
    all_ref[links.dp, :, own_lanes] = sums_buf[0] + sums_buf[1] + sums_buf[2] + sums_buf[3]
    late = None
    y_copy = links.copy(y_send, y_recv, links.across, links.slots(1))
    started = False
    for n in range(count):
        for s in range(1, n_z):
            z_send[n][s] = x_sum(n, s).astype(BF)
            if not started:
                y_copy.start()
                started = True
                here = all_ref.at[links.dp, :, own_lanes]
                sums_dp = [links.send(here, here, peer) for peer in dp_peers]
            if late is not None:
                z_copy(*late).start()
            late = (n, s)
        g_refs[n][...] = x_sum(n, 0)
    z_copy(*late).start()

    for copy in sums_dp:
        copy.wait_recv()
    here = all_ref.at[:, :, own_lanes]
    there = all_ref.at[:, :, lanes(links.y_rank)]
    sums_last = [links.send(here, here, links.across), links.send(here, here, links.core)]
    y_copy.wait_recv()
    grad = part_refs[0][...].astype(F32) + core_buf[0].astype(F32) + y_recv[...].astype(F32)
    normed, inverse = normalize(x_ref[...])
    own_vec = jnp.concatenate(
        [jnp.sum(grad * normed, axis=0, keepdims=True), jnp.sum(grad, axis=0, keepdims=True)], axis=1
    )
    vec[links.t] = own_vec
    in_grad_ref[...] = h_ref[...] + norm_back(grad * gain_ref[...], normed, inverse)
    tensor_sends = [
        links.send(vec.at[links.t], vec.at[links.t], peer)
        for peer in (links.core, links.across, diagonal)
    ]
    sums_last[0].wait_recv()
    sums_last.append(links.send(there, there, links.core))
    for copy in tensor_sends:
        copy.wait()
    total = vec[0] + vec[1] + vec[2] + vec[3]
    all_vec[links.dp] = total
    for n in range(count):
        for s in range(1, n_z):
            z_copy(n, s).wait_recv()
            g_refs[n][...] += z_recv[n][s].astype(F32)
    dp_sends = [links.send(all_vec.at[links.dp], all_vec.at[links.dp], peer) for peer in dp_peers]
    for copy in dp_sends:
        copy.wait_recv()
    total = all_vec[0]
    for r in range(1, n_dp):
        total = total + all_vec[r]
    tail_ref[...] = total
    sums_last[1].wait_recv()
    sums_last[2].wait_recv()
    for copy in [c1, c3, y_copy] + dp_sends + sums_tensor + sums_dp + sums_last:
        copy.wait_send()
    for n in range(count):
        for s in range(n_z):
            x_copy(n, s).wait_send()
            if s > 0:
                z_copy(n, s).wait_send()


def closing(parts, weights, residual_in, hidden_grad, gain, sums, n_dp):
    rows, width = residual_in.shape
    n_z = n_dp // 2
    count = len(weights)
    blocks = [w.reshape(n_z, 2, w.shape[0] // n_dp, w.shape[1]) for w in weights]
    shards = [b.shape[2:] for b in blocks]
    slots = 2 + 2 * count * n_z + 1 + 3 + (n_dp - 1) + 3 + (n_dp - 1) + 3
    vmem = pl.BlockSpec(memory_space=pltpu.VMEM)
    out = pl.pallas_call(
        functools.partial(closing_kernel, n_z, count),
        name="closing",
        in_specs=[vmem] * (8 + count),
        out_specs=[vmem] * (3 + count),
        out_shape=[
            jax.ShapeDtypeStruct((rows, width), F32),
            jax.ShapeDtypeStruct((1, 2 * width), F32),
            jax.ShapeDtypeStruct((n_dp,) + sums.shape, F32),
        ]
        + [jax.ShapeDtypeStruct(shape, F32) for shape in shards],
        scratch_shapes=[
            pltpu.VMEM((2, rows, width), BF),
            pltpu.VMEM((rows, width), BF),
            pltpu.VMEM((rows, width), BF),
            pltpu.VMEM((4, 1, 2 * width), F32),
            pltpu.VMEM((n_dp, 1, 2 * width), F32),
            pltpu.VMEM((4, sums.shape[0], sums.shape[1] // 4), F32),
        ]
        + [pltpu.VMEM((n_z,) + shape, BF) for _ in range(3) for shape in shards]
        + [pltpu.SemaphoreType.DMA((slots,)), pltpu.SemaphoreType.DMA((slots,))],
        compiler_params=pltpu.CompilerParams(
            collective_id=1, has_side_effects=True, vmem_limit_bytes=VMEM_LIMIT
        ),
        cost_estimate=pl.CostEstimate(flops=0, bytes_accessed=64 << 20, transcendentals=0),
    )(*parts, *blocks, residual_in, hidden_grad, gain[None, :], sums)
    return out[0], out[1].reshape(2, width), out[2], out[3:]


ROWS = 128
STRIP = 256


def middle_kernel(slots, *refs):
    (
        mixed_ref,
        proj_ref,
        up_hbm,
        down_hbm,
        down_far_hbm,
        x_ref,
        grad_ref,
        mod_ref,
        sel_ref,
        embed_ref,
        proj_bias_ref,
        up_bias_ref,
        down_bias_ref,
    ) = refs[:13]
    out_ref, h_grad_ref, mixed_grad_ref, sums_ref, up_near, down_near, proj_near, far, proj_far = refs[
        13:22
    ]
    (
        mix_buf,
        mix_t,
        up_buf,
        down_buf,
        hid_s,
        m_s,
        flip_s,
        dz_s,
        dz_t,
        act_s,
        du_s,
        z_acc,
        m_acc,
        up_send,
        down_send,
        up_recv,
        down_recv,
        low_s,
        back_s,
        proj_send,
        proj_recv,
        local_sem,
        send_sem,
        recv_sem,
    ) = refs[22:]
    links = Links(send_sem, recv_sem, slots)
    rows, width = x_ref.shape
    peers = [None, links.core, links.across, {"tensor": 3 - links.t}]
    ranks = [links.t, links.core_rank, links.y_rank, 3 - links.t]
    greet(peers[1:])

    def lanes(rank):
        return pl.ds(pl.multiple_of(rank * rows, rows), rows)

    mix_copies = [
        links.send(mixed_ref.at[:, lanes(ranks[d])], mix_buf.at[d], peers[d]) for d in (3, 2, 1)
    ]
    w_copies = [
        links.send(up_hbm.at[0], up_buf.at[1], links.core),
        links.send(down_hbm, down_buf.at[1], links.core),
        links.send(up_hbm.at[1], up_buf.at[3], links.core),
        links.send(down_far_hbm, down_buf.at[3], links.core),
    ]
    local = [
        pltpu.make_async_copy(up_hbm.at[0], up_buf.at[0], local_sem.at[0]),
        pltpu.make_async_copy(down_hbm, down_buf.at[0], local_sem.at[1]),
        pltpu.make_async_copy(up_hbm.at[1], up_buf.at[2], local_sem.at[2]),
        pltpu.make_async_copy(down_far_hbm, down_buf.at[2], local_sem.at[3]),
    ]
    for copy in local:
        copy.start()

    def tiles(body, carry=0):
        return lax.fori_loop(0, rows // ROWS, body, carry)

    def tile(i):
        return pl.ds(pl.multiple_of(i * ROWS, ROWS), ROWS)

    def gate_step(i, total):
        here = tile(i)
        dz = grad_ref[here, :] * mod_ref[here, 2 * width :]
        dz_s[here, :] = dz.astype(BF)
        return total + jnp.sum(dz, axis=0, keepdims=True)

    down_bias_sum = tiles(gate_step, jnp.zeros((1, width), F32))
    dz_t[...] = dz_s[...].T
    sums_ref[...] = jnp.zeros_like(sums_ref)
    mix_t[0] = mixed_ref[:, lanes(links.t)].T
    for d, copy in zip((3, 2, 1), mix_copies):
        copy.wait_recv()
        mix_t[d] = mix_buf[d].T

    def hidden_step(i, carry):
        here = tile(i)
        hidden = x_ref[here, :] + proj_bias_ref[...]
        for d in range(4):
            hidden = hidden + dot(mix_t[d, here, :], proj_ref[d], 1, 1)
        hid_s[here, :] = hidden
        normed, _ = normalize(hidden)
        scale = mod_ref[here, :width]
        shift = mod_ref[here, width : 2 * width]
        m_s[here, :] = (normed * (1.0 + scale) + shift).astype(BF)
        return carry

    tiles(hidden_step)
    flip_s[...] = m_s[...].T
    z_acc[...] = jnp.zeros_like(z_acc)
    m_acc[...] = jnp.zeros_like(m_acc)
    root = math.sqrt(2.0 / math.pi)

    def feed(d):
        up = up_buf.at[d]
        down = down_buf.at[d]

        def step(i, total):
            here = pl.ds(pl.multiple_of(i * STRIP, STRIP), STRIP)
            u = dot(m_s[here, :], up[...], 1, 0) + up_bias_ref[d]
            square = u * u
            bend = jnp.tanh(root * u * (1.0 + 0.044715 * square))
            half = 0.5 * (1.0 + bend)
            act = (u * half).astype(BF)
            act_s[here, :] = act
            slope = half + 0.5 * u * (1.0 - bend * bend) * (root * (1.0 + 3.0 * 0.044715 * square))
            du = dot(dz_s[here, :], down[...], 1, 0) * slope
            low = du.astype(BF)
            du_s[here, :] = low
            z_acc[here, :] += dot(act, down[...], 1, 1)
            m_acc[here, :] += dot(low, up[...], 1, 1)
            return total + jnp.sum(low.astype(F32), axis=0, keepdims=True)

        total = lax.fori_loop(0, rows // STRIP, step, jnp.zeros((1, width), F32))
        y, c = (d // 2), (d % 2)
        rank = 2 * (y + links.y - 2 * y * links.y) + (c + links.c - 2 * c * links.c)
        sums_ref[pl.ds(17 + rank, 1), :width] = total

    def grads(store):
        def step(j, carry):
            here = pl.ds(pl.multiple_of(j * STRIP, STRIP), STRIP)
            store(here, dot(flip_s[here, :], du_s[...], 1, 0), dot(dz_t[here, :], act_s[...], 1, 0))
            return carry

        lax.fori_loop(0, width // STRIP, step, 0)

    for copy in w_copies:
        copy.wait_recv()

    def outward(e, carry):
        feed(2 * e + 1)

        def store(here, up_part, down_part):
            up_send[e, here, :] = up_part.astype(BF)
            down_send[e, here, :] = down_part.astype(BF)

        grads(store)
        return carry

    lax.fori_loop(0, 2, outward, 0)
    first = links.slots(2)
    second = links.slots(2)

    def up_copy(e):
        return links.copy(up_send.at[e], up_recv.at[e], links.core, first + e)

    def down_copy(e):
        return links.copy(down_send.at[e], down_recv.at[e], links.core, second + e)

    for e in range(2):
        up_copy(e).start()
        down_copy(e).start()
    for copy in local:
        copy.wait()

    for e, up_out, down_out in ((1, far.at[0], far.at[1]), (0, up_near, down_near)):
        feed(2 * e)
        up_copy(e).wait_recv()
        down_copy(e).wait_recv()

        def store(here, up_part, down_part):
            up_out[here, :] = (up_part + up_recv[e, here, :].astype(F32)).astype(BF)
            down_out[here, :] = (down_part + down_recv[e, here, :].astype(F32)).astype(BF)

        grads(store)

    def back_step(i, total):
        here = tile(i)
        hidden = hid_s[here, :]
        normed, inverse = normalize(hidden)
        scale = mod_ref[here, :width]
        gate = mod_ref[here, 2 * width :]
        grad = grad_ref[here, :]
        branch = z_acc[here, :] + down_bias_ref[...]
        shift_grad = m_acc[here, :]
        out_ref[here, :] = hidden + gate * branch
        h_grad = grad + norm_back(shift_grad * (1.0 + scale), normed, inverse)
        h_grad_ref[here, :] = h_grad
        low_s[here, :] = h_grad.astype(BF)
        sel = sel_ref[:, here]
        for part, value in ((0, shift_grad * normed), (1, shift_grad), (2, grad * branch)):
            sums_ref[:, part * width : (part + 1) * width] += lax.dot_general(
                sel, value, (((1,), (0,)), ((), ())), precision=highest, preferred_element_type=F32
            )
        return total + jnp.sum(h_grad, axis=0, keepdims=True)

    proj_bias_sum = tiles(back_step, jnp.zeros((1, width), F32))
    back_copies = []
    for d in (3, 2, 1, 0):
        part = dot(low_s[...], proj_ref[d], 1, 0).astype(BF).T
        if d == 0:
            mixed_grad_ref[:, lanes(links.t)] = part
        else:
            back_s[d] = part
        if d < 3:
            back_copies.append(
                links.send(back_s.at[d + 1], mixed_grad_ref.at[:, lanes(links.t)], peers[d + 1])
            )
    sums_ref[16:17, :width] = proj_bias_sum
    sums_ref[16:17, width : 2 * width] = down_bias_sum
    embed_at = 3 * width
    sums_ref[: embed_ref.shape[0], embed_at : embed_at + embed_ref.shape[1]] = embed_ref[...]
    flip_s[...] = low_s[...].T
    for d in (1, 3):
        proj_send[d // 2] = dot(flip_s[...], mix_t[d], 1, 0).astype(BF)
    own_part = dot(flip_s[...], mix_t[0], 1, 0)
    proj_copies = [links.send(proj_send.at[e], proj_recv.at[e], links.core) for e in range(2)]
    far_part = dot(flip_s[...], mix_t[2], 1, 0)
    for e, part, out in ((0, own_part, proj_near), (1, far_part, proj_far)):
        proj_copies[e].wait_recv()
        out[...] = (part + proj_recv[e].astype(F32)).astype(BF)
    for copy in back_copies:
        copy.wait_recv()
    for copy in mix_copies + w_copies + back_copies + proj_copies:
        copy.wait_send()
    for e in range(2):
        up_copy(e).wait_send()
        down_copy(e).wait_send()


def middle(mixed, proj, up, down, down_far, x, grad, mod, sel, embed, proj_bias, up_bias, down_bias):
    rows, width = x.shape
    head_width, total_rows = mixed.shape
    units = down.shape[1]
    vmem = pl.BlockSpec(memory_space=pltpu.VMEM)
    hbm = pl.BlockSpec(memory_space=pl.ANY)
    sums = (sel.shape[0], -(-(3 * width + embed.shape[1]) // 512) * 512)
    slots = 3 + 4 + 4 + 3 + 2
    square = (2, width, units)
    return pl.pallas_call(
        functools.partial(middle_kernel, 1),
        name="middle",
        in_specs=[vmem, vmem, hbm, hbm, hbm] + [vmem] * 8,
        out_specs=[vmem] * 9,
        out_shape=[
            jax.ShapeDtypeStruct((rows, width), F32),
            jax.ShapeDtypeStruct((rows, width), F32),
            jax.ShapeDtypeStruct((head_width, total_rows), BF),
            jax.ShapeDtypeStruct(sums, F32),
            jax.ShapeDtypeStruct(square[1:], BF),
            jax.ShapeDtypeStruct(square[1:], BF),
            jax.ShapeDtypeStruct((width, head_width), BF),
            jax.ShapeDtypeStruct(square, BF),
            jax.ShapeDtypeStruct((width, head_width), BF),
        ],
        scratch_shapes=[
            pltpu.VMEM((4, head_width, rows), BF),
            pltpu.VMEM((4, rows, head_width), BF),
            pltpu.VMEM((4, width, units), BF),
            pltpu.VMEM((4, width, units), BF),
            pltpu.VMEM((rows, width), F32),
            pltpu.VMEM((rows, width), BF),
            pltpu.VMEM((width, rows), BF),
            pltpu.VMEM((rows, width), BF),
            pltpu.VMEM((width, rows), BF),
            pltpu.VMEM((rows, units), BF),
            pltpu.VMEM((rows, units), BF),
            pltpu.VMEM((rows, width), F32),
            pltpu.VMEM((rows, width), F32),
            pltpu.VMEM(square, BF),
            pltpu.VMEM(square, BF),
            pltpu.VMEM(square, BF),
            pltpu.VMEM(square, BF),
            pltpu.VMEM((rows, width), BF),
            pltpu.VMEM((4, head_width, rows), BF),
            pltpu.VMEM((2, width, head_width), BF),
            pltpu.VMEM((2, width, head_width), BF),
            pltpu.SemaphoreType.DMA((4,)),
            pltpu.SemaphoreType.DMA((slots,)),
            pltpu.SemaphoreType.DMA((slots,)),
        ],
        compiler_params=pltpu.CompilerParams(
            collective_id=2, has_side_effects=True, vmem_limit_bytes=63 * 1024 * 1024
        ),
        cost_estimate=pl.CostEstimate(
            flops=12 * rows * width * units * 4, bytes_accessed=64 << 20, transcendentals=0
        ),
    )(mixed, proj, up, down, down_far, x, grad, mod, sel, embed, proj_bias, up_bias, down_bias)


def to_tensor_peer(value, distance):
    size = lax.axis_size("tensor")
    return lax.ppermute(value, "tensor", [(r, r ^ distance) for r in range(size)])


def shards(
    residual_in,
    out_grad,
    seq_lengths,
    timesteps,
    norm_gain,
    norm_bias,
    qkv_weight,
    proj_weight,
    proj_bias,
    up_weight,
    up_bias,
    down_weight,
    down_bias,
    time_weight,
    time_bias,
):
    row_count, width_model = residual_in.shape
    n_dp = lax.axis_size("dp")
    n_tensor = lax.axis_size("tensor")
    tensor_rank = lax.axis_index("tensor")
    total_rows = row_count * n_tensor
    slot_count = seq_lengths.shape[1]
    head_width = qkv_weight.shape[2]
    heads = head_width // HDIM
    units = up_weight.shape[1]
    ranks = [tensor_rank ^ d for d in range(n_tensor)]

    normed_in, _ = normalize(residual_in)
    normed_low = (normed_in * norm_gain + norm_bias).astype(BF)
    qkv_shard = jnp.transpose(qkv_weight, (1, 0, 2)).reshape(qkv_weight.shape[1], -1).astype(BF)
    normed_full, qkv_full, proj_all, up_own, down_own = opening(
        normed_low,
        (
            qkv_shard,
            proj_weight.T.astype(BF),
            up_weight.astype(BF),
            down_weight.T.astype(BF),
        ),
        n_dp,
        n_tensor,
    )
    qkv_full = qkv_full.reshape(width_model, -1)
    proj_all = proj_all.reshape(n_tensor, width_model, -1)
    up_both = up_own.reshape(2, width_model, -1)
    down_own = down_own.reshape(width_model, -1)
    down_far = to_tensor_peer(down_own, 2)

    segment, positions = pack_info(seq_lengths[0], total_rows)
    lo, hi = key_ranges(seq_lengths[0], total_rows)
    own_segment = lax.dynamic_slice_in_dim(segment, tensor_rank * row_count, row_count)
    slots = jnp.arange(slot_count, dtype=jnp.int32)
    onehot = (own_segment[:, None] == slots[None, :]).astype(F32)
    embedded = time_embed(timesteps[0], time_weight.shape[0])
    mod_table = jnp.dot(embedded, time_weight, precision=highest) + time_bias
    modulation = jnp.dot(onehot, mod_table, precision=highest)
    sums_rows = -(-(slot_count + 1 + n_tensor) // 8) * 8
    chosen = (own_segment[None, :] == jnp.arange(sums_rows, dtype=jnp.int32)[:, None]) & (
        own_segment[None, :] < slot_count
    )
    own_embed = jnp.where(tensor_rank == 0, embedded, 0.0)
    up_bias_rel = jnp.stack(
        [lax.dynamic_slice_in_dim(up_bias, ranks[d] * units, units)[None] for d in range(n_tensor)]
    )
    cos, sin = rope_tables(positions)
    seg_row = segment[None, :]
    seg_col = segment[:, None]

    queries, keys, values = project(normed_full, qkv_full.T, cos, sin, heads)
    mixed, log_totals = attend(queries, keys, values, seg_row, seg_col, lo, hi)

    def rows_of(array, rank):
        return lax.dynamic_slice_in_dim(array, rank * row_count, row_count, 1)

    residual_out, hidden_grad, mixed_grad, sums, up_near, down_near, proj_near, far, proj_far = middle(
        mixed,
        proj_all,
        up_both,
        down_own,
        down_far,
        residual_in,
        out_grad,
        modulation,
        chosen.astype(F32),
        own_embed,
        proj_bias[None, :],
        up_bias_rel,
        down_bias[None, :],
    )

    qkv_grad = attend_back(
        queries, keys, values, mixed_grad, mixed, log_totals, seg_row, seg_col, cos, sin, lo, hi
    )

    proj_far = to_tensor_peer(proj_far, 2)
    far = to_tensor_peer(far, 2)

    def add(near, other):
        return (near.astype(F32) + other.astype(F32)).astype(BF)

    up_sum = add(up_near, far[0])
    down_sum = add(down_near, far[1])
    proj_sum = add(proj_near, proj_far)
    embed_width, mod_width = time_weight.shape

    qkv_part = dot(normed_full, qkv_grad, 0, 1).astype(BF)
    normed_parts = [
        dot(rows_of(qkv_grad, ranks[d]), qkv_full, 0, 1).astype(BF) for d in range(n_tensor)
    ]
    input_grad, tail, packs, grads = closing(
        normed_parts,
        (up_sum, down_sum, proj_sum, qkv_part),
        residual_in,
        hidden_grad,
        norm_gain,
        sums,
        n_dp,
    )
    all_mod = packs[:, :slot_count, :mod_width].reshape(-1, mod_width)
    all_embed = packs[:, :slot_count, mod_width : mod_width + embed_width].reshape(-1, embed_width)
    grad_time_weight = lax.dot_general(
        all_embed, all_mod, (((0,), (0,)), ((), ())), precision=highest
    )
    grad_time_bias = jnp.sum(all_mod, axis=0)
    biases = jnp.sum(packs[:, slot_count : slot_count + 1 + n_tensor], axis=0)
    grad_proj_bias = biases[0, :width_model]
    grad_down_bias = biases[0, width_model : 2 * width_model]
    grad_up_bias = biases[1:, :units].reshape(-1)
    grad_up, grad_down, grad_proj, grad_qkv = grads
    grad_down = grad_down.T
    grad_proj = grad_proj.T
    grad_qkv = grad_qkv.reshape(grad_qkv.shape[0], 3, head_width).transpose(1, 0, 2)
    return (
        residual_out,
        input_grad,
        tail[0],
        tail[1],
        grad_qkv,
        grad_proj,
        grad_proj_bias,
        grad_up,
        grad_up_bias,
        grad_down,
        grad_down_bias,
        grad_time_weight,
        grad_time_bias,
    )


def solution(mesh):
    in_specs = (
        P(("dp", "tensor"), None),
        P(("dp", "tensor"), None),
        P("dp", None),
        P("dp", None),
        P(),
        P(),
        P(None, "dp", "tensor"),
        P("tensor", "dp"),
        P(),
        P("dp", "tensor"),
        P(),
        P("tensor", "dp"),
        P(),
        P(),
        P(),
    )
    out_specs = (
        P(("dp", "tensor"), None),
        P(("dp", "tensor"), None),
        P(),
        P(),
        P(None, "dp", "tensor"),
        P("tensor", "dp"),
        P(),
        P("dp", "tensor"),
        P(),
        P("tensor", "dp"),
        P(),
        P(),
        P(),
    )

    return jax.shard_map(shards, mesh=mesh, in_specs=in_specs, out_specs=out_specs, check_vma=False)
```

```python
import functools
import math

import jax
import jax.numpy as jnp
from jax import lax
from jax.experimental import pallas as pl
from jax.experimental.pallas import tpu as pltpu
from jax.sharding import PartitionSpec as P


HDIM = 64
HALF = HDIM // 2
BQ = 512
BK = 512
ROWS = 128
STRIP = 256
NEG = -1000000000.0
MESH = pl.DeviceIdType.MESH
BF = jnp.bfloat16
F32 = jnp.float32
VMEM_LIMIT = 60 * 1024 * 1024


highest = lax.Precision.HIGHEST


def dot(a, b, ca, cb, out=F32):
    return lax.dot_general(a, b, (((ca,), (cb,)), ((), ())), preferred_element_type=out)


def normalize(values):
    center = values - jnp.mean(values, axis=-1, keepdims=True)
    inverse = lax.rsqrt(jnp.mean(center * center, axis=-1, keepdims=True) + 1e-05)
    return (center * inverse, inverse)


def norm_back(grad_in, normed, inverse):
    return inverse * (
        grad_in
        - jnp.mean(grad_in, axis=-1, keepdims=True)
        - normed * jnp.mean(grad_in * normed, axis=-1, keepdims=True)
    )


def pack_info(lengths, row_total):
    row_index = jnp.arange(row_total, dtype=jnp.int32)
    seq_ends = jnp.cumsum(lengths)
    passed = row_index[:, None] >= seq_ends[None, :]
    segment = jnp.sum(passed.astype(jnp.int32), axis=1)
    starts = jnp.sum(jnp.where(passed, lengths[None, :], 0), axis=1)
    return (segment, row_index - starts)


def key_ranges(lengths, row_total):
    seq_ends = jnp.cumsum(lengths)
    first = jnp.arange(row_total // BQ, dtype=jnp.int32) * BQ
    last = first + (BQ - 1)
    start = jnp.sum(jnp.where(first[:, None] >= seq_ends[None, :], lengths[None, :], 0), axis=1)
    end = jnp.min(jnp.where(seq_ends[None, :] > last[:, None], seq_ends[None, :], row_total), axis=1)
    return (start // BK).astype(jnp.int32), ((end + BK - 1) // BK).astype(jnp.int32)


def time_embed(time_index, embed_width):
    half_width = embed_width // 2
    freqs = jnp.exp(-math.log(10000.0) * jnp.arange(half_width, dtype=jnp.float32) / half_width)
    angles = time_index.astype(jnp.float32)[:, None] * freqs[None, :]
    return jnp.concatenate([jnp.cos(angles), jnp.sin(angles)], axis=1)


def rope_tables(positions):
    inverse = jnp.exp(-math.log(10000.0) * jnp.arange(HALF, dtype=jnp.float32) * (2.0 / HDIM))
    angles = inverse[:, None] * positions.astype(jnp.float32)[None, :]
    return (jnp.cos(angles), jnp.sin(angles))


def project_kernel(heads, n_ref, w_ref, cos_ref, sin_ref, q_ref, k_ref, v_ref, wt_ref):
    width = heads * HDIM

    @pl.when(pl.program_id(0) == 0)
    def _():
        wt_ref[...] = w_ref[...].T

    raw = dot(wt_ref[...], n_ref[...], 1, 1)
    cos = cos_ref[...]
    sin = sin_ref[...]
    for part, out_ref, factor in ((0, q_ref, 1.0 / math.sqrt(HDIM)), (1, k_ref, 1.0)):
        for h in range(heads):
            base = part * width + h * HDIM
            a = raw[base : base + HALF]
            b = raw[base + HALF : base + HDIM]
            out_ref[h * HDIM : h * HDIM + HALF] = ((a * cos - b * sin) * factor).astype(BF)
            out_ref[h * HDIM + HALF : (h + 1) * HDIM] = ((b * cos + a * sin) * factor).astype(BF)
    v_ref[...] = raw[2 * width :].astype(BF)


def project(normed, weight, cos, sin, heads):
    rows, width_model = normed.shape
    width = heads * HDIM
    tile = 512
    out = jax.ShapeDtypeStruct((width, rows), BF)
    spec = pl.BlockSpec((width, tile), lambda i: (0, i))
    return pl.pallas_call(
        functools.partial(project_kernel, heads),
        name="project_qkv",
        grid=(rows // tile,),
        in_specs=[
            pl.BlockSpec((tile, width_model), lambda i: (i, 0)),
            pl.BlockSpec((width_model, 3 * width), lambda i: (0, 0)),
            pl.BlockSpec((HALF, tile), lambda i: (0, i)),
            pl.BlockSpec((HALF, tile), lambda i: (0, i)),
        ],
        out_specs=[spec, spec, spec],
        out_shape=[out, out, out],
        scratch_shapes=[pltpu.VMEM((3 * width, width_model), BF)],
        cost_estimate=pl.CostEstimate(
            flops=2 * rows * width_model * 3 * width, bytes_accessed=8 << 20, transcendentals=0
        ),
    )(normed, weight, cos, sin)


def wide(column, lanes):
    return jnp.concatenate([column] * (lanes // 128), axis=1)


def attend_kernel(
    heads, lo_ref, hi_ref, q_ref, k_ref, v_ref, srow_ref, scol_ref, o_ref, lse_ref, kt_ref, sc_ref
):
    i = pl.program_id(0)

    @pl.when(i == 0)
    def _():
        for h in range(heads):
            kt_ref[h] = k_ref[h * HDIM : (h + 1) * HDIM, :].T
        sc_ref[...] = jnp.broadcast_to(scol_ref[...], sc_ref.shape)

    srow = srow_ref[...]

    def step(j, carry):
        base = pl.multiple_of(j * BK, BK)
        allowed = wide(sc_ref[pl.ds(base, BK), :], BQ) == srow
        out = []
        for h in range(heads):
            m, l, acc = carry[h]
            s = dot(kt_ref[h, pl.ds(base, BK), :], q_ref[h * HDIM : (h + 1) * HDIM, :], 1, 0)
            s = jnp.where(allowed, s, NEG)
            m_new = jnp.maximum(m, jnp.max(s, axis=0, keepdims=True))
            fade = jnp.exp(m - m_new)
            p = jnp.exp(s - m_new)
            l = fade * l + jnp.sum(p, axis=0, keepdims=True)
            acc = fade * acc + dot(
                v_ref[h * HDIM : (h + 1) * HDIM, pl.ds(base, BK)], p.astype(BF), 1, 0
            )
            out.append((m_new, l, acc))
        return tuple(out)

    empty = (
        jnp.full((1, BQ), -3.0e38, F32),
        jnp.zeros((1, BQ), F32),
        jnp.zeros((HDIM, BQ), F32),
    )
    done = lax.fori_loop(lo_ref[i], hi_ref[i], step, (empty,) * heads)
    for h in range(heads):
        m, l, acc = done[h]
        o_ref[h * HDIM : (h + 1) * HDIM, :] = (acc / l).astype(BF)
        lse_ref[h : h + 1, :] = m + jnp.log(l)


def attend(q, k, v, seg_row, seg_col, lo, hi):
    width, rows = q.shape
    heads = width // HDIM
    whole = lambda i, *_: (0, 0)
    block = lambda i, *_: (0, i)
    return pl.pallas_call(
        functools.partial(attend_kernel, heads),
        name="attend",
        grid_spec=pltpu.PrefetchScalarGridSpec(
            num_scalar_prefetch=2,
            grid=(rows // BQ,),
            in_specs=[
                pl.BlockSpec((width, BQ), block),
                pl.BlockSpec((width, rows), whole),
                pl.BlockSpec((width, rows), whole),
                pl.BlockSpec((1, BQ), block),
                pl.BlockSpec((rows, 1), whole),
            ],
            out_specs=[
                pl.BlockSpec((width, BQ), block),
                pl.BlockSpec((heads, BQ), block),
            ],
            scratch_shapes=[
                pltpu.VMEM((heads, rows, HDIM), BF),
                pltpu.VMEM((rows, 128), jnp.int32),
            ],
        ),
        out_shape=[
            jax.ShapeDtypeStruct((width, rows), BF),
            jax.ShapeDtypeStruct((heads, rows), F32),
        ],
        compiler_params=pltpu.CompilerParams(vmem_limit_bytes=VMEM_LIMIT),
        cost_estimate=pl.CostEstimate(
            flops=rows * rows * heads * HDIM * 8, bytes_accessed=8 << 20, transcendentals=rows * rows
        ),
    )(lo, hi, q, k, v, seg_row, seg_col)


def attend_back_kernel(
    heads,
    lo_ref,
    hi_ref,
    q_ref,
    k_ref,
    v_ref,
    do_ref,
    o_ref,
    lse_ref,
    srow_ref,
    scol_ref,
    cos_ref,
    sin_ref,
    g_ref,
    kt_ref,
    vt_ref,
    sc_ref,
    dk_ref,
    dv_ref,
):
    i = pl.program_id(0)
    width = heads * HDIM

    @pl.when(i == 0)
    def _():
        for h in range(heads):
            kt_ref[h] = k_ref[h * HDIM : (h + 1) * HDIM, :].T
            vt_ref[h] = v_ref[h * HDIM : (h + 1) * HDIM, :].T
        sc_ref[...] = jnp.broadcast_to(scol_ref[...], sc_ref.shape)
        dk_ref[...] = jnp.zeros_like(dk_ref)
        dv_ref[...] = jnp.zeros_like(dv_ref)

    srow = srow_ref[...]
    inner = []
    for h in range(heads):
        part = slice(h * HDIM, (h + 1) * HDIM)
        inner.append(
            jnp.sum(do_ref[part, :].astype(F32) * o_ref[part, :].astype(F32), axis=0, keepdims=True)
        )

    def step(j, carry):
        base = pl.multiple_of(j * BK, BK)
        keys = pl.ds(base, BK)
        allowed = wide(sc_ref[keys, :], BQ) == srow
        out = []
        for h in range(heads):
            part = slice(h * HDIM, (h + 1) * HDIM)
            q = q_ref[part, :]
            grad = do_ref[part, :]
            s = dot(kt_ref[h, keys, :], q, 1, 0)
            s = jnp.where(allowed, s, NEG)
            p = jnp.exp(s - lse_ref[h : h + 1, :])
            dp = dot(vt_ref[h, keys, :], grad, 1, 0)
            ds = (p * (dp - inner[h])).astype(BF)
            out.append(carry[h] + dot(k_ref[part, keys], ds, 1, 0))
            dk_ref[part, keys] += dot(q, ds, 1, 1)
            dv_ref[part, keys] += dot(grad, p.astype(BF), 1, 1)
        return tuple(out)

    done = lax.fori_loop(
        lo_ref[i], hi_ref[i], step, (jnp.zeros((HDIM, BQ), F32),) * heads
    )
    here = pl.ds(pl.multiple_of(i * BQ, BQ), BQ)
    cos = cos_ref[:, here]
    sin = sin_ref[:, here]
    factor = 1.0 / math.sqrt(HDIM)
    for h in range(heads):
        a = done[h][:HALF] * factor
        b = done[h][HALF:] * factor
        g_ref[h * HDIM : h * HDIM + HALF, here] = (a * cos + b * sin).astype(BF)
        g_ref[h * HDIM + HALF : (h + 1) * HDIM, here] = (b * cos - a * sin).astype(BF)

    @pl.when(i == pl.num_programs(0) - 1)
    def _():
        cos_all = cos_ref[...]
        sin_all = sin_ref[...]
        for h in range(heads):
            a = dk_ref[h * HDIM : h * HDIM + HALF, :]
            b = dk_ref[h * HDIM + HALF : (h + 1) * HDIM, :]
            base = width + h * HDIM
            g_ref[base : base + HALF, :] = (a * cos_all + b * sin_all).astype(BF)
            g_ref[base + HALF : base + HDIM, :] = (b * cos_all - a * sin_all).astype(BF)
        g_ref[2 * width :, :] = dv_ref[...].astype(BF)


def attend_back(q, k, v, do, o, lse, seg_row, seg_col, cos, sin, lo, hi):
    width, rows = q.shape
    heads = width // HDIM
    whole = lambda i, *_: (0, 0)
    block = lambda i, *_: (0, i)
    return pl.pallas_call(
        functools.partial(attend_back_kernel, heads),
        name="attend_back",
        grid_spec=pltpu.PrefetchScalarGridSpec(
            num_scalar_prefetch=2,
            grid=(rows // BQ,),
            in_specs=[
                pl.BlockSpec((width, BQ), block),
                pl.BlockSpec((width, rows), whole),
                pl.BlockSpec((width, rows), whole),
                pl.BlockSpec((width, BQ), block),
                pl.BlockSpec((width, BQ), block),
                pl.BlockSpec((heads, BQ), block),
                pl.BlockSpec((1, BQ), block),
                pl.BlockSpec((rows, 1), whole),
                pl.BlockSpec((HALF, rows), whole),
                pl.BlockSpec((HALF, rows), whole),
            ],
            out_specs=pl.BlockSpec((3 * width, rows), whole),
            scratch_shapes=[
                pltpu.VMEM((heads, rows, HDIM), BF),
                pltpu.VMEM((heads, rows, HDIM), BF),
                pltpu.VMEM((rows, 128), jnp.int32),
                pltpu.VMEM((width, rows), F32),
                pltpu.VMEM((width, rows), F32),
            ],
        ),
        out_shape=jax.ShapeDtypeStruct((3 * width, rows), BF),
        compiler_params=pltpu.CompilerParams(vmem_limit_bytes=VMEM_LIMIT),
        cost_estimate=pl.CostEstimate(
            flops=rows * rows * heads * HDIM * 20, bytes_accessed=8 << 20, transcendentals=rows * rows
        ),
    )(lo, hi, q, k, v, do, o, lse, seg_row, seg_col, cos, sin)


class Links:
    def __init__(self, send_sem, recv_sem, n_z):
        dp = lax.axis_index("dp")
        t = lax.axis_index("tensor")
        self.n_z, self.dp, self.t = n_z, dp, t
        self.z, self.x = dp // 2, dp % 2
        self.y, self.c = t // 2, t % 2
        self.core_rank = 2 * self.y + (1 - self.c)
        self.y_rank = 2 * (1 - self.y) + self.c
        self.core = {"tensor": self.core_rank}
        self.across = {"tensor": self.y_rank}
        self.beside = {"dp": 2 * self.z + (1 - self.x)}
        self.send_sem, self.recv_sem = send_sem, recv_sem
        self.slot = 0

    def along(self, step):
        return {"dp": 2 * ((self.z + step) % self.n_z) + self.x}

    def slots(self, count):
        first = self.slot
        self.slot += count
        return first

    def copy(self, src, dst, peer, slot):
        return pltpu.make_async_remote_copy(
            src_ref=src,
            dst_ref=dst,
            send_sem=self.send_sem.at[slot],
            recv_sem=self.recv_sem.at[slot],
            device_id=peer,
            device_id_type=MESH,
        )

    def send(self, src, dst, peer):
        copy = self.copy(src, dst, peer, self.slots(1))
        copy.start()
        return copy


def greet(peers):
    barrier = pltpu.get_barrier_semaphore()
    for peer in peers:
        pl.semaphore_signal(barrier, inc=1, device_id=peer, device_id_type=MESH)
    pl.semaphore_wait(barrier, len(peers))


def opening_kernel(n_z, count, *refs):
    x_ref, gain_ref, bias_ref, sel_ref, table_ref = refs[:5]
    w_refs = refs[5 : 5 + count]
    n_out, mod_out, w_outs = refs[5 + count], refs[6 + count], refs[7 + count : 7 + 2 * count]
    n_ref, mod_s, local_sem, send_sem, recv_sem = refs[7 + 2 * count :]
    links = Links(send_sem, recv_sem, n_z)
    greet([links.core, links.across, links.beside] + [links.along(k) for k in range(1, n_z)])
    rows = x_ref.shape[0]

    def n_at(rank):
        return n_out.at[pl.ds(pl.multiple_of(rank * rows, rows), rows)]

    def w_at(n, rank):
        return w_outs[n].at[0, rank] if n in (1, 2) else w_outs[n].at[rank]

    crossed = []

    def cross(rank):
        crossed.append(links.send(w_outs[2].at[0, rank], w_outs[2].at[1, rank], links.across))

    def norm_step(i, carry):
        here = pl.ds(pl.multiple_of(i * ROWS, ROWS), ROWS)
        normed, _ = normalize(x_ref[here, :])
        n_ref[here, :] = (normed * gain_ref[...] + bias_ref[...]).astype(BF)
        return carry

    def mod_step(i):
        here = pl.ds(i * ROWS, ROWS)
        mod_s[here, :] = lax.dot_general(
            sel_ref[here, :],
            table_ref[...],
            (((1,), (0,)), ((), ())),
            precision=highest,
            preferred_element_type=F32,
        )
        copy = pltpu.make_async_copy(mod_s.at[here], mod_out.at[here], local_sem.at[1 + count + i])
        copy.start()
        return copy

    near, far = [], []
    for n in range(count):
        near.append([links.send(w_refs[n], w_at(n, links.dp), links.along(k)) for k in range(1, n_z)])
        far.append([links.send(w_refs[n], w_at(n, links.dp), links.beside)])
    lax.fori_loop(0, rows // ROWS, norm_step, 0)
    tiles = rows // ROWS
    mod_copies = []
    local = [pltpu.make_async_copy(n_ref, n_at(links.t), local_sem.at[0])]
    for n in range(count):
        local.append(pltpu.make_async_copy(w_refs[n], w_at(n, links.dp), local_sem.at[1 + n]))
    for copy in local:
        copy.start()
    n_y = links.send(n_ref, n_at(links.t), links.across)
    n_core = links.send(n_ref, n_at(links.t), links.core)
    others = []
    for n in range(count):
        for k in range(1, n_z):
            near[n][k - 1].wait_recv()
            rank = 2 * ((links.z + n_z - k) % n_z) + links.x
            far[n].append(links.send(w_at(n, rank), w_at(n, rank), links.beside))
            if n == 2:
                cross(rank)
        if n < 2:
            for i in range(n * tiles // 2, (n + 1) * tiles // 2):
                mod_copies.append(mod_step(i))
        if n == 2:
            local[1 + n].wait()
            cross(links.dp)
        if n == 1:
            n_y.wait_recv()
            n_relay = links.send(n_at(links.y_rank), n_at(links.y_rank), links.core)
            for copy in far[n]:
                copy.wait_recv()
            local[1 + n].wait()
            others.append(links.send(w_outs[n].at[0], w_outs[n].at[2], links.across))
            others.append(links.send(w_outs[n].at[0], w_outs[n].at[1], links.core))
    for k in range(n_z):
        far[2][k].wait_recv()
        cross(2 * ((links.z + n_z - k) % n_z) + 1 - links.x)
    others[0].wait_recv()
    others.append(links.send(w_outs[1].at[2], w_outs[1].at[3], links.core))
    n_core.wait_recv()
    n_relay.wait_recv()
    others[1].wait_recv()
    others[2].wait_recv()
    for n in range(count):
        if n not in (1, 2):
            for copy in far[n]:
                copy.wait_recv()
            local[1 + n].wait()
        for copy in near[n] + far[n]:
            copy.wait_send()
    for copy in crossed:
        copy.wait_recv()
    for copy in [n_y, n_core, n_relay] + others + crossed:
        copy.wait_send()
    for copy in local[:1] + mod_copies:
        copy.wait()


def opening(x, gain, bias, sel, table, weights, n_dp, n_tensor):
    rows, width = x.shape
    n_z = n_dp // 2
    count = len(weights)
    slots = count * (2 * n_z - 1) + 6 + n_dp
    shapes = [(n_dp,) + w.shape for w in weights]
    shapes[1] = (n_tensor,) + shapes[1]
    shapes[2] = (2,) + shapes[2]
    return pl.pallas_call(
        functools.partial(opening_kernel, n_z, count),
        name="opening",
        in_specs=[pl.BlockSpec(memory_space=pltpu.VMEM)] * (5 + count),
        out_specs=[pl.BlockSpec(memory_space=pl.ANY)] * (2 + count),
        out_shape=[
            jax.ShapeDtypeStruct((n_tensor * rows, width), BF),
            jax.ShapeDtypeStruct((rows, table.shape[1]), F32),
        ]
        + [jax.ShapeDtypeStruct(shape, BF) for shape in shapes],
        scratch_shapes=[
            pltpu.VMEM((rows, width), BF),
            pltpu.VMEM((rows, table.shape[1]), F32),
            pltpu.SemaphoreType.DMA((1 + count + rows // ROWS,)),
            pltpu.SemaphoreType.DMA((slots,)),
            pltpu.SemaphoreType.DMA((slots,)),
        ],
        compiler_params=pltpu.CompilerParams(
            collective_id=0, has_side_effects=True, vmem_limit_bytes=VMEM_LIMIT
        ),
        cost_estimate=pl.CostEstimate(flops=0, bytes_accessed=64 << 20, transcendentals=0),
    )(x, gain[None, :], bias[None, :], sel, table, *weights)


def closing_kernel(n_z, *refs):
    g_ref, n_ref, w_ref, up_keep, up_got, down_near, down_far, proj_near, proj_far = refs[:9]
    x_ref, h_ref, gain_ref, sums_ref = refs[9:13]
    in_grad_ref, tail_ref, all_ref, up_out, down_out, proj_out, qkv_out = refs[13:20]
    part_send, core_buf, y_send, y_recv, vec, all_vec, qkv_flat, qkv_ref = refs[20:28]
    up_y_send, up_y_recv = refs[28:30]
    x_send, x_recv = refs[30:32], refs[32:35]
    z_send, z_recv = refs[35:39], refs[39:43]
    send_sem, recv_sem = refs[43:]
    links = Links(send_sem, recv_sem, n_z)
    z, x = links.z, links.x
    n_dp = 2 * n_z
    rows, width = x_ref.shape
    outs = (up_out, down_out, proj_out, qkv_out)
    pairs = (None, (down_near, down_far), (proj_near, proj_far))
    dp_peers = [{"dp": (links.dp + k) % n_dp} for k in range(1, n_dp)]
    diagonal = {"tensor": 3 - links.t}
    ranks = [links.t, links.core_rank, links.y_rank, 3 - links.t]
    greet([links.core, links.across, diagonal] + dp_peers)

    quarter = sums_ref.shape[2]

    def lanes(rank):
        return pl.ds(pl.multiple_of(rank * quarter, 128), quarter)

    own_lanes = lanes(links.t)
    all_ref[:, :, own_lanes] = sums_ref[...]
    up_slots = links.slots(n_z)
    x_slots = [None] + [links.slots(n_z) for _ in range(3)]
    z_slots = [links.slots(n_z) for _ in range(4)]
    order = list(range(1, n_z)) + [0]

    def at(s):
        return (z + s) % n_z

    def up_copy(s):
        return links.copy(up_y_send.at[s], up_y_recv.at[s], links.across, up_slots + s)

    def x_copy(n, s):
        src = qkv_ref.at[at(s), 1 - x] if n == 3 else x_send[n - 1].at[s]
        return links.copy(src, x_recv[n - 1].at[s], links.beside, x_slots[n] + s)

    def z_copy(n, s):
        peer = {"dp": 2 * at(s) + x}
        return links.copy(z_send[n].at[s], z_recv[n].at[s], peer, z_slots[n] + s)

    def both(n, s, side):
        near, far = pairs[n]
        return near[at(s), side].astype(F32) + far[at(s), side].astype(F32)

    def x_start(n):
        for s in order:
            if n < 3:
                x_send[n - 1][s] = both(n, s, 1 - x).astype(BF)
            x_copy(n, s).start()

    def value(n, s):
        if n == 0:
            up_copy(s).wait_recv()
            own = up_keep[0, at(s)].astype(F32) + up_got[0, at(s)].astype(F32)
            return own + up_y_recv[s].astype(F32)
        x_copy(n, s).wait_recv()
        own = qkv_ref[at(s), x].astype(F32) if n == 3 else both(n, s, x)
        return own + x_recv[n - 1][s].astype(F32)

    def z_start(n):
        for s in range(1, n_z):
            z_send[n][s] = value(n, s).astype(BF)
            z_copy(n, s).start()
        outs[n][...] = value(n, 0)

    def finish(n):
        for s in range(1, n_z):
            z_copy(n, s).wait_recv()
            outs[n][...] += z_recv[n][s].astype(F32)

    def part(d):
        here = pl.ds(pl.multiple_of(ranks[d] * rows, rows), rows)
        return dot(g_ref[:, here].T, w_ref[...], 1, 1)

    x_start(1)
    for s in order:
        up_y_send[s] = (up_keep[1, at(s)].astype(F32) + up_got[1, at(s)].astype(F32)).astype(BF)
        up_copy(s).start()
    x_start(2)
    part_send[0] = part(3).astype(BF)
    part_send[1] = part(1).astype(BF)
    c3 = links.send(part_send.at[0], core_buf.at[0], links.core)
    z_start(1)
    c1 = links.send(part_send.at[1], core_buf.at[1], links.core)
    far = part(2)
    c3.wait_recv()
    y_send[...] = (far + core_buf[0].astype(F32)).astype(BF)

    strip = 256

    def qkv_step(j, carry):
        here = pl.ds(pl.multiple_of(j * strip, strip), strip)
        qkv_flat[here, :] = dot(g_ref[...], n_ref[:, here], 1, 0).T.astype(BF)
        return carry

    y_copy = links.send(y_send, y_recv, links.across)
    here = all_ref.at[:, :, own_lanes]
    there = all_ref.at[:, :, lanes(links.y_rank)]
    sums_last = [
        links.send(sums_ref, here, links.across),
        links.send(sums_ref, here, links.core),
    ]
    lax.fori_loop(0, width // strip, qkv_step, 0)
    depth = qkv_ref.shape[2]
    for r in range(n_dp):
        qkv_ref[r // 2, r % 2] = qkv_flat[r * depth : (r + 1) * depth, :]
    z_start(0)
    x_start(3)
    z_start(2)
    near = part(0)
    c1.wait_recv()
    near = near + core_buf[1].astype(F32)
    z_start(3)
    y_copy.wait_recv()
    grad = near + y_recv[...].astype(F32)
    normed, inverse = normalize(x_ref[...])
    own_vec = jnp.concatenate(
        [jnp.sum(grad * normed, axis=0, keepdims=True), jnp.sum(grad, axis=0, keepdims=True)], axis=1
    )
    vec[links.t] = own_vec
    in_grad_ref[...] = h_ref[...] + norm_back(grad * gain_ref[...], normed, inverse)
    tensor_sends = [
        links.send(vec.at[links.t], vec.at[links.t], peer)
        for peer in (links.core, links.across, diagonal)
    ]
    finish(1)
    for copy in tensor_sends:
        copy.wait_recv()
    all_vec[links.dp] = vec[0] + vec[1] + vec[2] + vec[3]
    finish(0)
    dp_sends = [links.send(all_vec.at[links.dp], all_vec.at[links.dp], peer) for peer in dp_peers]
    sums_last[0].wait_recv()
    sums_last.append(links.send(there, there, links.core))
    finish(2)
    finish(3)
    for copy in dp_sends:
        copy.wait_recv()
    total = all_vec[0]
    for r in range(1, n_dp):
        total = total + all_vec[r]
    tail_ref[...] = total
    sums_last[1].wait_recv()
    sums_last[2].wait_recv()
    for copy in [c1, c3, y_copy] + dp_sends + sums_last + tensor_sends:
        copy.wait_send()
    for s in range(n_z):
        up_copy(s).wait_send()
        for n in range(4):
            if n > 0:
                x_copy(n, s).wait_send()
            if s > 0:
                z_copy(n, s).wait_send()


def closing(qkv_grad, normed, weight, up, down, proj, residual_in, hidden_grad, gain, sums, n_dp):
    rows, width = residual_in.shape
    head_width = weight.shape[1]
    n_z = n_dp // 2
    depth = width // n_dp

    def blocks(pair):
        return [w.reshape(n_z, 2, depth, w.shape[-1]) for w in pair]

    columns = [up[0].shape[-1], down[0].shape[-1], proj[0].shape[-1], head_width]
    shards = [(depth, c) for c in columns]
    stacks = [(n_z,) + shard for shard in shards]
    slots = 8 * n_z + 2 + 1 + 3 + 3 + (n_dp - 1)
    vmem = pl.BlockSpec(memory_space=pltpu.VMEM)
    out = pl.pallas_call(
        functools.partial(closing_kernel, n_z),
        name="closing",
        in_specs=[vmem] * 13,
        out_specs=[vmem] * 7,
        out_shape=[
            jax.ShapeDtypeStruct((rows, width), F32),
            jax.ShapeDtypeStruct((1, 2 * width), F32),
            jax.ShapeDtypeStruct(sums.shape[:2] + (4 * sums.shape[2],), F32),
        ]
        + [jax.ShapeDtypeStruct(shape, F32) for shape in shards],
        scratch_shapes=[
            pltpu.VMEM((2, rows, width), BF),
            pltpu.VMEM((2, rows, width), BF),
            pltpu.VMEM((rows, width), BF),
            pltpu.VMEM((rows, width), BF),
            pltpu.VMEM((4, 1, 2 * width), F32),
            pltpu.VMEM((n_dp, 1, 2 * width), F32),
            pltpu.VMEM((width, head_width), BF),
            pltpu.VMEM((n_z, 2) + shards[3], BF),
            pltpu.VMEM(stacks[0], BF),
            pltpu.VMEM(stacks[0], BF),
        ]
        + [pltpu.VMEM(shape, BF) for shape in stacks[1:3]]
        + [pltpu.VMEM(shape, BF) for shape in stacks[1:]]
        + [pltpu.VMEM(shape, BF) for _ in range(2) for shape in stacks]
        + [pltpu.SemaphoreType.DMA((slots,)), pltpu.SemaphoreType.DMA((slots,))],
        compiler_params=pltpu.CompilerParams(
            collective_id=1, has_side_effects=True, vmem_limit_bytes=VMEM_LIMIT
        ),
        cost_estimate=pl.CostEstimate(flops=0, bytes_accessed=64 << 20, transcendentals=0),
    )(
        qkv_grad,
        normed,
        weight,
        *up,
        *blocks(down),
        *blocks(proj),
        residual_in,
        hidden_grad,
        gain[None, :],
        sums,
    )
    return out[0], out[1].reshape(2, width), out[2], out[3:]


def middle_kernel(n_z, *refs):
    (
        mixed_ref,
        proj_ref,
        up_hbm,
        down_hbm,
        down_far_hbm,
        x_ref,
        grad_ref,
        mod_ref,
        sel_ref,
        embed_ref,
        proj_bias_ref,
        up_bias_ref,
        down_bias_ref,
    ) = refs[:13]
    out_ref, h_grad_ref, mixed_grad_ref, packs_ref, down_near, proj_near, down_far, proj_far = refs[13:21]
    up_keep, up_away = refs[21:23]
    (
        mix_buf,
        mix_t,
        up_buf,
        down_buf,
        hid_s,
        m_s,
        flip_s,
        dz_s,
        dz_t,
        act_s,
        du_s,
        z_acc,
        m_acc,
        up_send,
        down_send,
        up_recv,
        down_recv,
        low_s,
        back_s,
        proj_send,
        proj_recv,
        sums_ref,
        sums_buf,
        local_sem,
        send_sem,
        recv_sem,
    ) = refs[23:]
    links = Links(send_sem, recv_sem, n_z)
    depth = up_keep.shape[2]
    rows, width = x_ref.shape
    peers = [None, links.core, links.across, {"tensor": 3 - links.t}]
    ranks = [links.t, links.core_rank, links.y_rank, 3 - links.t]
    n_dp = 2 * n_z
    dp_peers = [{"dp": (links.dp + k) % n_dp} for k in range(1, n_dp)]
    greet(peers[1:] + dp_peers)
    quarter = sums_ref.shape[1] // 4

    def lanes(rank):
        return pl.ds(pl.multiple_of(rank * rows, rows), rows)

    mix_copies = [
        links.send(mixed_ref.at[:, lanes(ranks[d])], mix_buf.at[d], peers[d]) for d in (3, 2, 1)
    ]
    w_copies = [
        links.send(up_hbm.at[0], up_buf.at[1], links.core),
        links.send(down_hbm, down_buf.at[1], links.core),
        links.send(up_hbm.at[1], up_buf.at[3], links.core),
        links.send(down_far_hbm, down_buf.at[3], links.core),
    ]
    local = [
        pltpu.make_async_copy(up_hbm.at[0], up_buf.at[0], local_sem.at[0]),
        pltpu.make_async_copy(down_hbm, down_buf.at[0], local_sem.at[1]),
        pltpu.make_async_copy(up_hbm.at[1], up_buf.at[2], local_sem.at[2]),
        pltpu.make_async_copy(down_far_hbm, down_buf.at[2], local_sem.at[3]),
    ]
    for copy in local:
        copy.start()

    def tiles(body, carry=0):
        return lax.fori_loop(0, rows // ROWS, body, carry)

    def tile(i):
        return pl.ds(pl.multiple_of(i * ROWS, ROWS), ROWS)

    def gate_step(i, total):
        here = tile(i)
        dz = grad_ref[here, :] * mod_ref[here, 2 * width :]
        dz_s[here, :] = dz.astype(BF)
        return total + jnp.sum(dz, axis=0, keepdims=True)

    down_bias_sum = tiles(gate_step, jnp.zeros((1, width), F32))
    dz_t[...] = dz_s[...].T
    sums_ref[...] = jnp.zeros_like(sums_ref)
    mix_t[0] = mixed_ref[:, lanes(links.t)].T
    for d, copy in zip((3, 2, 1), mix_copies):
        copy.wait_recv()
        mix_t[d] = mix_buf[d].T

    def hidden_step(i, carry):
        here = tile(i)
        hidden = x_ref[here, :] + proj_bias_ref[...]
        for d in range(4):
            hidden = hidden + dot(mix_t[d, here, :], proj_ref[d], 1, 1)
        hid_s[here, :] = hidden
        normed, _ = normalize(hidden)
        scale = mod_ref[here, :width]
        shift = mod_ref[here, width : 2 * width]
        m_s[here, :] = (normed * (1.0 + scale) + shift).astype(BF)
        return carry

    tiles(hidden_step)
    flip_s[...] = m_s[...].T
    z_acc[...] = jnp.zeros_like(z_acc)
    m_acc[...] = jnp.zeros_like(m_acc)
    root = math.sqrt(2.0 / math.pi)

    def feed(d):
        up = up_buf.at[d]
        down = down_buf.at[d]

        def step(i, total):
            here = pl.ds(pl.multiple_of(i * STRIP, STRIP), STRIP)
            u = dot(m_s[here, :], up[...], 1, 0) + up_bias_ref[d]
            square = u * u
            bend = jnp.tanh(root * u * (1.0 + 0.044715 * square))
            half = 0.5 * (1.0 + bend)
            act = (u * half).astype(BF)
            act_s[here, :] = act
            slope = half + 0.5 * u * (1.0 - bend * bend) * (root * (1.0 + 3.0 * 0.044715 * square))
            du = dot(dz_s[here, :], down[...], 1, 0) * slope
            low = du.astype(BF)
            du_s[here, :] = low
            z_acc[here, :] += dot(act, down[...], 1, 1)
            m_acc[here, :] += dot(low, up[...], 1, 1)
            return total + jnp.sum(low.astype(F32), axis=0, keepdims=True)

        total = lax.fori_loop(0, rows // STRIP, step, jnp.zeros((1, width), F32))
        y, c = (d // 2), (d % 2)
        rank = 2 * (y + links.y - 2 * y * links.y) + (c + links.c - 2 * c * links.c)
        sums_ref[pl.ds(17 + rank, 1), :width] = total

    def grads(store):
        def step(j, carry):
            here = pl.ds(pl.multiple_of(j * STRIP, STRIP), STRIP)
            store(here, dot(flip_s[here, :], du_s[...], 1, 0), dot(dz_t[here, :], act_s[...], 1, 0))
            return carry

        lax.fori_loop(0, width // STRIP, step, 0)

    for copy in w_copies:
        copy.wait_recv()

    def outward(e, carry):
        feed(2 * e + 1)

        def store(here, up_part, down_part):
            up_send[e, here, :] = up_part.astype(BF)
            down_send[e, here, :] = down_part.astype(BF)

        grads(store)
        return carry

    lax.fori_loop(0, 2, outward, 0)
    first = links.slots(2)
    second = links.slots(2)

    def up_copy(e):
        return links.copy(up_send.at[e], up_recv.at[e], links.core, first + e)

    def down_copy(e):
        return links.copy(down_send.at[e], down_recv.at[e], links.core, second + e)

    for e in range(2):
        up_copy(e).start()
        down_copy(e).start()
    for copy in local:
        copy.wait()

    for e, down_sum in ((1, down_far), (0, down_near)):
        feed(2 * e)
        up_copy(e).wait_recv()
        down_copy(e).wait_recv()

        def store(here, up_part, down_part):
            up_send[e, here, :] = (up_part + up_recv[e, here, :].astype(F32)).astype(BF)
            down_sum[here, :] = (down_part + down_recv[e, here, :].astype(F32)).astype(BF)

        up_copy(e).wait_send()
        grads(store)
        for r in range(2 * n_z):
            block = up_send[e, r * depth : (r + 1) * depth, :]

            @pl.when(links.x == r % 2)
            def _():
                up_keep[e, r // 2] = block

            @pl.when(links.x != r % 2)
            def _():
                up_away[e, r // 2] = block

    def back_step(i, total):
        here = tile(i)
        hidden = hid_s[here, :]
        normed, inverse = normalize(hidden)
        scale = mod_ref[here, :width]
        gate = mod_ref[here, 2 * width :]
        grad = grad_ref[here, :]
        branch = z_acc[here, :] + down_bias_ref[...]
        shift_grad = m_acc[here, :]
        out_ref[here, :] = hidden + gate * branch
        h_grad = grad + norm_back(shift_grad * (1.0 + scale), normed, inverse)
        h_grad_ref[here, :] = h_grad
        low_s[here, :] = h_grad.astype(BF)
        sel = sel_ref[:, here]
        for part, value in ((0, shift_grad * normed), (1, shift_grad), (2, grad * branch)):
            sums_ref[:, part * width : (part + 1) * width] += lax.dot_general(
                sel, value, (((1,), (0,)), ((), ())), precision=highest, preferred_element_type=F32
            )
        return total + jnp.sum(h_grad, axis=0, keepdims=True)

    proj_bias_sum = tiles(back_step, jnp.zeros((1, width), F32))
    sums_ref[16:17, :width] = proj_bias_sum
    sums_ref[16:17, width : 2 * width] = down_bias_sum
    embed_at = 3 * width
    sums_ref[: embed_ref.shape[0], embed_at : embed_at + embed_ref.shape[1]] = embed_ref[...]

    def columns(rank):
        return pl.ds(pl.multiple_of(rank * quarter, 128), quarter)

    back_copies = []
    sums_copies = []
    for d in (3, 2, 1, 0):
        part = dot(low_s[...], proj_ref[d], 1, 0).astype(BF).T
        if d == 0:
            mixed_grad_ref[:, lanes(links.t)] = part
        else:
            back_s[d] = part
            sums_copies.append(
                links.send(sums_ref.at[:, columns(ranks[d])], sums_buf.at[links.t], peers[d])
            )
        if d < 3:
            back_copies.append(
                links.send(back_s.at[d + 1], mixed_grad_ref.at[:, lanes(links.t)], peers[d + 1])
            )
    sums_buf[links.t] = sums_ref[:, columns(links.t)]
    flip_s[...] = low_s[...].T
    for d in (1, 3):
        proj_send[d // 2] = dot(flip_s[...], mix_t[d], 1, 0).astype(BF)
    for copy in sums_copies:
        copy.wait_recv()
    packs_ref[links.dp] = sums_buf[0] + sums_buf[1] + sums_buf[2] + sums_buf[3]
    own_part = dot(flip_s[...], mix_t[0], 1, 0)
    here = packs_ref.at[links.dp]
    sums_dp = [links.send(here, here, peer) for peer in dp_peers]
    proj_copies = [links.send(proj_send.at[e], proj_recv.at[e], links.core) for e in range(2)]
    far_part = dot(flip_s[...], mix_t[2], 1, 0)
    for e, part, out in ((0, own_part, proj_near), (1, far_part, proj_far)):
        proj_copies[e].wait_recv()
        out[...] = (part + proj_recv[e].astype(F32)).astype(BF)
    for copy in back_copies + sums_dp:
        copy.wait_recv()
    for copy in mix_copies + w_copies + back_copies + proj_copies + sums_copies + sums_dp:
        copy.wait_send()
    for e in range(2):
        down_copy(e).wait_send()


def middle(
    mixed, proj, up, down, down_far, x, grad, mod, sel, embed, proj_bias, up_bias, down_bias, n_dp
):
    rows, width = x.shape
    head_width, total_rows = mixed.shape
    units = down.shape[1]
    vmem = pl.BlockSpec(memory_space=pltpu.VMEM)
    hbm = pl.BlockSpec(memory_space=pl.ANY)
    sums = (sel.shape[0], -(-(3 * width + embed.shape[1]) // 512) * 512)
    slots = 3 + 4 + 4 + 3 + 2 + 3 + (n_dp - 1)
    square = (2, width, units)
    halves = (2, n_dp // 2, width // n_dp, units)
    return pl.pallas_call(
        functools.partial(middle_kernel, n_dp // 2),
        name="middle",
        in_specs=[vmem, vmem, hbm, hbm, hbm] + [vmem] * 8,
        out_specs=[vmem] * 10,
        out_shape=[
            jax.ShapeDtypeStruct((rows, width), F32),
            jax.ShapeDtypeStruct((rows, width), F32),
            jax.ShapeDtypeStruct((head_width, total_rows), BF),
            jax.ShapeDtypeStruct((n_dp, sums[0], sums[1] // 4), F32),
            jax.ShapeDtypeStruct(square[1:], BF),
            jax.ShapeDtypeStruct((width, head_width), BF),
            jax.ShapeDtypeStruct(square[1:], BF),
            jax.ShapeDtypeStruct((width, head_width), BF),
            jax.ShapeDtypeStruct(halves, BF),
            jax.ShapeDtypeStruct(halves, BF),
        ],
        scratch_shapes=[
            pltpu.VMEM((4, head_width, rows), BF),
            pltpu.VMEM((4, rows, head_width), BF),
            pltpu.VMEM((4, width, units), BF),
            pltpu.VMEM((4, width, units), BF),
            pltpu.VMEM((rows, width), F32),
            pltpu.VMEM((rows, width), BF),
            pltpu.VMEM((width, rows), BF),
            pltpu.VMEM((rows, width), BF),
            pltpu.VMEM((width, rows), BF),
            pltpu.VMEM((rows, units), BF),
            pltpu.VMEM((rows, units), BF),
            pltpu.VMEM((rows, width), F32),
            pltpu.VMEM((rows, width), F32),
            pltpu.VMEM(square, BF),
            pltpu.VMEM(square, BF),
            pltpu.VMEM(square, BF),
            pltpu.VMEM(square, BF),
            pltpu.VMEM((rows, width), BF),
            pltpu.VMEM((4, head_width, rows), BF),
            pltpu.VMEM((2, width, head_width), BF),
            pltpu.VMEM((2, width, head_width), BF),
            pltpu.VMEM(sums, F32),
            pltpu.VMEM((4, sums[0], sums[1] // 4), F32),
            pltpu.SemaphoreType.DMA((4,)),
            pltpu.SemaphoreType.DMA((slots,)),
            pltpu.SemaphoreType.DMA((slots,)),
        ],
        compiler_params=pltpu.CompilerParams(
            collective_id=2, has_side_effects=True, vmem_limit_bytes=63 * 1024 * 1024
        ),
        cost_estimate=pl.CostEstimate(
            flops=12 * rows * width * units * 4, bytes_accessed=64 << 20, transcendentals=0
        ),
    )(mixed, proj, up, down, down_far, x, grad, mod, sel, embed, proj_bias, up_bias, down_bias)


def to_tensor_peer(value, distance):
    size = lax.axis_size("tensor")
    return lax.ppermute(value, "tensor", [(r, r ^ distance) for r in range(size)])


def shards(
    residual_in,
    out_grad,
    seq_lengths,
    timesteps,
    norm_gain,
    norm_bias,
    qkv_weight,
    proj_weight,
    proj_bias,
    up_weight,
    up_bias,
    down_weight,
    down_bias,
    time_weight,
    time_bias,
):
    row_count, width_model = residual_in.shape
    n_dp = lax.axis_size("dp")
    n_tensor = lax.axis_size("tensor")
    tensor_rank = lax.axis_index("tensor")
    total_rows = row_count * n_tensor
    slot_count = seq_lengths.shape[1]
    head_width = qkv_weight.shape[2]
    heads = head_width // HDIM
    units = up_weight.shape[1]
    ranks = [tensor_rank ^ d for d in range(n_tensor)]

    segment, positions = pack_info(seq_lengths[0], total_rows)
    lo, hi = key_ranges(seq_lengths[0], total_rows)
    own_segment = lax.dynamic_slice_in_dim(segment, tensor_rank * row_count, row_count)
    slots = jnp.arange(slot_count, dtype=jnp.int32)
    onehot = (own_segment[:, None] == slots[None, :]).astype(F32)
    embedded = time_embed(timesteps[0], time_weight.shape[0])
    mod_table = jnp.dot(embedded, time_weight, precision=highest) + time_bias
    sums_rows = -(-(slot_count + 1 + n_tensor) // 8) * 8
    chosen = (own_segment[None, :] == jnp.arange(sums_rows, dtype=jnp.int32)[:, None]) & (
        own_segment[None, :] < slot_count
    )
    own_embed = jnp.where(tensor_rank == 0, embedded, 0.0)
    up_bias_rel = jnp.stack(
        [lax.dynamic_slice_in_dim(up_bias, ranks[d] * units, units)[None] for d in range(n_tensor)]
    )
    qkv_shard = jnp.transpose(qkv_weight, (1, 0, 2)).reshape(qkv_weight.shape[1], -1).astype(BF)
    normed_full, modulation, qkv_full, proj_all, up_own, down_own = opening(
        residual_in,
        norm_gain,
        norm_bias,
        onehot,
        mod_table,
        (
            qkv_shard,
            proj_weight.T.astype(BF),
            up_weight.astype(BF),
            down_weight.T.astype(BF),
        ),
        n_dp,
        n_tensor,
    )
    qkv_full = qkv_full.reshape(width_model, -1)
    proj_all = proj_all.reshape(n_tensor, width_model, -1)
    up_both = up_own.reshape(2, width_model, -1)
    down_own = down_own.reshape(width_model, -1)
    down_far = to_tensor_peer(down_own, 2)

    cos, sin = rope_tables(positions)
    seg_row = segment[None, :]
    seg_col = segment[:, None]

    queries, keys, values = project(normed_full, qkv_full, cos, sin, heads)
    mixed, log_totals = attend(queries, keys, values, seg_row, seg_col, lo, hi)

    outs = middle(
        mixed,
        proj_all,
        up_both,
        down_own,
        down_far,
        residual_in,
        out_grad,
        modulation,
        chosen.astype(F32),
        own_embed,
        proj_bias[None, :],
        up_bias_rel,
        down_bias[None, :],
        n_dp,
    )
    residual_out, hidden_grad, mixed_grad, sums, down_near, proj_near, down_other, proj_other = outs[:8]
    up_keep, up_away = outs[8:]

    qkv_grad = attend_back(
        queries, keys, values, mixed_grad, mixed, log_totals, seg_row, seg_col, cos, sin, lo, hi
    )

    proj_far = to_tensor_peer(proj_other, 2)
    down_far = to_tensor_peer(down_other, 2)
    up_got = lax.ppermute(up_away, "dp", [(r, r ^ 1) for r in range(n_dp)])
    embed_width, mod_width = time_weight.shape

    input_grad, tail, packs, grads = closing(
        qkv_grad,
        normed_full,
        qkv_full,
        (up_keep, up_got),
        (down_near, down_far),
        (proj_near, proj_far),
        residual_in,
        hidden_grad,
        norm_gain,
        sums,
        n_dp,
    )
    all_mod = packs[:, :slot_count, :mod_width].reshape(-1, mod_width)
    all_embed = packs[:, :slot_count, mod_width : mod_width + embed_width].reshape(-1, embed_width)
    grad_time_weight = lax.dot_general(
        all_embed, all_mod, (((0,), (0,)), ((), ())), precision=highest
    )
    grad_time_bias = jnp.sum(all_mod, axis=0)
    biases = jnp.sum(packs[:, slot_count : slot_count + 1 + n_tensor], axis=0)
    grad_proj_bias = biases[0, :width_model]
    grad_down_bias = biases[0, width_model : 2 * width_model]
    grad_up_bias = biases[1:, :units].reshape(-1)
    grad_up, grad_down, grad_proj, grad_qkv = grads
    grad_down = grad_down.T
    grad_proj = grad_proj.T
    grad_qkv = grad_qkv.reshape(grad_qkv.shape[0], 3, head_width).transpose(1, 0, 2)
    return (
        residual_out,
        input_grad,
        tail[0],
        tail[1],
        grad_qkv,
        grad_proj,
        grad_proj_bias,
        grad_up,
        grad_up_bias,
        grad_down,
        grad_down_bias,
        grad_time_weight,
        grad_time_bias,
    )


def solution(mesh):
    in_specs = (
        P(("dp", "tensor"), None),
        P(("dp", "tensor"), None),
        P("dp", None),
        P("dp", None),
        P(),
        P(),
        P(None, "dp", "tensor"),
        P("tensor", "dp"),
        P(),
        P("dp", "tensor"),
        P(),
        P("tensor", "dp"),
        P(),
        P(),
        P(),
    )
    out_specs = (
        P(("dp", "tensor"), None),
        P(("dp", "tensor"), None),
        P(),
        P(),
        P(None, "dp", "tensor"),
        P("tensor", "dp"),
        P(),
        P("dp", "tensor"),
        P(),
        P("tensor", "dp"),
        P(),
        P(),
        P(),
    )

    return jax.shard_map(shards, mesh=mesh, in_specs=in_specs, out_specs=out_specs, check_vma=False)
```

```python
import functools
import math

import jax
import jax.numpy as jnp
from jax import lax
from jax.experimental import pallas as pl
from jax.experimental.pallas import tpu as pltpu
from jax.sharding import PartitionSpec as P


HDIM = 64
HALF = HDIM // 2
BQ = 512
BK = 512
ROWS = 128
STRIP = 256
NEG = -1000000000.0
MESH = pl.DeviceIdType.MESH
BF = jnp.bfloat16
F32 = jnp.float32
VMEM_LIMIT = 60 * 1024 * 1024


highest = lax.Precision.HIGHEST


def dot(a, b, ca, cb, out=F32):
    return lax.dot_general(a, b, (((ca,), (cb,)), ((), ())), preferred_element_type=out)


def normalize(values):
    center = values - jnp.mean(values, axis=-1, keepdims=True)
    inverse = lax.rsqrt(jnp.mean(center * center, axis=-1, keepdims=True) + 1e-05)
    return (center * inverse, inverse)


def norm_back(grad_in, normed, inverse):
    return inverse * (
        grad_in
        - jnp.mean(grad_in, axis=-1, keepdims=True)
        - normed * jnp.mean(grad_in * normed, axis=-1, keepdims=True)
    )


def pack_info(lengths, row_total):
    row_index = jnp.arange(row_total, dtype=jnp.int32)
    seq_ends = jnp.cumsum(lengths)
    passed = row_index[:, None] >= seq_ends[None, :]
    segment = jnp.sum(passed.astype(jnp.int32), axis=1)
    starts = jnp.sum(jnp.where(passed, lengths[None, :], 0), axis=1)
    return (segment, row_index - starts)


def key_ranges(lengths, row_total):
    seq_ends = jnp.cumsum(lengths)
    first = jnp.arange(row_total // BQ, dtype=jnp.int32) * BQ
    last = first + (BQ - 1)
    start = jnp.sum(jnp.where(first[:, None] >= seq_ends[None, :], lengths[None, :], 0), axis=1)
    end = jnp.min(jnp.where(seq_ends[None, :] > last[:, None], seq_ends[None, :], row_total), axis=1)
    return (start // BK).astype(jnp.int32), ((end + BK - 1) // BK).astype(jnp.int32)


def time_embed(time_index, embed_width):
    half_width = embed_width // 2
    freqs = jnp.exp(-math.log(10000.0) * jnp.arange(half_width, dtype=jnp.float32) / half_width)
    angles = time_index.astype(jnp.float32)[:, None] * freqs[None, :]
    return jnp.concatenate([jnp.cos(angles), jnp.sin(angles)], axis=1)


def rope_tables(positions):
    inverse = jnp.exp(-math.log(10000.0) * jnp.arange(HALF, dtype=jnp.float32) * (2.0 / HDIM))
    angles = inverse[:, None] * positions.astype(jnp.float32)[None, :]
    return (jnp.cos(angles), jnp.sin(angles))


def project_kernel(heads, n_ref, w_ref, cos_ref, sin_ref, q_ref, k_ref, v_ref, wt_ref):
    width = heads * HDIM

    @pl.when(pl.program_id(0) == 0)
    def _():
        wt_ref[...] = w_ref[...].T

    raw = dot(wt_ref[...], n_ref[...], 1, 1)
    cos = cos_ref[...]
    sin = sin_ref[...]
    for part, out_ref, factor in ((0, q_ref, 1.0 / math.sqrt(HDIM)), (1, k_ref, 1.0)):
        for h in range(heads):
            base = part * width + h * HDIM
            a = raw[base : base + HALF]
            b = raw[base + HALF : base + HDIM]
            out_ref[h * HDIM : h * HDIM + HALF] = ((a * cos - b * sin) * factor).astype(BF)
            out_ref[h * HDIM + HALF : (h + 1) * HDIM] = ((b * cos + a * sin) * factor).astype(BF)
    v_ref[...] = raw[2 * width :].astype(BF)


def project(normed, weight, cos, sin, heads):
    rows, width_model = normed.shape
    width = heads * HDIM
    tile = 512
    out = jax.ShapeDtypeStruct((width, rows), BF)
    spec = pl.BlockSpec((width, tile), lambda i: (0, i))
    return pl.pallas_call(
        functools.partial(project_kernel, heads),
        name="project_qkv",
        grid=(rows // tile,),
        in_specs=[
            pl.BlockSpec((tile, width_model), lambda i: (i, 0)),
            pl.BlockSpec((width_model, 3 * width), lambda i: (0, 0)),
            pl.BlockSpec((HALF, tile), lambda i: (0, i)),
            pl.BlockSpec((HALF, tile), lambda i: (0, i)),
        ],
        out_specs=[spec, spec, spec],
        out_shape=[out, out, out],
        scratch_shapes=[pltpu.VMEM((3 * width, width_model), BF)],
        cost_estimate=pl.CostEstimate(
            flops=2 * rows * width_model * 3 * width, bytes_accessed=8 << 20, transcendentals=0
        ),
    )(normed, weight, cos, sin)


def wide(column, lanes):
    return jnp.concatenate([column] * (lanes // 128), axis=1)


def attend_kernel(
    heads, lo_ref, hi_ref, q_ref, k_ref, v_ref, srow_ref, scol_ref, o_ref, lse_ref, kt_ref, sc_ref
):
    i = pl.program_id(0)

    @pl.when(i == 0)
    def _():
        for h in range(heads):
            kt_ref[h] = k_ref[h * HDIM : (h + 1) * HDIM, :].T
        sc_ref[...] = jnp.broadcast_to(scol_ref[...], sc_ref.shape)

    srow = srow_ref[...]

    def step(j, carry):
        base = pl.multiple_of(j * BK, BK)
        allowed = wide(sc_ref[pl.ds(base, BK), :], BQ) == srow
        out = []
        for h in range(heads):
            m, l, acc = carry[h]
            s = dot(kt_ref[h, pl.ds(base, BK), :], q_ref[h * HDIM : (h + 1) * HDIM, :], 1, 0)
            s = jnp.where(allowed, s, NEG)
            m_new = jnp.maximum(m, jnp.max(s, axis=0, keepdims=True))
            fade = jnp.exp(m - m_new)
            p = jnp.exp(s - m_new)
            l = fade * l + jnp.sum(p, axis=0, keepdims=True)
            acc = fade * acc + dot(
                v_ref[h * HDIM : (h + 1) * HDIM, pl.ds(base, BK)], p.astype(BF), 1, 0
            )
            out.append((m_new, l, acc))
        return tuple(out)

    empty = (
        jnp.full((1, BQ), -3.0e38, F32),
        jnp.zeros((1, BQ), F32),
        jnp.zeros((HDIM, BQ), F32),
    )
    done = lax.fori_loop(lo_ref[i], hi_ref[i], step, (empty,) * heads)
    for h in range(heads):
        m, l, acc = done[h]
        o_ref[h * HDIM : (h + 1) * HDIM, :] = (acc / l).astype(BF)
        lse_ref[h : h + 1, :] = m + jnp.log(l)


def attend(q, k, v, seg_row, seg_col, lo, hi):
    width, rows = q.shape
    heads = width // HDIM
    whole = lambda i, *_: (0, 0)
    block = lambda i, *_: (0, i)
    return pl.pallas_call(
        functools.partial(attend_kernel, heads),
        name="attend",
        grid_spec=pltpu.PrefetchScalarGridSpec(
            num_scalar_prefetch=2,
            grid=(rows // BQ,),
            in_specs=[
                pl.BlockSpec((width, BQ), block),
                pl.BlockSpec((width, rows), whole),
                pl.BlockSpec((width, rows), whole),
                pl.BlockSpec((1, BQ), block),
                pl.BlockSpec((rows, 1), whole),
            ],
            out_specs=[
                pl.BlockSpec((width, BQ), block),
                pl.BlockSpec((heads, BQ), block),
            ],
            scratch_shapes=[
                pltpu.VMEM((heads, rows, HDIM), BF),
                pltpu.VMEM((rows, 128), jnp.int32),
            ],
        ),
        out_shape=[
            jax.ShapeDtypeStruct((width, rows), BF),
            jax.ShapeDtypeStruct((heads, rows), F32),
        ],
        compiler_params=pltpu.CompilerParams(vmem_limit_bytes=VMEM_LIMIT),
        cost_estimate=pl.CostEstimate(
            flops=rows * rows * heads * HDIM * 8, bytes_accessed=8 << 20, transcendentals=rows * rows
        ),
    )(lo, hi, q, k, v, seg_row, seg_col)


def attend_back_kernel(
    heads,
    lo_ref,
    hi_ref,
    q_ref,
    k_ref,
    v_ref,
    do_ref,
    o_ref,
    lse_ref,
    srow_ref,
    scol_ref,
    cos_ref,
    sin_ref,
    g_ref,
    kt_ref,
    vt_ref,
    sc_ref,
    dk_ref,
    dv_ref,
):
    i = pl.program_id(0)
    width = heads * HDIM

    @pl.when(i == 0)
    def _():
        for h in range(heads):
            kt_ref[h] = k_ref[h * HDIM : (h + 1) * HDIM, :].T
            vt_ref[h] = v_ref[h * HDIM : (h + 1) * HDIM, :].T
        sc_ref[...] = jnp.broadcast_to(scol_ref[...], sc_ref.shape)
        dk_ref[...] = jnp.zeros_like(dk_ref)
        dv_ref[...] = jnp.zeros_like(dv_ref)

    srow = srow_ref[...]
    inner = []
    for h in range(heads):
        part = slice(h * HDIM, (h + 1) * HDIM)
        inner.append(
            jnp.sum(do_ref[part, :].astype(F32) * o_ref[part, :].astype(F32), axis=0, keepdims=True)
        )

    def step(j, carry):
        base = pl.multiple_of(j * BK, BK)
        keys = pl.ds(base, BK)
        allowed = wide(sc_ref[keys, :], BQ) == srow
        out = []
        for h in range(heads):
            part = slice(h * HDIM, (h + 1) * HDIM)
            q = q_ref[part, :]
            grad = do_ref[part, :]
            s = dot(kt_ref[h, keys, :], q, 1, 0)
            s = jnp.where(allowed, s, NEG)
            p = jnp.exp(s - lse_ref[h : h + 1, :])
            dp = dot(vt_ref[h, keys, :], grad, 1, 0)
            ds = (p * (dp - inner[h])).astype(BF)
            out.append(carry[h] + dot(k_ref[part, keys], ds, 1, 0))
            dk_ref[part, keys] += dot(q, ds, 1, 1)
            dv_ref[part, keys] += dot(grad, p.astype(BF), 1, 1)
        return tuple(out)

    done = lax.fori_loop(
        lo_ref[i], hi_ref[i], step, (jnp.zeros((HDIM, BQ), F32),) * heads
    )
    here = pl.ds(pl.multiple_of(i * BQ, BQ), BQ)
    cos = cos_ref[:, here]
    sin = sin_ref[:, here]
    factor = 1.0 / math.sqrt(HDIM)
    for h in range(heads):
        a = done[h][:HALF] * factor
        b = done[h][HALF:] * factor
        g_ref[h * HDIM : h * HDIM + HALF, here] = (a * cos + b * sin).astype(BF)
        g_ref[h * HDIM + HALF : (h + 1) * HDIM, here] = (b * cos - a * sin).astype(BF)

    @pl.when(i == pl.num_programs(0) - 1)
    def _():
        cos_all = cos_ref[...]
        sin_all = sin_ref[...]
        for h in range(heads):
            a = dk_ref[h * HDIM : h * HDIM + HALF, :]
            b = dk_ref[h * HDIM + HALF : (h + 1) * HDIM, :]
            base = width + h * HDIM
            g_ref[base : base + HALF, :] = (a * cos_all + b * sin_all).astype(BF)
            g_ref[base + HALF : base + HDIM, :] = (b * cos_all - a * sin_all).astype(BF)
        g_ref[2 * width :, :] = dv_ref[...].astype(BF)


def attend_back(q, k, v, do, o, lse, seg_row, seg_col, cos, sin, lo, hi):
    width, rows = q.shape
    heads = width // HDIM
    whole = lambda i, *_: (0, 0)
    block = lambda i, *_: (0, i)
    return pl.pallas_call(
        functools.partial(attend_back_kernel, heads),
        name="attend_back",
        grid_spec=pltpu.PrefetchScalarGridSpec(
            num_scalar_prefetch=2,
            grid=(rows // BQ,),
            in_specs=[
                pl.BlockSpec((width, BQ), block),
                pl.BlockSpec((width, rows), whole),
                pl.BlockSpec((width, rows), whole),
                pl.BlockSpec((width, BQ), block),
                pl.BlockSpec((width, BQ), block),
                pl.BlockSpec((heads, BQ), block),
                pl.BlockSpec((1, BQ), block),
                pl.BlockSpec((rows, 1), whole),
                pl.BlockSpec((HALF, rows), whole),
                pl.BlockSpec((HALF, rows), whole),
            ],
            out_specs=pl.BlockSpec((3 * width, rows), whole),
            scratch_shapes=[
                pltpu.VMEM((heads, rows, HDIM), BF),
                pltpu.VMEM((heads, rows, HDIM), BF),
                pltpu.VMEM((rows, 128), jnp.int32),
                pltpu.VMEM((width, rows), F32),
                pltpu.VMEM((width, rows), F32),
            ],
        ),
        out_shape=jax.ShapeDtypeStruct((3 * width, rows), BF),
        compiler_params=pltpu.CompilerParams(vmem_limit_bytes=VMEM_LIMIT),
        cost_estimate=pl.CostEstimate(
            flops=rows * rows * heads * HDIM * 20, bytes_accessed=8 << 20, transcendentals=rows * rows
        ),
    )(lo, hi, q, k, v, do, o, lse, seg_row, seg_col, cos, sin)


class Links:
    def __init__(self, send_sem, recv_sem, n_z):
        dp = lax.axis_index("dp")
        t = lax.axis_index("tensor")
        self.n_z, self.dp, self.t = n_z, dp, t
        self.z, self.x = dp // 2, dp % 2
        self.y, self.c = t // 2, t % 2
        self.core_rank = 2 * self.y + (1 - self.c)
        self.y_rank = 2 * (1 - self.y) + self.c
        self.core = {"tensor": self.core_rank}
        self.across = {"tensor": self.y_rank}
        self.beside = {"dp": 2 * self.z + (1 - self.x)}
        self.send_sem, self.recv_sem = send_sem, recv_sem
        self.slot = 0

    def along(self, step):
        return {"dp": 2 * ((self.z + step) % self.n_z) + self.x}

    def slots(self, count):
        first = self.slot
        self.slot += count
        return first

    def copy(self, src, dst, peer, slot):
        return pltpu.make_async_remote_copy(
            src_ref=src,
            dst_ref=dst,
            send_sem=self.send_sem.at[slot],
            recv_sem=self.recv_sem.at[slot],
            device_id=peer,
            device_id_type=MESH,
        )

    def send(self, src, dst, peer):
        copy = self.copy(src, dst, peer, self.slots(1))
        copy.start()
        return copy


def greet(peers):
    barrier = pltpu.get_barrier_semaphore()
    for peer in peers:
        pl.semaphore_signal(barrier, inc=1, device_id=peer, device_id_type=MESH)
    pl.semaphore_wait(barrier, len(peers))


def opening_kernel(n_z, count, *refs):
    x_ref, gain_ref, bias_ref, sel_ref, table_ref, qkv_ref, proj_ref, up_ref, down_ref = refs[:9]
    n_out, mod_out, w_outs = refs[9], refs[10], refs[11 : 11 + count]
    w_refs = refs[11 + count : 11 + 2 * count]
    n_ref, mod_s, local_sem, send_sem, recv_sem = refs[11 + 2 * count :]
    links = Links(send_sem, recv_sem, n_z)
    head_width = qkv_ref.shape[2]
    for part in range(3):
        w_refs[0][:, part * head_width : (part + 1) * head_width] = qkv_ref[part].astype(BF)
    w_refs[1][...] = proj_ref[...].T.astype(BF)
    half = w_refs[2].shape[1]
    w_refs[2][...] = up_ref[:, :half].astype(BF)
    w_refs[3][...] = down_ref[...].astype(BF)
    w_refs[4][...] = up_ref[:, half:].astype(BF)
    greet([links.core, links.across, links.beside] + [links.along(k) for k in range(1, n_z)])
    rows = x_ref.shape[0]

    def n_at(rank):
        return n_out.at[pl.ds(pl.multiple_of(rank * rows, rows), rows)]

    def w_at(n, rank):
        return w_outs[n].at[0, rank] if n in (1, 2) else w_outs[n].at[rank]

    crossed = []

    def cross(rank):
        crossed.append(links.send(w_outs[2].at[0, rank], w_outs[2].at[1, rank], links.across))

    def norm_step(i, carry):
        here = pl.ds(pl.multiple_of(i * ROWS, ROWS), ROWS)
        normed, _ = normalize(x_ref[here, :])
        n_ref[here, :] = (normed * gain_ref[...][None, :] + bias_ref[...][None, :]).astype(BF)
        return carry

    def mod_step(i):
        here = pl.ds(i * ROWS, ROWS)
        mod_s[here, :] = lax.dot_general(
            sel_ref[here, :],
            table_ref[...],
            (((1,), (0,)), ((), ())),
            precision=highest,
            preferred_element_type=F32,
        )
        copy = pltpu.make_async_copy(mod_s.at[here], mod_out.at[here], local_sem.at[1 + count + i])
        copy.start()
        return copy

    near, far = [], []
    for n in range(count):
        near.append([links.send(w_refs[n], w_at(n, links.dp), links.along(k)) for k in range(1, n_z)])
        far.append([links.send(w_refs[n], w_at(n, links.dp), links.beside)])
    lax.fori_loop(0, rows // ROWS, norm_step, 0)
    tiles = rows // ROWS
    mod_copies = []
    local = [pltpu.make_async_copy(n_ref, n_at(links.t), local_sem.at[0])]
    for n in range(count):
        local.append(pltpu.make_async_copy(w_refs[n], w_at(n, links.dp), local_sem.at[1 + n]))
    for copy in local:
        copy.start()
    n_y = links.send(n_ref, n_at(links.t), links.across)
    n_core = links.send(n_ref, n_at(links.t), links.core)
    others = []
    for n in range(count):
        for k in range(1, n_z):
            near[n][k - 1].wait_recv()
            rank = 2 * ((links.z + n_z - k) % n_z) + links.x
            far[n].append(links.send(w_at(n, rank), w_at(n, rank), links.beside))
            if n == 2:
                cross(rank)
        if n < 2:
            for i in range(n * tiles // 2, (n + 1) * tiles // 2):
                mod_copies.append(mod_step(i))
        if n == 2:
            local[1 + n].wait()
            cross(links.dp)
        if n == 1:
            n_y.wait_recv()
            n_relay = links.send(n_at(links.y_rank), n_at(links.y_rank), links.core)
            for copy in far[n]:
                copy.wait_recv()
            local[1 + n].wait()
            others.append(links.send(w_outs[n].at[0], w_outs[n].at[2], links.across))
            others.append(links.send(w_outs[n].at[0], w_outs[n].at[1], links.core))
    for k in range(n_z):
        far[2][k].wait_recv()
        cross(2 * ((links.z + n_z - k) % n_z) + 1 - links.x)
    others[0].wait_recv()
    others.append(links.send(w_outs[1].at[2], w_outs[1].at[3], links.core))
    n_core.wait_recv()
    n_relay.wait_recv()
    others[1].wait_recv()
    others[2].wait_recv()
    for n in range(count):
        if n not in (1, 2):
            for copy in far[n]:
                copy.wait_recv()
            local[1 + n].wait()
        for copy in near[n] + far[n]:
            copy.wait_send()
    for copy in crossed:
        copy.wait_recv()
    for copy in [n_y, n_core, n_relay] + others + crossed:
        copy.wait_send()
    for copy in local[:1] + mod_copies:
        copy.wait()


def opening(x, gain, bias, sel, table, weights, n_dp, n_tensor):
    rows, width = x.shape
    n_z = n_dp // 2
    qkv, proj, up, down = weights
    depth = up.shape[0]
    early = up.shape[1] * 2 // 3 // 128 * 128
    columns = (3 * qkv.shape[2], proj.shape[0], early, down.shape[1], up.shape[1] - early)
    count = len(columns)
    slots = count * (2 * n_z - 1) + 6 + n_dp
    shapes = [(n_dp, depth, c) for c in columns]
    shapes[1] = (n_tensor,) + shapes[1]
    shapes[2] = (2,) + shapes[2]
    return pl.pallas_call(
        functools.partial(opening_kernel, n_z, count),
        name="opening",
        in_specs=[pl.BlockSpec(memory_space=pltpu.VMEM)] * 9,
        out_specs=[pl.BlockSpec(memory_space=pl.ANY)] * (2 + count),
        out_shape=[
            jax.ShapeDtypeStruct((n_tensor * rows, width), BF),
            jax.ShapeDtypeStruct((rows, table.shape[1]), F32),
        ]
        + [jax.ShapeDtypeStruct(shape, BF) for shape in shapes],
        scratch_shapes=[pltpu.VMEM((depth, c), BF) for c in columns]
        + [
            pltpu.VMEM((rows, width), BF),
            pltpu.VMEM((rows, table.shape[1]), F32),
            pltpu.SemaphoreType.DMA((1 + count + rows // ROWS,)),
            pltpu.SemaphoreType.DMA((slots,)),
            pltpu.SemaphoreType.DMA((slots,)),
        ],
        compiler_params=pltpu.CompilerParams(
            collective_id=0, has_side_effects=True, vmem_limit_bytes=VMEM_LIMIT
        ),
        cost_estimate=pl.CostEstimate(flops=0, bytes_accessed=64 << 20, transcendentals=0),
    )(x, gain, bias, sel, table, *weights)


def closing_kernel(n_z, slot_count, embed_width, *refs):
    g_ref, n_ref, w_ref, up_keep, up_got, down_near, down_far, proj_near, proj_far = refs[:9]
    x_ref, h_ref, gain_ref, sums_ref = refs[9:13]
    in_grad_ref, tail_ref, time_ref, time_bias_ref, biases_ref = refs[13:18]
    up_out, down_out, proj_out, qkv_out = refs[18:22]
    all_ref, part_send, core_buf, y_send, y_recv, vec, all_vec, qkv_flat, qkv_ref = refs[22:31]
    up_y_send, up_y_recv = refs[31:33]
    x_send, x_recv = refs[33:35], refs[35:38]
    z_send, z_recv = refs[38:42], refs[42:46]
    send_sem, recv_sem = refs[46:]
    links = Links(send_sem, recv_sem, n_z)
    z, x = links.z, links.x
    n_dp = 2 * n_z
    rows, width = x_ref.shape
    outs = (up_out, down_out, proj_out, qkv_out)
    pairs = (None, (down_near, down_far), (proj_near, proj_far))
    dp_peers = [{"dp": (links.dp + k) % n_dp} for k in range(1, n_dp)]
    diagonal = {"tensor": 3 - links.t}
    ranks = [links.t, links.core_rank, links.y_rank, 3 - links.t]
    greet([links.core, links.across, diagonal] + dp_peers)

    quarter = sums_ref.shape[2]

    def lanes(rank):
        return pl.ds(pl.multiple_of(rank * quarter, 128), quarter)

    own_lanes = lanes(links.t)
    all_ref[:, :, own_lanes] = sums_ref[...]
    up_slots = links.slots(n_z)
    x_slots = [None] + [links.slots(n_z) for _ in range(3)]
    z_slots = [links.slots(n_z) for _ in range(4)]
    order = list(range(1, n_z)) + [0]

    def at(s):
        return (z + s) % n_z

    def up_copy(s):
        return links.copy(up_y_send.at[s], up_y_recv.at[s], links.across, up_slots + s)

    def x_copy(n, s):
        src = qkv_ref.at[at(s), 1 - x] if n == 3 else x_send[n - 1].at[s]
        return links.copy(src, x_recv[n - 1].at[s], links.beside, x_slots[n] + s)

    def z_copy(n, s):
        peer = {"dp": 2 * at(s) + x}
        return links.copy(z_send[n].at[s], z_recv[n].at[s], peer, z_slots[n] + s)

    def both(n, s, side):
        near, far = pairs[n]
        return near[at(s), side].astype(F32) + far[at(s), side].astype(F32)

    def x_start(n):
        for s in order:
            if n < 3:
                x_send[n - 1][s] = both(n, s, 1 - x).astype(BF)
            x_copy(n, s).start()

    def value(n, s):
        if n == 0:
            up_copy(s).wait_recv()
            own = up_keep[0, at(s)].astype(F32) + up_got[0, at(s)].astype(F32)
            return own + up_y_recv[s].astype(F32)
        x_copy(n, s).wait_recv()
        own = qkv_ref[at(s), x].astype(F32) if n == 3 else both(n, s, x)
        return own + x_recv[n - 1][s].astype(F32)

    def z_start(n):
        for s in range(1, n_z):
            z_send[n][s] = value(n, s).astype(BF)
            z_copy(n, s).start()
        outs[n][...] = value(n, 0)

    def finish(n):
        for s in range(1, n_z):
            z_copy(n, s).wait_recv()
            outs[n][...] += z_recv[n][s].astype(F32)

    def part(d):
        here = pl.ds(pl.multiple_of(ranks[d] * rows, rows), rows)
        return dot(g_ref[:, here].T, w_ref[...], 1, 1)

    x_start(1)
    for s in order:
        up_y_send[s] = (up_keep[1, at(s)].astype(F32) + up_got[1, at(s)].astype(F32)).astype(BF)
        up_copy(s).start()
    x_start(2)
    part_send[0] = part(3).astype(BF)
    part_send[1] = part(1).astype(BF)
    c3 = links.send(part_send.at[0], core_buf.at[0], links.core)
    z_start(1)
    c1 = links.send(part_send.at[1], core_buf.at[1], links.core)
    far = part(2)
    c3.wait_recv()
    y_send[...] = (far + core_buf[0].astype(F32)).astype(BF)

    strip = 256

    def qkv_step(j, carry):
        here = pl.ds(pl.multiple_of(j * strip, strip), strip)
        qkv_flat[here, :] = dot(g_ref[...], n_ref[:, here], 1, 0).T.astype(BF)
        return carry

    y_copy = links.send(y_send, y_recv, links.across)
    lax.fori_loop(0, width // strip, qkv_step, 0)
    depth = qkv_ref.shape[2]
    for r in range(n_dp):
        qkv_ref[r // 2, r % 2] = qkv_flat[r * depth : (r + 1) * depth, :]
    z_start(0)
    x_start(3)
    z_start(2)
    near = part(0)
    c1.wait_recv()
    near = near + core_buf[1].astype(F32)
    z_start(3)
    y_copy.wait_recv()
    grad = near + y_recv[...].astype(F32)
    normed, inverse = normalize(x_ref[...])
    own_vec = jnp.concatenate(
        [jnp.sum(grad * normed, axis=0, keepdims=True), jnp.sum(grad, axis=0, keepdims=True)], axis=1
    )
    vec[links.t] = own_vec
    in_grad_ref[...] = h_ref[...] + norm_back(grad * gain_ref[...][None, :], normed, inverse)
    tensor_sends = [
        links.send(vec.at[links.t], vec.at[links.t], peer)
        for peer in (links.core, links.across, diagonal)
    ]
    here = all_ref.at[:, :, own_lanes]
    there = all_ref.at[:, :, lanes(links.y_rank)]
    sums_last = [
        links.send(sums_ref, here, links.across),
        links.send(sums_ref, here, links.core),
    ]
    finish(1)
    for copy in tensor_sends:
        copy.wait_recv()
    all_vec[links.dp] = vec[0] + vec[1] + vec[2] + vec[3]
    finish(0)
    dp_sends = [links.send(all_vec.at[links.dp], all_vec.at[links.dp], peer) for peer in dp_peers]
    sums_last[0].wait_recv()
    sums_last.append(links.send(there, there, links.core))
    finish(2)
    finish(3)
    sums_last[1].wait_recv()
    sums_last[2].wait_recv()
    mod_width = 3 * width
    mods = jnp.concatenate([all_ref[r, :slot_count, :mod_width] for r in range(n_dp)], axis=0)
    embeds = jnp.concatenate(
        [all_ref[r, :slot_count, mod_width : mod_width + embed_width] for r in range(n_dp)], axis=0
    )
    time_ref[...] = lax.dot_general(
        embeds, mods, (((0,), (0,)), ((), ())), precision=highest, preferred_element_type=F32
    )
    time_bias_ref[...] = jnp.sum(mods, axis=0, keepdims=True)
    biases = all_ref[0, slot_count:, : 2 * width]
    for r in range(1, n_dp):
        biases = biases + all_ref[r, slot_count:, : 2 * width]
    biases_ref[...] = biases
    for copy in dp_sends:
        copy.wait_recv()
    total = all_vec[0]
    for r in range(1, n_dp):
        total = total + all_vec[r]
    tail_ref[...] = total
    for copy in [c1, c3, y_copy] + dp_sends + sums_last + tensor_sends:
        copy.wait_send()
    for s in range(n_z):
        up_copy(s).wait_send()
        for n in range(4):
            if n > 0:
                x_copy(n, s).wait_send()
            if s > 0:
                z_copy(n, s).wait_send()


def closing(
    qkv_grad, normed, weight, up, down, proj, residual_in, hidden_grad, gain, sums, n_dp, slot_count, embed_width
):
    rows, width = residual_in.shape
    head_width = weight.shape[1]
    n_z = n_dp // 2
    depth = width // n_dp

    def blocks(pair):
        return [w.reshape(n_z, 2, depth, w.shape[-1]) for w in pair]

    columns = [up[0].shape[-1], down[0].shape[-1], proj[0].shape[-1], head_width]
    shards = [(depth, c) for c in columns]
    stacks = [(n_z,) + shard for shard in shards]
    slots = 8 * n_z + 2 + 1 + 3 + 3 + (n_dp - 1)
    vmem = pl.BlockSpec(memory_space=pltpu.VMEM)
    out = pl.pallas_call(
        functools.partial(closing_kernel, n_z, slot_count, embed_width),
        name="closing",
        in_specs=[vmem] * 13,
        out_specs=[vmem] * 9,
        out_shape=[
            jax.ShapeDtypeStruct((rows, width), F32),
            jax.ShapeDtypeStruct((1, 2 * width), F32),
            jax.ShapeDtypeStruct((embed_width, 3 * width), F32),
            jax.ShapeDtypeStruct((1, 3 * width), F32),
            jax.ShapeDtypeStruct((sums.shape[1] - slot_count, 2 * width), F32),
        ]
        + [jax.ShapeDtypeStruct(shape, F32) for shape in shards],
        scratch_shapes=[
            pltpu.VMEM(sums.shape[:2] + (4 * sums.shape[2],), F32),
            pltpu.VMEM((2, rows, width), BF),
            pltpu.VMEM((2, rows, width), BF),
            pltpu.VMEM((rows, width), BF),
            pltpu.VMEM((rows, width), BF),
            pltpu.VMEM((4, 1, 2 * width), F32),
            pltpu.VMEM((n_dp, 1, 2 * width), F32),
            pltpu.VMEM((width, head_width), BF),
            pltpu.VMEM((n_z, 2) + shards[3], BF),
            pltpu.VMEM(stacks[0], BF),
            pltpu.VMEM(stacks[0], BF),
        ]
        + [pltpu.VMEM(shape, BF) for shape in stacks[1:3]]
        + [pltpu.VMEM(shape, BF) for shape in stacks[1:]]
        + [pltpu.VMEM(shape, BF) for _ in range(2) for shape in stacks]
        + [pltpu.SemaphoreType.DMA((slots,)), pltpu.SemaphoreType.DMA((slots,))],
        compiler_params=pltpu.CompilerParams(
            collective_id=1, has_side_effects=True, vmem_limit_bytes=VMEM_LIMIT
        ),
        cost_estimate=pl.CostEstimate(flops=0, bytes_accessed=64 << 20, transcendentals=0),
    )(
        qkv_grad,
        normed,
        weight,
        *up,
        *blocks(down),
        *blocks(proj),
        residual_in,
        hidden_grad,
        gain,
        sums,
    )
    return out[0], out[1], out[2:5], out[5:]


def middle_kernel(n_z, *refs):
    (
        mixed_ref,
        proj_ref,
        up_hbm,
        up_late_hbm,
        up_late_far_hbm,
        down_hbm,
        down_far_hbm,
        x_ref,
        grad_ref,
        mod_ref,
        sel_ref,
        embed_ref,
        proj_bias_ref,
        up_bias_ref,
        down_bias_ref,
    ) = refs[:15]
    out_ref, h_grad_ref, mixed_grad_ref, packs_ref, down_near, proj_near, down_far, proj_far = refs[15:23]
    up_keep, up_away = refs[23:25]
    (
        mix_buf,
        mix_t,
        up_buf,
        down_buf,
        hid_s,
        m_s,
        flip_s,
        dz_s,
        dz_t,
        act_s,
        du_s,
        z_acc,
        m_acc,
        up_send,
        down_send,
        up_recv,
        down_recv,
        low_s,
        back_s,
        proj_send,
        proj_recv,
        sums_ref,
        sums_buf,
        early_s,
        local_sem,
        send_sem,
        recv_sem,
    ) = refs[25:]
    links = Links(send_sem, recv_sem, n_z)
    depth = up_keep.shape[2]
    rows, width = x_ref.shape
    peers = [None, links.core, links.across, {"tensor": 3 - links.t}]
    ranks = [links.t, links.core_rank, links.y_rank, 3 - links.t]
    n_dp = 2 * n_z
    dp_peers = [{"dp": (links.dp + k) % n_dp} for k in range(1, n_dp)]
    greet(peers[1:] + dp_peers)
    quarter = sums_ref.shape[1] // 4

    def lanes(rank):
        return pl.ds(pl.multiple_of(rank * rows, rows), rows)

    mix_copies = [
        links.send(mixed_ref.at[:, lanes(ranks[d])], mix_buf.at[d], peers[d]) for d in (3, 2, 1)
    ]
    half = up_hbm.shape[2]

    def pieces(shift):
        return [
            (up_hbm.at[0], up_buf.at[shift, :, :half]),
            (up_late_hbm, up_buf.at[shift, :, half:]),
            (down_hbm, down_buf.at[shift]),
            (up_hbm.at[1], up_buf.at[2 + shift, :, :half]),
            (up_late_far_hbm, up_buf.at[2 + shift, :, half:]),
            (down_far_hbm, down_buf.at[2 + shift]),
        ]

    w_copies = [links.send(src, dst, links.core) for src, dst in pieces(1)]
    local = [
        pltpu.make_async_copy(src, dst, local_sem.at[i]) for i, (src, dst) in enumerate(pieces(0))
    ]
    for copy in local:
        copy.start()

    def tiles(body, carry=0):
        return lax.fori_loop(0, rows // ROWS, body, carry)

    def tile(i):
        return pl.ds(pl.multiple_of(i * ROWS, ROWS), ROWS)

    def gate_step(i, total):
        here = tile(i)
        dz = grad_ref[here, :] * mod_ref[here, 2 * width :]
        dz_s[here, :] = dz.astype(BF)
        return total + jnp.sum(dz, axis=0, keepdims=True)

    down_bias_sum = tiles(gate_step, jnp.zeros((1, width), F32))
    dz_t[...] = dz_s[...].T
    sums_ref[...] = jnp.zeros_like(sums_ref)
    for e, copy in ((0, local[2]), (1, local[5])):
        copy.wait()

        def early_step(i, carry):
            here = pl.ds(pl.multiple_of(i * STRIP, STRIP), STRIP)
            early_s[e, here, :] = dot(dz_s[here, :], down_buf[2 * e], 1, 0)
            return carry

        lax.fori_loop(0, rows // STRIP, early_step, 0)
    mix_t[0] = mixed_ref[:, lanes(links.t)].T
    for d, copy in zip((3, 2, 1), mix_copies):
        copy.wait_recv()
        mix_t[d] = mix_buf[d].T

    def hidden_step(i, carry):
        here = tile(i)
        hidden = x_ref[here, :] + proj_bias_ref[...][None, :]
        for d in range(4):
            hidden = hidden + dot(mix_t[d, here, :], proj_ref[d], 1, 1)
        hid_s[here, :] = hidden
        normed, _ = normalize(hidden)
        scale = mod_ref[here, :width]
        shift = mod_ref[here, width : 2 * width]
        m_s[here, :] = (normed * (1.0 + scale) + shift).astype(BF)
        return carry

    tiles(hidden_step)
    flip_s[...] = m_s[...].T
    z_acc[...] = jnp.zeros_like(z_acc)
    m_acc[...] = jnp.zeros_like(m_acc)
    root = math.sqrt(2.0 / math.pi)

    def feed(d, early=None):
        up = up_buf.at[d]
        down = down_buf.at[d]

        def step(i, total):
            here = pl.ds(pl.multiple_of(i * STRIP, STRIP), STRIP)
            u = dot(m_s[here, :], up[...], 1, 0) + up_bias_ref[d]
            square = u * u
            bend = jnp.tanh(root * u * (1.0 + 0.044715 * square))
            half = 0.5 * (1.0 + bend)
            act = (u * half).astype(BF)
            act_s[here, :] = act
            slope = half + 0.5 * u * (1.0 - bend * bend) * (root * (1.0 + 3.0 * 0.044715 * square))
            act_grad = dot(dz_s[here, :], down[...], 1, 0) if early is None else early[here, :]
            du = act_grad * slope
            low = du.astype(BF)
            du_s[here, :] = low
            z_acc[here, :] += dot(act, down[...], 1, 1)
            m_acc[here, :] += dot(low, up[...], 1, 1)
            return total + jnp.sum(low.astype(F32), axis=0, keepdims=True)

        total = lax.fori_loop(0, rows // STRIP, step, jnp.zeros((1, width), F32))
        y, c = (d // 2), (d % 2)
        rank = 2 * (y + links.y - 2 * y * links.y) + (c + links.c - 2 * c * links.c)
        sums_ref[pl.ds(17 + rank, 1), :width] = total

    def grads(store):
        def step(j, carry):
            here = pl.ds(pl.multiple_of(j * STRIP, STRIP), STRIP)
            store(here, dot(flip_s[here, :], du_s[...], 1, 0), dot(dz_t[here, :], act_s[...], 1, 0))
            return carry

        lax.fori_loop(0, width // STRIP, step, 0)

    for copy in w_copies:
        copy.wait_recv()

    def outward(e, carry):
        feed(2 * e + 1)

        def store(here, up_part, down_part):
            up_send[e, here, :] = up_part.astype(BF)
            down_send[e, here, :] = down_part.astype(BF)

        grads(store)
        return carry

    lax.fori_loop(0, 2, outward, 0)
    first = links.slots(2)
    second = links.slots(2)

    def up_copy(e):
        return links.copy(up_send.at[e], up_recv.at[e], links.core, first + e)

    def down_copy(e):
        return links.copy(down_send.at[e], down_recv.at[e], links.core, second + e)

    for e in range(2):
        up_copy(e).start()
        down_copy(e).start()
    for i in (0, 1, 3, 4):
        local[i].wait()

    for e, down_sum in ((1, down_far), (0, down_near)):
        feed(2 * e, early_s.at[e])
        up_copy(e).wait_recv()
        down_copy(e).wait_recv()

        def store(here, up_part, down_part):
            up_send[e, here, :] = (up_part + up_recv[e, here, :].astype(F32)).astype(BF)
            down_sum[here, :] = (down_part + down_recv[e, here, :].astype(F32)).astype(BF)

        up_copy(e).wait_send()
        grads(store)
        for r in range(2 * n_z):
            block = up_send[e, r * depth : (r + 1) * depth, :]

            @pl.when(links.x == r % 2)
            def _():
                up_keep[e, r // 2] = block

            @pl.when(links.x != r % 2)
            def _():
                up_away[e, r // 2] = block

    def back_step(i, total):
        here = tile(i)
        hidden = hid_s[here, :]
        normed, inverse = normalize(hidden)
        scale = mod_ref[here, :width]
        gate = mod_ref[here, 2 * width :]
        grad = grad_ref[here, :]
        branch = z_acc[here, :] + down_bias_ref[...][None, :]
        shift_grad = m_acc[here, :]
        out_ref[here, :] = hidden + gate * branch
        h_grad = grad + norm_back(shift_grad * (1.0 + scale), normed, inverse)
        h_grad_ref[here, :] = h_grad
        low_s[here, :] = h_grad.astype(BF)
        sel = sel_ref[:, here]
        for part, value in ((0, shift_grad * normed), (1, shift_grad), (2, grad * branch)):
            sums_ref[:, part * width : (part + 1) * width] += lax.dot_general(
                sel, value, (((1,), (0,)), ((), ())), precision=highest, preferred_element_type=F32
            )
        return total + jnp.sum(h_grad, axis=0, keepdims=True)

    proj_bias_sum = tiles(back_step, jnp.zeros((1, width), F32))
    sums_ref[16:17, :width] = proj_bias_sum
    sums_ref[16:17, width : 2 * width] = down_bias_sum
    embed_at = 3 * width
    sums_ref[: embed_ref.shape[0], embed_at : embed_at + embed_ref.shape[1]] = embed_ref[...]

    def columns(rank):
        return pl.ds(pl.multiple_of(rank * quarter, 128), quarter)

    back_copies = []
    sums_copies = []
    for d in (3, 2, 1, 0):
        part = dot(low_s[...], proj_ref[d], 1, 0).astype(BF).T
        if d == 0:
            mixed_grad_ref[:, lanes(links.t)] = part
        else:
            back_s[d] = part
            sums_copies.append(
                links.send(sums_ref.at[:, columns(ranks[d])], sums_buf.at[links.t], peers[d])
            )
        if d < 3:
            back_copies.append(
                links.send(back_s.at[d + 1], mixed_grad_ref.at[:, lanes(links.t)], peers[d + 1])
            )
    sums_buf[links.t] = sums_ref[:, columns(links.t)]
    flip_s[...] = low_s[...].T
    for d in (1, 3):
        proj_send[d // 2] = dot(flip_s[...], mix_t[d], 1, 0).astype(BF)
    for copy in sums_copies:
        copy.wait_recv()
    packs_ref[links.dp] = sums_buf[0] + sums_buf[1] + sums_buf[2] + sums_buf[3]
    own_part = dot(flip_s[...], mix_t[0], 1, 0)
    here = packs_ref.at[links.dp]
    sums_dp = [links.send(here, here, peer) for peer in dp_peers]
    proj_copies = [links.send(proj_send.at[e], proj_recv.at[e], links.core) for e in range(2)]
    far_part = dot(flip_s[...], mix_t[2], 1, 0)
    for e, part, out in ((0, own_part, proj_near), (1, far_part, proj_far)):
        proj_copies[e].wait_recv()
        out[...] = (part + proj_recv[e].astype(F32)).astype(BF)
    for copy in back_copies + sums_dp:
        copy.wait_recv()
    for copy in mix_copies + w_copies + back_copies + proj_copies + sums_copies + sums_dp:
        copy.wait_send()
    for e in range(2):
        down_copy(e).wait_send()


def middle(
    mixed, proj, weights, x, grad, mod, sel, embed, proj_bias, up_bias, down_bias, n_dp
):
    rows, width = x.shape
    head_width, total_rows = mixed.shape
    units = weights[3].shape[1]
    vmem = pl.BlockSpec(memory_space=pltpu.VMEM)
    hbm = pl.BlockSpec(memory_space=pl.ANY)
    sums = (sel.shape[0], -(-(3 * width + embed.shape[1]) // 512) * 512)
    slots = 3 + 6 + 4 + 3 + 2 + 3 + (n_dp - 1)
    square = (2, width, units)
    halves = (2, n_dp // 2, width // n_dp, units)
    return pl.pallas_call(
        functools.partial(middle_kernel, n_dp // 2),
        name="middle",
        in_specs=[vmem, vmem] + [hbm] * 5 + [vmem] * 8,
        out_specs=[vmem] * 10,
        out_shape=[
            jax.ShapeDtypeStruct((rows, width), F32),
            jax.ShapeDtypeStruct((rows, width), F32),
            jax.ShapeDtypeStruct((head_width, total_rows), BF),
            jax.ShapeDtypeStruct((n_dp, sums[0], sums[1] // 4), F32),
            jax.ShapeDtypeStruct(square[1:], BF),
            jax.ShapeDtypeStruct((width, head_width), BF),
            jax.ShapeDtypeStruct(square[1:], BF),
            jax.ShapeDtypeStruct((width, head_width), BF),
            jax.ShapeDtypeStruct(halves, BF),
            jax.ShapeDtypeStruct(halves, BF),
        ],
        scratch_shapes=[
            pltpu.VMEM((4, head_width, rows), BF),
            pltpu.VMEM((4, rows, head_width), BF),
            pltpu.VMEM((4, width, units), BF),
            pltpu.VMEM((4, width, units), BF),
            pltpu.VMEM((rows, width), F32),
            pltpu.VMEM((rows, width), BF),
            pltpu.VMEM((width, rows), BF),
            pltpu.VMEM((rows, width), BF),
            pltpu.VMEM((width, rows), BF),
            pltpu.VMEM((rows, units), BF),
            pltpu.VMEM((rows, units), BF),
            pltpu.VMEM((rows, width), F32),
            pltpu.VMEM((rows, width), F32),
            pltpu.VMEM(square, BF),
            pltpu.VMEM(square, BF),
            pltpu.VMEM(square, BF),
            pltpu.VMEM(square, BF),
            pltpu.VMEM((rows, width), BF),
            pltpu.VMEM((4, head_width, rows), BF),
            pltpu.VMEM((2, width, head_width), BF),
            pltpu.VMEM((2, width, head_width), BF),
            pltpu.VMEM(sums, F32),
            pltpu.VMEM((4, sums[0], sums[1] // 4), F32),
            pltpu.VMEM((2, rows, units), F32),
            pltpu.SemaphoreType.DMA((6,)),
            pltpu.SemaphoreType.DMA((slots,)),
            pltpu.SemaphoreType.DMA((slots,)),
        ],
        compiler_params=pltpu.CompilerParams(
            collective_id=2, has_side_effects=True, vmem_limit_bytes=63 * 1024 * 1024
        ),
        cost_estimate=pl.CostEstimate(
            flops=12 * rows * width * units * 4, bytes_accessed=64 << 20, transcendentals=0
        ),
    )(mixed, proj, *weights, x, grad, mod, sel, embed, proj_bias, up_bias, down_bias)


def results_kernel(*refs):
    out_ref, in_grad_ref, tail_ref, time_ref, time_bias_ref, biases_ref = refs[:6]
    up_ref, down_ref, proj_ref, qkv_ref = refs[6:10]
    (
        out,
        in_grad,
        gain,
        bias,
        qkv,
        proj,
        proj_bias,
        up,
        up_bias,
        down,
        down_bias,
        time,
        time_bias,
    ) = refs[10:]
    width = out.shape[1]
    out[...] = out_ref[...]
    in_grad[...] = in_grad_ref[...]
    gain[...] = tail_ref[0, :width]
    bias[...] = tail_ref[0, width:]
    columns = qkv.shape[2]
    for part in range(3):
        qkv[part] = qkv_ref[:, part * columns : (part + 1) * columns]
    proj[...] = proj_ref[...].T
    down[...] = down_ref[...]
    up[...] = up_ref[...]
    proj_bias[...] = biases_ref[0, :width]
    down_bias[...] = biases_ref[0, width:]
    units = up.shape[1]
    for r in range(up_bias.shape[0] // units):
        up_bias[r * units : (r + 1) * units] = biases_ref[1 + r, :units]
    time[...] = time_ref[...]
    time_bias[...] = time_bias_ref[0, :]


def results(residual_out, in_grad, tail, times, grads, tensor_units):
    rows, width = in_grad.shape
    depth, units = grads[0].shape
    columns = grads[2].shape[1]
    shapes = [
        (rows, width),
        (rows, width),
        (width,),
        (width,),
        (3, depth, columns),
        (columns, depth),
        (width,),
        (depth, units),
        (tensor_units,),
        (depth, units),
        (width,),
        times[0].shape,
        (times[0].shape[1],),
    ]
    vmem = pl.BlockSpec(memory_space=pltpu.VMEM)
    return pl.pallas_call(
        results_kernel,
        name="results",
        in_specs=[vmem] * 10,
        out_specs=[vmem] * len(shapes),
        out_shape=[jax.ShapeDtypeStruct(shape, F32) for shape in shapes],
        compiler_params=pltpu.CompilerParams(vmem_limit_bytes=VMEM_LIMIT),
    )(residual_out, in_grad, tail, *times, *grads)


def to_tensor_peer(value, distance):
    size = lax.axis_size("tensor")
    return lax.ppermute(value, "tensor", [(r, r ^ distance) for r in range(size)])


def shards(
    residual_in,
    out_grad,
    seq_lengths,
    timesteps,
    norm_gain,
    norm_bias,
    qkv_weight,
    proj_weight,
    proj_bias,
    up_weight,
    up_bias,
    down_weight,
    down_bias,
    time_weight,
    time_bias,
):
    row_count, width_model = residual_in.shape
    n_dp = lax.axis_size("dp")
    n_tensor = lax.axis_size("tensor")
    tensor_rank = lax.axis_index("tensor")
    total_rows = row_count * n_tensor
    slot_count = seq_lengths.shape[1]
    head_width = qkv_weight.shape[2]
    heads = head_width // HDIM
    units = up_weight.shape[1]
    ranks = [tensor_rank ^ d for d in range(n_tensor)]

    segment, positions = pack_info(seq_lengths[0], total_rows)
    lo, hi = key_ranges(seq_lengths[0], total_rows)
    own_segment = lax.dynamic_slice_in_dim(segment, tensor_rank * row_count, row_count)
    slots = jnp.arange(slot_count, dtype=jnp.int32)
    onehot = (own_segment[:, None] == slots[None, :]).astype(F32)
    embedded = time_embed(timesteps[0], time_weight.shape[0])
    mod_table = jnp.dot(embedded, time_weight, precision=highest) + time_bias
    sums_rows = -(-(slot_count + 1 + n_tensor) // 8) * 8
    chosen = (own_segment[None, :] == jnp.arange(sums_rows, dtype=jnp.int32)[:, None]) & (
        own_segment[None, :] < slot_count
    )
    own_embed = jnp.where(tensor_rank == 0, embedded, 0.0)
    up_bias_rel = jnp.stack(
        [lax.dynamic_slice_in_dim(up_bias, ranks[d] * units, units)[None] for d in range(n_tensor)]
    )
    normed_full, modulation, qkv_full, proj_all, up_both, down_own, up_late = opening(
        residual_in,
        norm_gain,
        norm_bias,
        onehot,
        mod_table,
        (qkv_weight, proj_weight, up_weight, down_weight.T),
        n_dp,
        n_tensor,
    )
    qkv_full = qkv_full.reshape(width_model, -1)
    proj_all = proj_all.reshape(n_tensor, width_model, -1)
    up_both = up_both.reshape(2, width_model, -1)
    down_own = down_own.reshape(width_model, -1)
    up_late = up_late.reshape(width_model, -1)
    up_late_far = to_tensor_peer(up_late, 2)
    down_far = to_tensor_peer(down_own, 2)

    cos, sin = rope_tables(positions)
    seg_row = segment[None, :]
    seg_col = segment[:, None]

    queries, keys, values = project(normed_full, qkv_full, cos, sin, heads)
    mixed, log_totals = attend(queries, keys, values, seg_row, seg_col, lo, hi)

    outs = middle(
        mixed,
        proj_all,
        (up_both, up_late, up_late_far, down_own, down_far),
        residual_in,
        out_grad,
        modulation,
        chosen.astype(F32),
        own_embed,
        proj_bias,
        up_bias_rel,
        down_bias,
        n_dp,
    )
    residual_out, hidden_grad, mixed_grad, sums, down_near, proj_near, down_other, proj_other = outs[:8]
    up_keep, up_away = outs[8:]

    qkv_grad = attend_back(
        queries, keys, values, mixed_grad, mixed, log_totals, seg_row, seg_col, cos, sin, lo, hi
    )

    proj_far = to_tensor_peer(proj_other, 2)
    down_far = to_tensor_peer(down_other, 2)
    up_got = lax.ppermute(up_away, "dp", [(r, r ^ 1) for r in range(n_dp)])

    input_grad, tail, times, grads = closing(
        qkv_grad,
        normed_full,
        qkv_full,
        (up_keep, up_got),
        (down_near, down_far),
        (proj_near, proj_far),
        residual_in,
        hidden_grad,
        norm_gain,
        sums,
        n_dp,
        slot_count,
        time_weight.shape[0],
    )
    done = list(results(residual_out, input_grad, tail, times, grads, up_bias.shape[0]))
    done[9] = done[9].T
    return tuple(done)


def solution(mesh):
    in_specs = (
        P(("dp", "tensor"), None),
        P(("dp", "tensor"), None),
        P("dp", None),
        P("dp", None),
        P(),
        P(),
        P(None, "dp", "tensor"),
        P("tensor", "dp"),
        P(),
        P("dp", "tensor"),
        P(),
        P("tensor", "dp"),
        P(),
        P(),
        P(),
    )
    out_specs = (
        P(("dp", "tensor"), None),
        P(("dp", "tensor"), None),
        P(),
        P(),
        P(None, "dp", "tensor"),
        P("tensor", "dp"),
        P(),
        P("dp", "tensor"),
        P(),
        P("tensor", "dp"),
        P(),
        P(),
        P(),
    )

    return jax.shard_map(shards, mesh=mesh, in_specs=in_specs, out_specs=out_specs, check_vma=False)
```

```python
import functools
import math

import jax
import jax.numpy as jnp
from jax import lax
from jax.experimental import pallas as pl
from jax.experimental.pallas import tpu as pltpu
from jax.sharding import PartitionSpec as P


HDIM = 64
HALF = HDIM // 2
BQ = 512
BK = 512
ROWS = 128
STRIP = 256
NEG = -1000000000.0
MESH = pl.DeviceIdType.MESH
BF = jnp.bfloat16
F32 = jnp.float32
VMEM_LIMIT = 60 * 1024 * 1024


highest = lax.Precision.HIGHEST


def dot(a, b, ca, cb, out=F32):
    return lax.dot_general(a, b, (((ca,), (cb,)), ((), ())), preferred_element_type=out)


def normalize(values):
    center = values - jnp.mean(values, axis=-1, keepdims=True)
    inverse = lax.rsqrt(jnp.mean(center * center, axis=-1, keepdims=True) + 1e-05)
    return (center * inverse, inverse)


def norm_back(grad_in, normed, inverse):
    return inverse * (
        grad_in
        - jnp.mean(grad_in, axis=-1, keepdims=True)
        - normed * jnp.mean(grad_in * normed, axis=-1, keepdims=True)
    )


def pack_info(lengths, row_total):
    row_index = jnp.arange(row_total, dtype=jnp.int32)
    seq_ends = jnp.cumsum(lengths)
    passed = row_index[:, None] >= seq_ends[None, :]
    segment = jnp.sum(passed.astype(jnp.int32), axis=1)
    starts = jnp.sum(jnp.where(passed, lengths[None, :], 0), axis=1)
    return (segment, row_index - starts)


def key_ranges(lengths, row_total):
    seq_ends = jnp.cumsum(lengths)
    first = jnp.arange(row_total // BQ, dtype=jnp.int32) * BQ
    last = first + (BQ - 1)
    start = jnp.sum(jnp.where(first[:, None] >= seq_ends[None, :], lengths[None, :], 0), axis=1)
    end = jnp.min(jnp.where(seq_ends[None, :] > last[:, None], seq_ends[None, :], row_total), axis=1)
    return (start // BK).astype(jnp.int32), ((end + BK - 1) // BK).astype(jnp.int32)


def time_embed(time_index, embed_width):
    half_width = embed_width // 2
    freqs = jnp.exp(-math.log(10000.0) * jnp.arange(half_width, dtype=jnp.float32) / half_width)
    angles = time_index.astype(jnp.float32)[:, None] * freqs[None, :]
    return jnp.concatenate([jnp.cos(angles), jnp.sin(angles)], axis=1)


def rope_tables(positions):
    inverse = jnp.exp(-math.log(10000.0) * jnp.arange(HALF, dtype=jnp.float32) * (2.0 / HDIM))
    angles = inverse[:, None] * positions.astype(jnp.float32)[None, :]
    return (jnp.cos(angles), jnp.sin(angles))


def project_kernel(heads, n_ref, w_ref, cos_ref, sin_ref, q_ref, k_ref, v_ref, wt_ref):
    width = heads * HDIM

    @pl.when(pl.program_id(0) == 0)
    def _():
        wt_ref[...] = w_ref[...].T

    raw = dot(wt_ref[...], n_ref[...], 1, 1)
    cos = cos_ref[...]
    sin = sin_ref[...]
    for part, out_ref, factor in ((0, q_ref, 1.0 / math.sqrt(HDIM)), (1, k_ref, 1.0)):
        for h in range(heads):
            base = part * width + h * HDIM
            a = raw[base : base + HALF]
            b = raw[base + HALF : base + HDIM]
            out_ref[h * HDIM : h * HDIM + HALF] = ((a * cos - b * sin) * factor).astype(BF)
            out_ref[h * HDIM + HALF : (h + 1) * HDIM] = ((b * cos + a * sin) * factor).astype(BF)
    v_ref[...] = raw[2 * width :].astype(BF)


def project(normed, weight, cos, sin, heads):
    rows, width_model = normed.shape
    width = heads * HDIM
    tile = 512
    out = jax.ShapeDtypeStruct((width, rows), BF)
    spec = pl.BlockSpec((width, tile), lambda i: (0, i))
    return pl.pallas_call(
        functools.partial(project_kernel, heads),
        name="project_qkv",
        grid=(rows // tile,),
        in_specs=[
            pl.BlockSpec((tile, width_model), lambda i: (i, 0)),
            pl.BlockSpec((width_model, 3 * width), lambda i: (0, 0)),
            pl.BlockSpec((HALF, tile), lambda i: (0, i)),
            pl.BlockSpec((HALF, tile), lambda i: (0, i)),
        ],
        out_specs=[spec, spec, spec],
        out_shape=[out, out, out],
        scratch_shapes=[pltpu.VMEM((3 * width, width_model), BF)],
        cost_estimate=pl.CostEstimate(
            flops=2 * rows * width_model * 3 * width, bytes_accessed=8 << 20, transcendentals=0
        ),
    )(normed, weight, cos, sin)


def wide(column, lanes):
    return jnp.concatenate([column] * (lanes // 128), axis=1)


def attend_kernel(
    heads, lo_ref, hi_ref, q_ref, k_ref, v_ref, srow_ref, scol_ref, o_ref, lse_ref, kt_ref, sc_ref
):
    i = pl.program_id(0)

    @pl.when(i == 0)
    def _():
        for h in range(heads):
            kt_ref[h] = k_ref[h * HDIM : (h + 1) * HDIM, :].T
        sc_ref[...] = jnp.broadcast_to(scol_ref[...], sc_ref.shape)

    srow = srow_ref[...]

    def step(j, carry):
        base = pl.multiple_of(j * BK, BK)
        allowed = wide(sc_ref[pl.ds(base, BK), :], BQ) == srow
        out = []
        for h in range(heads):
            m, l, acc = carry[h]
            s = dot(kt_ref[h, pl.ds(base, BK), :], q_ref[h * HDIM : (h + 1) * HDIM, :], 1, 0)
            s = jnp.where(allowed, s, NEG)
            m_new = jnp.maximum(m, jnp.max(s, axis=0, keepdims=True))
            fade = jnp.exp(m - m_new)
            p = jnp.exp(s - m_new)
            l = fade * l + jnp.sum(p, axis=0, keepdims=True)
            acc = fade * acc + dot(
                v_ref[h * HDIM : (h + 1) * HDIM, pl.ds(base, BK)], p.astype(BF), 1, 0
            )
            out.append((m_new, l, acc))
        return tuple(out)

    empty = (
        jnp.full((1, BQ), -3.0e38, F32),
        jnp.zeros((1, BQ), F32),
        jnp.zeros((HDIM, BQ), F32),
    )
    done = lax.fori_loop(lo_ref[i], hi_ref[i], step, (empty,) * heads)
    for h in range(heads):
        m, l, acc = done[h]
        o_ref[h * HDIM : (h + 1) * HDIM, :] = (acc / l).astype(BF)
        lse_ref[h : h + 1, :] = m + jnp.log(l)


def attend(q, k, v, seg_row, seg_col, lo, hi):
    width, rows = q.shape
    heads = width // HDIM
    whole = lambda i, *_: (0, 0)
    block = lambda i, *_: (0, i)
    return pl.pallas_call(
        functools.partial(attend_kernel, heads),
        name="attend",
        grid_spec=pltpu.PrefetchScalarGridSpec(
            num_scalar_prefetch=2,
            grid=(rows // BQ,),
            in_specs=[
                pl.BlockSpec((width, BQ), block),
                pl.BlockSpec((width, rows), whole),
                pl.BlockSpec((width, rows), whole),
                pl.BlockSpec((1, BQ), block),
                pl.BlockSpec((rows, 1), whole),
            ],
            out_specs=[
                pl.BlockSpec((width, BQ), block),
                pl.BlockSpec((heads, BQ), block),
            ],
            scratch_shapes=[
                pltpu.VMEM((heads, rows, HDIM), BF),
                pltpu.VMEM((rows, 128), jnp.int32),
            ],
        ),
        out_shape=[
            jax.ShapeDtypeStruct((width, rows), BF),
            jax.ShapeDtypeStruct((heads, rows), F32),
        ],
        compiler_params=pltpu.CompilerParams(vmem_limit_bytes=VMEM_LIMIT),
        cost_estimate=pl.CostEstimate(
            flops=rows * rows * heads * HDIM * 8, bytes_accessed=8 << 20, transcendentals=rows * rows
        ),
    )(lo, hi, q, k, v, seg_row, seg_col)


def attend_back_kernel(
    heads,
    lo_ref,
    hi_ref,
    q_ref,
    k_ref,
    v_ref,
    do_ref,
    o_ref,
    lse_ref,
    srow_ref,
    scol_ref,
    cos_ref,
    sin_ref,
    g_ref,
    kt_ref,
    vt_ref,
    sc_ref,
    dk_ref,
    dv_ref,
):
    i = pl.program_id(0)
    width = heads * HDIM

    @pl.when(i == 0)
    def _():
        for h in range(heads):
            kt_ref[h] = k_ref[h * HDIM : (h + 1) * HDIM, :].T
            vt_ref[h] = v_ref[h * HDIM : (h + 1) * HDIM, :].T
        sc_ref[...] = jnp.broadcast_to(scol_ref[...], sc_ref.shape)
        dk_ref[...] = jnp.zeros_like(dk_ref)
        dv_ref[...] = jnp.zeros_like(dv_ref)

    srow = srow_ref[...]
    inner = []
    for h in range(heads):
        part = slice(h * HDIM, (h + 1) * HDIM)
        inner.append(
            jnp.sum(do_ref[part, :].astype(F32) * o_ref[part, :].astype(F32), axis=0, keepdims=True)
        )

    def step(j, carry):
        base = pl.multiple_of(j * BK, BK)
        keys = pl.ds(base, BK)
        allowed = wide(sc_ref[keys, :], BQ) == srow
        out = []
        for h in range(heads):
            part = slice(h * HDIM, (h + 1) * HDIM)
            q = q_ref[part, :]
            grad = do_ref[part, :]
            s = dot(kt_ref[h, keys, :], q, 1, 0)
            s = jnp.where(allowed, s, NEG)
            p = jnp.exp(s - lse_ref[h : h + 1, :])
            dp = dot(vt_ref[h, keys, :], grad, 1, 0)
            ds = (p * (dp - inner[h])).astype(BF)
            out.append(carry[h] + dot(k_ref[part, keys], ds, 1, 0))
            dk_ref[part, keys] += dot(q, ds, 1, 1)
            dv_ref[part, keys] += dot(grad, p.astype(BF), 1, 1)
        return tuple(out)

    done = lax.fori_loop(
        lo_ref[i], hi_ref[i], step, (jnp.zeros((HDIM, BQ), F32),) * heads
    )
    here = pl.ds(pl.multiple_of(i * BQ, BQ), BQ)
    cos = cos_ref[:, here]
    sin = sin_ref[:, here]
    factor = 1.0 / math.sqrt(HDIM)
    for h in range(heads):
        a = done[h][:HALF] * factor
        b = done[h][HALF:] * factor
        g_ref[h * HDIM : h * HDIM + HALF, here] = (a * cos + b * sin).astype(BF)
        g_ref[h * HDIM + HALF : (h + 1) * HDIM, here] = (b * cos - a * sin).astype(BF)

    @pl.when(i == pl.num_programs(0) - 1)
    def _():
        cos_all = cos_ref[...]
        sin_all = sin_ref[...]
        for h in range(heads):
            a = dk_ref[h * HDIM : h * HDIM + HALF, :]
            b = dk_ref[h * HDIM + HALF : (h + 1) * HDIM, :]
            base = width + h * HDIM
            g_ref[base : base + HALF, :] = (a * cos_all + b * sin_all).astype(BF)
            g_ref[base + HALF : base + HDIM, :] = (b * cos_all - a * sin_all).astype(BF)
        g_ref[2 * width :, :] = dv_ref[...].astype(BF)


def attend_back(q, k, v, do, o, lse, seg_row, seg_col, cos, sin, lo, hi):
    width, rows = q.shape
    heads = width // HDIM
    whole = lambda i, *_: (0, 0)
    block = lambda i, *_: (0, i)
    return pl.pallas_call(
        functools.partial(attend_back_kernel, heads),
        name="attend_back",
        grid_spec=pltpu.PrefetchScalarGridSpec(
            num_scalar_prefetch=2,
            grid=(rows // BQ,),
            in_specs=[
                pl.BlockSpec((width, BQ), block),
                pl.BlockSpec((width, rows), whole),
                pl.BlockSpec((width, rows), whole),
                pl.BlockSpec((width, BQ), block),
                pl.BlockSpec((width, BQ), block),
                pl.BlockSpec((heads, BQ), block),
                pl.BlockSpec((1, BQ), block),
                pl.BlockSpec((rows, 1), whole),
                pl.BlockSpec((HALF, rows), whole),
                pl.BlockSpec((HALF, rows), whole),
            ],
            out_specs=pl.BlockSpec((3 * width, rows), whole),
            scratch_shapes=[
                pltpu.VMEM((heads, rows, HDIM), BF),
                pltpu.VMEM((heads, rows, HDIM), BF),
                pltpu.VMEM((rows, 128), jnp.int32),
                pltpu.VMEM((width, rows), F32),
                pltpu.VMEM((width, rows), F32),
            ],
        ),
        out_shape=jax.ShapeDtypeStruct((3 * width, rows), BF),
        compiler_params=pltpu.CompilerParams(vmem_limit_bytes=VMEM_LIMIT),
        cost_estimate=pl.CostEstimate(
            flops=rows * rows * heads * HDIM * 20, bytes_accessed=8 << 20, transcendentals=rows * rows
        ),
    )(lo, hi, q, k, v, do, o, lse, seg_row, seg_col, cos, sin)


class Links:
    def __init__(self, send_sem, recv_sem, n_z):
        dp = lax.axis_index("dp")
        t = lax.axis_index("tensor")
        self.n_z, self.dp, self.t = n_z, dp, t
        self.z, self.x = dp // 2, dp % 2
        self.y, self.c = t // 2, t % 2
        self.core_rank = 2 * self.y + (1 - self.c)
        self.y_rank = 2 * (1 - self.y) + self.c
        self.core = {"tensor": self.core_rank}
        self.across = {"tensor": self.y_rank}
        self.beside = {"dp": 2 * self.z + (1 - self.x)}
        self.send_sem, self.recv_sem = send_sem, recv_sem
        self.slot = 0

    def along(self, step):
        return {"dp": 2 * ((self.z + step) % self.n_z) + self.x}

    def slots(self, count):
        first = self.slot
        self.slot += count
        return first

    def copy(self, src, dst, peer, slot):
        return pltpu.make_async_remote_copy(
            src_ref=src,
            dst_ref=dst,
            send_sem=self.send_sem.at[slot],
            recv_sem=self.recv_sem.at[slot],
            device_id=peer,
            device_id_type=MESH,
        )

    def send(self, src, dst, peer):
        copy = self.copy(src, dst, peer, self.slots(1))
        copy.start()
        return copy


def greet(peers):
    barrier = pltpu.get_barrier_semaphore()
    for peer in peers:
        pl.semaphore_signal(barrier, inc=1, device_id=peer, device_id_type=MESH)
    pl.semaphore_wait(barrier, len(peers))


def opening_kernel(n_z, count, *refs):
    x_ref, gain_ref, bias_ref, sel_ref, embed_ref, time_ref, time_bias_ref = refs[:7]
    qkv_ref, proj_ref, up_ref, down_ref = refs[7:11]
    n_out, mod_out, w_outs = refs[11], refs[12], refs[13 : 13 + count]
    w_refs = refs[13 + count : 13 + 2 * count]
    n_ref, mod_s, table_ref, local_sem, send_sem, recv_sem = refs[13 + 2 * count :]
    links = Links(send_sem, recv_sem, n_z)
    head_width = qkv_ref.shape[2]
    for part in range(3):
        w_refs[0][:, part * head_width : (part + 1) * head_width] = qkv_ref[part].astype(BF)
    w_refs[1][...] = proj_ref[...].T.astype(BF)
    half = w_refs[2].shape[1]
    w_refs[2][...] = up_ref[:, :half].astype(BF)
    w_refs[3][...] = down_ref[...].astype(BF)
    w_refs[4][...] = up_ref[:, half:].astype(BF)
    greet([links.core, links.across, links.beside] + [links.along(k) for k in range(1, n_z)])
    rows = x_ref.shape[0]

    def n_at(rank):
        return n_out.at[pl.ds(pl.multiple_of(rank * rows, rows), rows)]

    z, x = links.z, links.x
    right = {"dp": 2 * ((z + 1) % n_z) + x}
    left = {"dp": 2 * ((z + n_z - 1) % n_z) + x}
    right_slots = [links.slots(n_z) for _ in range(count)]
    left_slots = [links.slots(n_z) for _ in range(count)]
    side_slots = [links.slots(n_z) for _ in range(count)]
    cross_slots = links.slots(2 * n_z)

    def w_at(n, rank):
        return w_outs[n].at[0, rank] if n in (1, 2) else w_outs[n].at[rank]

    def own_or(n, j, src):
        return w_at(n, 2 * j + x) if src is None else src

    def right_copy(n, j, src=None):
        here = w_at(n, 2 * j + x)
        return links.copy(own_or(n, j, src), here, right, right_slots[n] + j)

    def left_copy(n, j, src=None):
        here = w_at(n, 2 * j + x)
        return links.copy(own_or(n, j, src), here, left, left_slots[n] + j)

    def side_copy(n, j, src=None):
        here = w_at(n, 2 * j + x)
        return links.copy(own_or(n, j, src), here, links.beside, side_slots[n] + j)

    def cross_copy(rank):
        return links.copy(
            w_outs[2].at[0, rank], w_outs[2].at[1, rank], links.across, cross_slots + rank
        )

    def arrived(n, j):
        side_copy(n, j).start()
        if n == 2:
            cross_copy(2 * j + x).start()

    def travel(n):
        def step(d, carry):
            @pl.when(z - d >= 0)
            def _():
                right_copy(n, z - d).wait_recv()

                @pl.when(z < n_z - 1)
                def _():
                    right_copy(n, z - d).start()

                arrived(n, z - d)

            @pl.when(z + d <= n_z - 1)
            def _():
                left_copy(n, z + d).wait_recv()

                @pl.when(z > 0)
                def _():
                    left_copy(n, z + d).start()

                arrived(n, z + d)

            return carry

        lax.fori_loop(1, n_z, step, 0)

    def each(body):
        def step(j, carry):
            body(j)
            return carry

        lax.fori_loop(0, n_z, step, 0)

    def norm_step(i, carry):
        here = pl.ds(pl.multiple_of(i * ROWS, ROWS), ROWS)
        normed, _ = normalize(x_ref[here, :])
        n_ref[here, :] = (normed * gain_ref[...][None, :] + bias_ref[...][None, :]).astype(BF)
        return carry

    def mod_step(i):
        here = pl.ds(i * ROWS, ROWS)
        mod_s[here, :] = lax.dot_general(
            sel_ref[here, :],
            table_ref[...],
            (((1,), (0,)), ((), ())),
            precision=highest,
            preferred_element_type=F32,
        )
        copy = pltpu.make_async_copy(mod_s.at[here], mod_out.at[here], local_sem.at[1 + count + i])
        copy.start()
        return copy

    for n in range(count):

        @pl.when(z < n_z - 1)
        def _():
            right_copy(n, z, w_refs[n]).start()

        @pl.when(z > 0)
        def _():
            left_copy(n, z, w_refs[n]).start()

        side_copy(n, z, w_refs[n]).start()
    lax.fori_loop(0, rows // ROWS, norm_step, 0)
    tiles = rows // ROWS
    mod_copies = []
    local = [pltpu.make_async_copy(n_ref, n_at(links.t), local_sem.at[0])]
    for n in range(count):
        local.append(pltpu.make_async_copy(w_refs[n], w_at(n, links.dp), local_sem.at[1 + n]))
    for copy in local:
        copy.start()
    n_y = links.send(n_ref, n_at(links.t), links.across)
    n_core = links.send(n_ref, n_at(links.t), links.core)
    table_ref[...] = (
        lax.dot_general(
            embed_ref[...],
            time_ref[...],
            (((1,), (0,)), ((), ())),
            precision=highest,
            preferred_element_type=F32,
        )
        + time_bias_ref[...][None, :]
    )
    others = []
    for n in range(count):
        travel(n)
        if n < 2:
            for i in range(n * tiles // 2, (n + 1) * tiles // 2):
                mod_copies.append(mod_step(i))
        if n == 2:
            local[1 + n].wait()
            cross_copy(links.dp).start()
        if n == 1:
            n_y.wait_recv()
            n_relay = links.send(n_at(links.y_rank), n_at(links.y_rank), links.core)
            each(lambda j: side_copy(1, j).wait_recv())
            local[1 + n].wait()
            others.append(links.send(w_outs[n].at[0], w_outs[n].at[2], links.across))
            others.append(links.send(w_outs[n].at[0], w_outs[n].at[1], links.core))

    def late_cross(j):
        side_copy(2, j).wait_recv()
        cross_copy(2 * j + 1 - x).start()

    each(late_cross)
    others[0].wait_recv()
    others.append(links.send(w_outs[1].at[2], w_outs[1].at[3], links.core))
    n_core.wait_recv()
    n_relay.wait_recv()
    others[1].wait_recv()
    others[2].wait_recv()
    for n in range(count):
        if n not in (1, 2):
            each(lambda j: side_copy(n, j).wait_recv())
            local[1 + n].wait()

        def drain(j):
            side_copy(n, j).wait_send()

            @pl.when((j <= z) & (z < n_z - 1))
            def _():
                right_copy(n, j).wait_send()

            @pl.when((j >= z) & (z > 0))
            def _():
                left_copy(n, j).wait_send()

        each(drain)

    def crossed(j):
        for rank in (2 * j, 2 * j + 1):
            cross_copy(rank).wait_recv()
            cross_copy(rank).wait_send()

    each(crossed)
    for copy in [n_y, n_core, n_relay] + others:
        copy.wait_send()
    for copy in local[:1] + mod_copies:
        copy.wait()


def opening(x, gain, bias, sel, embed, time_weight, time_bias, weights, n_dp, n_tensor):
    rows, width = x.shape
    n_z = n_dp // 2
    qkv, proj, up, down = weights
    depth = up.shape[0]
    early = up.shape[1] * 2 // 3 // 128 * 128
    columns = (3 * qkv.shape[2], proj.shape[0], early, down.shape[1], up.shape[1] - early)
    count = len(columns)
    slots = 3 * count * n_z + 6 + n_dp
    shapes = [(n_dp, depth, c) for c in columns]
    shapes[1] = (n_tensor,) + shapes[1]
    shapes[2] = (2,) + shapes[2]
    return pl.pallas_call(
        functools.partial(opening_kernel, n_z, count),
        name="opening",
        in_specs=[pl.BlockSpec(memory_space=pltpu.VMEM)] * 11,
        out_specs=[pl.BlockSpec(memory_space=pl.ANY)] * (2 + count),
        out_shape=[
            jax.ShapeDtypeStruct((n_tensor * rows, width), BF),
            jax.ShapeDtypeStruct((rows, time_weight.shape[1]), F32),
        ]
        + [jax.ShapeDtypeStruct(shape, BF) for shape in shapes],
        scratch_shapes=[pltpu.VMEM((depth, c), BF) for c in columns]
        + [
            pltpu.VMEM((rows, width), BF),
            pltpu.VMEM((rows, time_weight.shape[1]), F32),
            pltpu.VMEM((embed.shape[0], time_weight.shape[1]), F32),
            pltpu.SemaphoreType.DMA((1 + count + rows // ROWS,)),
            pltpu.SemaphoreType.DMA((slots,)),
            pltpu.SemaphoreType.DMA((slots,)),
        ],
        compiler_params=pltpu.CompilerParams(
            collective_id=0, has_side_effects=True, vmem_limit_bytes=VMEM_LIMIT
        ),
        cost_estimate=pl.CostEstimate(flops=0, bytes_accessed=64 << 20, transcendentals=0),
    )(x, gain, bias, sel, embed, time_weight, time_bias, *weights)


def closing_kernel(n_z, slot_count, embed_width, *refs):
    g_ref, n_ref, w_ref, up_keep, up_got, down_near, down_far, proj_near, proj_far = refs[:9]
    x_ref, h_ref, gain_ref, sums_ref = refs[9:13]
    in_grad_ref, tail_ref, time_ref, time_bias_ref, biases_ref = refs[13:18]
    up_out, down_out, proj_out, qkv_out = refs[18:22]
    all_ref, part_send, core_buf, y_send, y_recv, vec, all_vec, qkv_flat, qkv_ref = refs[22:31]
    up_y_send, up_y_recv = refs[31:33]
    x_send, x_recv = refs[33], refs[34:37]
    proj_y_send, proj_y_recv = refs[37:39]
    z_send, z_recv = refs[39:43], refs[43:47]
    send_sem, recv_sem = refs[47:]
    links = Links(send_sem, recv_sem, n_z)
    z, x = links.z, links.x
    n_dp = 2 * n_z
    rows, width = x_ref.shape
    outs = (up_out, down_out, proj_out, qkv_out)
    dp_peers = [{"dp": (links.dp + k) % n_dp} for k in range(1, n_dp)]
    diagonal = {"tensor": 3 - links.t}
    ranks = [links.t, links.core_rank, links.y_rank, 3 - links.t]
    greet([links.core, links.across, diagonal] + dp_peers)

    quarter = sums_ref.shape[2]

    def lanes(rank):
        return pl.ds(pl.multiple_of(rank * quarter, 128), quarter)

    own_lanes = lanes(links.t)
    all_ref[:, :, own_lanes] = sums_ref[...]
    up_slots = links.slots(n_z)
    x_slots = [None] + [links.slots(n_z) for _ in range(3)]
    proj_slots = links.slots(2 * n_z)
    z_slots = [links.slots(n_z) for _ in range(4)]
    order = list(range(1, n_z)) + [0]

    def at(s):
        return (z + s) % n_z

    def up_copy(s):
        return links.copy(up_y_send.at[s], up_y_recv.at[s], links.across, up_slots + s)

    def x_copy(n, s):
        src = qkv_ref.at[at(s), 1 - x] if n == 3 else x_send.at[s]
        return links.copy(src, x_recv[n - 1].at[s], links.beside, x_slots[n] + s)

    def z_copy(n, s):
        peer = {"dp": 2 * at(s) + x}
        return links.copy(z_send[n].at[s], z_recv[n].at[s], peer, z_slots[n] + s)

    def proj_copy(e, s):
        src = (proj_near, proj_far)[e].at[at(s), 1 - x]
        slot = (x_slots[2], proj_slots)[e] + s
        return links.copy(src, x_recv[1].at[e, s], links.beside, slot)

    def proj_y_copy(s):
        slot = proj_slots + n_z + s
        return links.copy(proj_y_send.at[s], proj_y_recv.at[s], links.across, slot)

    def both(s, side):
        return down_near[at(s), side].astype(F32) + down_far[at(s), side].astype(F32)

    def x_start(n):
        for s in order:
            if n == 2:
                proj_copy(1, s).start()
                proj_copy(0, s).start()
                continue
            if n == 1:
                x_send[s] = both(s, 1 - x).astype(BF)
            x_copy(n, s).start()

    def proj_cross():
        for s in order:
            proj_copy(1, s).wait_recv()
            own = proj_far[at(s), x].astype(F32) + x_recv[1][1, s].astype(F32)
            proj_y_send[s] = own.astype(BF)
            proj_y_copy(s).start()

    def value(n, s):
        if n == 0:
            up_copy(s).wait_recv()
            own = up_keep[0, at(s)].astype(F32) + up_got[0, at(s)].astype(F32)
            return own + up_y_recv[s].astype(F32)
        if n == 2:
            proj_copy(0, s).wait_recv()
            proj_y_copy(s).wait_recv()
            own = proj_near[at(s), x].astype(F32) + x_recv[1][0, s].astype(F32)
            return own + proj_y_recv[s].astype(F32)
        x_copy(n, s).wait_recv()
        own = qkv_ref[at(s), x].astype(F32) if n == 3 else both(s, x)
        return own + x_recv[n - 1][s].astype(F32)

    def z_start(n):
        for s in range(1, n_z):
            z_send[n][s] = value(n, s).astype(BF)
            z_copy(n, s).start()
        outs[n][...] = value(n, 0)

    def finish(n):
        for s in range(1, n_z):
            z_copy(n, s).wait_recv()
            outs[n][...] += z_recv[n][s].astype(F32)

    def part(d):
        here = pl.ds(pl.multiple_of(ranks[d] * rows, rows), rows)
        return dot(g_ref[:, here].T, w_ref[...], 1, 1)

    x_start(1)
    for s in order:
        up_y_send[s] = (up_keep[1, at(s)].astype(F32) + up_got[1, at(s)].astype(F32)).astype(BF)
        up_copy(s).start()
    x_start(2)
    part_send[0] = part(3).astype(BF)
    c3 = links.send(part_send.at[0], core_buf.at[0], links.core)
    far = part(2)
    c3.wait_recv()
    y_send[...] = (far + core_buf[0].astype(F32)).astype(BF)
    part_send[1] = part(1).astype(BF)
    y_copy = links.send(y_send, y_recv, links.across)
    strip = 256

    def qkv_step(j, carry):
        here = pl.ds(pl.multiple_of(j * strip, strip), strip)
        qkv_flat[here, :] = dot(g_ref[...], n_ref[:, here], 1, 0).T.astype(BF)
        return carry

    c1 = links.send(part_send.at[1], core_buf.at[1], links.core)
    z_start(1)
    lax.fori_loop(0, width // strip, qkv_step, 0)
    depth = qkv_ref.shape[2]
    for r in range(n_dp):
        qkv_ref[r // 2, r % 2] = qkv_flat[r * depth : (r + 1) * depth, :]
    x_start(3)
    proj_cross()
    z_start(0)
    z_start(2)
    near = part(0)
    c1.wait_recv()
    near = near + core_buf[1].astype(F32)
    z_start(3)
    y_copy.wait_recv()
    grad = near + y_recv[...].astype(F32)
    normed, inverse = normalize(x_ref[...])
    own_vec = jnp.concatenate(
        [jnp.sum(grad * normed, axis=0, keepdims=True), jnp.sum(grad, axis=0, keepdims=True)], axis=1
    )
    vec[links.t] = own_vec
    in_grad_ref[...] = h_ref[...] + norm_back(grad * gain_ref[...][None, :], normed, inverse)
    tensor_sends = [
        links.send(vec.at[links.t], vec.at[links.t], peer)
        for peer in (links.core, links.across, diagonal)
    ]
    here = all_ref.at[:, :, own_lanes]
    there = all_ref.at[:, :, lanes(links.y_rank)]
    sums_last = [
        links.send(sums_ref, here, links.across),
        links.send(sums_ref, here, links.core),
    ]
    finish(1)
    for copy in tensor_sends:
        copy.wait_recv()
    all_vec[links.dp] = vec[0] + vec[1] + vec[2] + vec[3]
    finish(0)
    dp_sends = [links.send(all_vec.at[links.dp], all_vec.at[links.dp], peer) for peer in dp_peers]
    sums_last[0].wait_recv()
    sums_last.append(links.send(there, there, links.core))
    finish(2)
    finish(3)
    sums_last[1].wait_recv()
    sums_last[2].wait_recv()
    mod_width = 3 * width
    mods = jnp.concatenate([all_ref[r, :slot_count, :mod_width] for r in range(n_dp)], axis=0)
    embeds = jnp.concatenate(
        [all_ref[r, :slot_count, mod_width : mod_width + embed_width] for r in range(n_dp)], axis=0
    )
    time_ref[...] = lax.dot_general(
        embeds, mods, (((0,), (0,)), ((), ())), precision=highest, preferred_element_type=F32
    )
    time_bias_ref[...] = jnp.sum(mods, axis=0, keepdims=True)
    biases = all_ref[0, slot_count:, : 2 * width]
    for r in range(1, n_dp):
        biases = biases + all_ref[r, slot_count:, : 2 * width]
    biases_ref[...] = biases
    for copy in dp_sends:
        copy.wait_recv()
    total = all_vec[0]
    for r in range(1, n_dp):
        total = total + all_vec[r]
    tail_ref[...] = total
    for copy in [c1, c3, y_copy] + dp_sends + sums_last + tensor_sends:
        copy.wait_send()
    for s in range(n_z):
        up_copy(s).wait_send()
        proj_copy(0, s).wait_send()
        proj_copy(1, s).wait_send()
        proj_y_copy(s).wait_send()
        for n in range(4):
            if n in (1, 3):
                x_copy(n, s).wait_send()
            if s > 0:
                z_copy(n, s).wait_send()


def closing(
    qkv_grad, normed, weight, up, down, proj, residual_in, hidden_grad, gain, sums, n_dp, slot_count, embed_width
):
    rows, width = residual_in.shape
    head_width = weight.shape[1]
    n_z = n_dp // 2
    depth = width // n_dp

    def blocks(pair):
        return [w.reshape(n_z, 2, depth, w.shape[-1]) for w in pair]

    columns = [up[0].shape[-1], down[0].shape[-1], proj[0].shape[-1], head_width]
    shards = [(depth, c) for c in columns]
    stacks = [(n_z,) + shard for shard in shards]
    slots = 10 * n_z + 2 + 1 + 3 + 3 + (n_dp - 1)
    vmem = pl.BlockSpec(memory_space=pltpu.VMEM)
    out = pl.pallas_call(
        functools.partial(closing_kernel, n_z, slot_count, embed_width),
        name="closing",
        in_specs=[vmem] * 13,
        out_specs=[vmem] * 9,
        out_shape=[
            jax.ShapeDtypeStruct((rows, width), F32),
            jax.ShapeDtypeStruct((1, 2 * width), F32),
            jax.ShapeDtypeStruct((embed_width, 3 * width), F32),
            jax.ShapeDtypeStruct((1, 3 * width), F32),
            jax.ShapeDtypeStruct((sums.shape[1] - slot_count, 2 * width), F32),
        ]
        + [jax.ShapeDtypeStruct(shape, F32) for shape in shards],
        scratch_shapes=[
            pltpu.VMEM(sums.shape[:2] + (4 * sums.shape[2],), F32),
            pltpu.VMEM((2, rows, width), BF),
            pltpu.VMEM((2, rows, width), BF),
            pltpu.VMEM((rows, width), BF),
            pltpu.VMEM((rows, width), BF),
            pltpu.VMEM((4, 1, 2 * width), F32),
            pltpu.VMEM((n_dp, 1, 2 * width), F32),
            pltpu.VMEM((width, head_width), BF),
            pltpu.VMEM((n_z, 2) + shards[3], BF),
            pltpu.VMEM(stacks[0], BF),
            pltpu.VMEM(stacks[0], BF),
        ]
        + [pltpu.VMEM(shape, BF) for shape in (stacks[1], stacks[1], (2,) + stacks[2], stacks[3])]
        + [pltpu.VMEM(shape, BF) for shape in (stacks[2], stacks[2])]
        + [pltpu.VMEM(shape, BF) for _ in range(2) for shape in stacks]
        + [pltpu.SemaphoreType.DMA((slots,)), pltpu.SemaphoreType.DMA((slots,))],
        compiler_params=pltpu.CompilerParams(
            collective_id=1, has_side_effects=True, vmem_limit_bytes=VMEM_LIMIT
        ),
        cost_estimate=pl.CostEstimate(flops=0, bytes_accessed=64 << 20, transcendentals=0),
    )(
        qkv_grad,
        normed,
        weight,
        *up,
        *blocks(down),
        *blocks(proj),
        residual_in,
        hidden_grad,
        gain,
        sums,
    )
    return out[0], out[1], out[2:5], out[5:]


def middle_kernel(n_z, *refs):
    (
        mixed_ref,
        proj_ref,
        up_hbm,
        up_late_hbm,
        up_late_far_hbm,
        down_hbm,
        down_far_hbm,
        x_ref,
        grad_ref,
        mod_ref,
        sel_ref,
        embed_ref,
        proj_bias_ref,
        up_bias_ref,
        down_bias_ref,
    ) = refs[:15]
    out_ref, h_grad_ref, mixed_grad_ref, packs_ref, down_near, proj_near, down_far, proj_far = refs[15:23]
    up_keep, up_away = refs[23:25]
    (
        mix_buf,
        mix_t,
        up_buf,
        down_buf,
        hid_s,
        m_s,
        flip_s,
        dz_s,
        dz_t,
        act_s,
        du_s,
        z_acc,
        m_acc,
        up_send,
        down_send,
        up_recv,
        down_recv,
        low_s,
        back_s,
        proj_send,
        proj_recv,
        sums_ref,
        sums_buf,
        early_s,
        local_sem,
        send_sem,
        recv_sem,
    ) = refs[25:]
    links = Links(send_sem, recv_sem, n_z)
    depth = up_keep.shape[2]
    rows, width = x_ref.shape
    peers = [None, links.core, links.across, {"tensor": 3 - links.t}]
    ranks = [links.t, links.core_rank, links.y_rank, 3 - links.t]
    n_dp = 2 * n_z
    dp_peers = [{"dp": (links.dp + k) % n_dp} for k in range(1, n_dp)]
    greet(peers[1:] + dp_peers)
    quarter = sums_ref.shape[1] // 4

    def lanes(rank):
        return pl.ds(pl.multiple_of(rank * rows, rows), rows)

    mix_copies = [
        links.send(mixed_ref.at[:, lanes(ranks[d])], mix_buf.at[d], peers[d]) for d in (3, 2, 1)
    ]
    half = up_hbm.shape[2]

    def pieces(shift):
        return [
            (up_hbm.at[0], up_buf.at[shift, :, :half]),
            (up_late_hbm, up_buf.at[shift, :, half:]),
            (down_hbm, down_buf.at[shift]),
            (up_hbm.at[1], up_buf.at[2 + shift, :, :half]),
            (up_late_far_hbm, up_buf.at[2 + shift, :, half:]),
            (down_far_hbm, down_buf.at[2 + shift]),
        ]

    w_copies = [links.send(src, dst, links.core) for src, dst in pieces(1)]
    local = [
        pltpu.make_async_copy(src, dst, local_sem.at[i]) for i, (src, dst) in enumerate(pieces(0))
    ]
    for copy in local:
        copy.start()

    def tiles(body, carry=0):
        return lax.fori_loop(0, rows // ROWS, body, carry)

    def tile(i):
        return pl.ds(pl.multiple_of(i * ROWS, ROWS), ROWS)

    def gate_step(i, total):
        here = tile(i)
        dz = grad_ref[here, :] * mod_ref[here, 2 * width :]
        dz_s[here, :] = dz.astype(BF)
        return total + jnp.sum(dz, axis=0, keepdims=True)

    down_bias_sum = tiles(gate_step, jnp.zeros((1, width), F32))
    dz_t[...] = dz_s[...].T
    sums_ref[...] = jnp.zeros_like(sums_ref)
    for e, copy in ((0, local[2]), (1, local[5])):
        copy.wait()

        def early_step(i, carry):
            here = pl.ds(pl.multiple_of(i * STRIP, STRIP), STRIP)
            early_s[e, here, :] = dot(dz_s[here, :], down_buf[2 * e], 1, 0)
            return carry

        lax.fori_loop(0, rows // STRIP, early_step, 0)
    mix_t[0] = mixed_ref[:, lanes(links.t)].T
    for d, copy in zip((3, 2, 1), mix_copies):
        copy.wait_recv()
        mix_t[d] = mix_buf[d].T

    def hidden_step(i, carry):
        here = tile(i)
        hidden = x_ref[here, :] + proj_bias_ref[...][None, :]
        for d in range(4):
            hidden = hidden + dot(mix_t[d, here, :], proj_ref[d], 1, 1)
        hid_s[here, :] = hidden
        normed, _ = normalize(hidden)
        scale = mod_ref[here, :width]
        shift = mod_ref[here, width : 2 * width]
        m_s[here, :] = (normed * (1.0 + scale) + shift).astype(BF)
        return carry

    tiles(hidden_step)
    flip_s[...] = m_s[...].T
    z_acc[...] = jnp.zeros_like(z_acc)
    m_acc[...] = jnp.zeros_like(m_acc)
    root = math.sqrt(2.0 / math.pi)

    def feed(d, early=None):
        up = up_buf.at[d]
        down = down_buf.at[d]

        def step(i, total):
            here = pl.ds(pl.multiple_of(i * STRIP, STRIP), STRIP)
            u = dot(m_s[here, :], up[...], 1, 0) + up_bias_ref[d]
            square = u * u
            bend = jnp.tanh(root * u * (1.0 + 0.044715 * square))
            half = 0.5 * (1.0 + bend)
            act = (u * half).astype(BF)
            act_s[here, :] = act
            slope = half + 0.5 * u * (1.0 - bend * bend) * (root * (1.0 + 3.0 * 0.044715 * square))
            act_grad = dot(dz_s[here, :], down[...], 1, 0) if early is None else early[here, :]
            du = act_grad * slope
            low = du.astype(BF)
            du_s[here, :] = low
            z_acc[here, :] += dot(act, down[...], 1, 1)
            m_acc[here, :] += dot(low, up[...], 1, 1)
            return total + jnp.sum(low.astype(F32), axis=0, keepdims=True)

        total = lax.fori_loop(0, rows // STRIP, step, jnp.zeros((1, width), F32))
        y, c = (d // 2), (d % 2)
        rank = 2 * (y + links.y - 2 * y * links.y) + (c + links.c - 2 * c * links.c)
        sums_ref[pl.ds(17 + rank, 1), :width] = total

    def grads(store):
        def step(j, carry):
            here = pl.ds(pl.multiple_of(j * STRIP, STRIP), STRIP)
            store(here, dot(flip_s[here, :], du_s[...], 1, 0), dot(dz_t[here, :], act_s[...], 1, 0))
            return carry

        lax.fori_loop(0, width // STRIP, step, 0)

    for copy in w_copies:
        copy.wait_recv()

    def outward(e, carry):
        feed(2 * e + 1)

        def store(here, up_part, down_part):
            up_send[e, here, :] = up_part.astype(BF)
            down_send[e, here, :] = down_part.astype(BF)

        grads(store)
        return carry

    lax.fori_loop(0, 2, outward, 0)
    first = links.slots(2)
    second = links.slots(2)

    def up_copy(e):
        return links.copy(up_send.at[e], up_recv.at[e], links.core, first + e)

    def down_copy(e):
        return links.copy(down_send.at[e], down_recv.at[e], links.core, second + e)

    for e in range(2):
        up_copy(e).start()
        down_copy(e).start()
    for i in (0, 1, 3, 4):
        local[i].wait()

    for e, down_sum in ((1, down_far), (0, down_near)):
        feed(2 * e, early_s.at[e])
        up_copy(e).wait_recv()
        down_copy(e).wait_recv()

        def store(here, up_part, down_part):
            up_send[e, here, :] = (up_part + up_recv[e, here, :].astype(F32)).astype(BF)
            down_sum[here, :] = (down_part + down_recv[e, here, :].astype(F32)).astype(BF)

        up_copy(e).wait_send()
        grads(store)
        for r in range(2 * n_z):
            block = up_send[e, r * depth : (r + 1) * depth, :]

            @pl.when(links.x == r % 2)
            def _():
                up_keep[e, r // 2] = block

            @pl.when(links.x != r % 2)
            def _():
                up_away[e, r // 2] = block

    def back_step(i, total):
        here = tile(i)
        hidden = hid_s[here, :]
        normed, inverse = normalize(hidden)
        scale = mod_ref[here, :width]
        gate = mod_ref[here, 2 * width :]
        grad = grad_ref[here, :]
        branch = z_acc[here, :] + down_bias_ref[...][None, :]
        shift_grad = m_acc[here, :]
        out_ref[here, :] = hidden + gate * branch
        h_grad = grad + norm_back(shift_grad * (1.0 + scale), normed, inverse)
        h_grad_ref[here, :] = h_grad
        low_s[here, :] = h_grad.astype(BF)
        sel = sel_ref[:, here]
        for part, value in ((0, shift_grad * normed), (1, shift_grad), (2, grad * branch)):
            sums_ref[:, part * width : (part + 1) * width] += lax.dot_general(
                sel, value, (((1,), (0,)), ((), ())), precision=highest, preferred_element_type=F32
            )
        return total + jnp.sum(h_grad, axis=0, keepdims=True)

    proj_bias_sum = tiles(back_step, jnp.zeros((1, width), F32))
    sums_ref[16:17, :width] = proj_bias_sum
    sums_ref[16:17, width : 2 * width] = down_bias_sum
    embed_at = 3 * width
    sums_ref[: embed_ref.shape[0], embed_at : embed_at + embed_ref.shape[1]] = embed_ref[...]

    def columns(rank):
        return pl.ds(pl.multiple_of(rank * quarter, 128), quarter)

    back_copies = []
    sums_copies = []
    for d in (3, 2, 1, 0):
        part = dot(low_s[...], proj_ref[d], 1, 0).astype(BF).T
        if d == 0:
            mixed_grad_ref[:, lanes(links.t)] = part
        else:
            back_s[d] = part
            sums_copies.append(
                links.send(sums_ref.at[:, columns(ranks[d])], sums_buf.at[links.t], peers[d])
            )
        if d < 3:
            back_copies.append(
                links.send(back_s.at[d + 1], mixed_grad_ref.at[:, lanes(links.t)], peers[d + 1])
            )
    sums_buf[links.t] = sums_ref[:, columns(links.t)]
    flip_s[...] = low_s[...].T
    for d in (1, 3):
        proj_send[d // 2] = dot(flip_s[...], mix_t[d], 1, 0).astype(BF)
    for copy in sums_copies:
        copy.wait_recv()
    packs_ref[links.dp] = sums_buf[0] + sums_buf[1] + sums_buf[2] + sums_buf[3]
    own_part = dot(flip_s[...], mix_t[0], 1, 0)
    here = packs_ref.at[links.dp]
    sums_dp = [links.send(here, here, peer) for peer in dp_peers]
    proj_copies = [links.send(proj_send.at[e], proj_recv.at[e], links.core) for e in range(2)]
    far_part = dot(flip_s[...], mix_t[2], 1, 0)
    for e, part, out in ((0, own_part, proj_near), (1, far_part, proj_far)):
        proj_copies[e].wait_recv()
        out[...] = (part + proj_recv[e].astype(F32)).astype(BF)
    for copy in back_copies + sums_dp:
        copy.wait_recv()
    for copy in mix_copies + w_copies + back_copies + proj_copies + sums_copies + sums_dp:
        copy.wait_send()
    for e in range(2):
        down_copy(e).wait_send()


def middle(
    mixed, proj, weights, x, grad, mod, sel, embed, proj_bias, up_bias, down_bias, n_dp
):
    rows, width = x.shape
    head_width, total_rows = mixed.shape
    units = weights[3].shape[1]
    vmem = pl.BlockSpec(memory_space=pltpu.VMEM)
    hbm = pl.BlockSpec(memory_space=pl.ANY)
    sums = (sel.shape[0], -(-(3 * width + embed.shape[1]) // 512) * 512)
    slots = 3 + 6 + 4 + 3 + 2 + 3 + (n_dp - 1)
    square = (2, width, units)
    halves = (2, n_dp // 2, width // n_dp, units)
    return pl.pallas_call(
        functools.partial(middle_kernel, n_dp // 2),
        name="middle",
        in_specs=[vmem, vmem] + [hbm] * 5 + [vmem] * 8,
        out_specs=[vmem] * 10,
        out_shape=[
            jax.ShapeDtypeStruct((rows, width), F32),
            jax.ShapeDtypeStruct((rows, width), F32),
            jax.ShapeDtypeStruct((head_width, total_rows), BF),
            jax.ShapeDtypeStruct((n_dp, sums[0], sums[1] // 4), F32),
            jax.ShapeDtypeStruct(square[1:], BF),
            jax.ShapeDtypeStruct((width, head_width), BF),
            jax.ShapeDtypeStruct(square[1:], BF),
            jax.ShapeDtypeStruct((width, head_width), BF),
            jax.ShapeDtypeStruct(halves, BF),
            jax.ShapeDtypeStruct(halves, BF),
        ],
        scratch_shapes=[
            pltpu.VMEM((4, head_width, rows), BF),
            pltpu.VMEM((4, rows, head_width), BF),
            pltpu.VMEM((4, width, units), BF),
            pltpu.VMEM((4, width, units), BF),
            pltpu.VMEM((rows, width), F32),
            pltpu.VMEM((rows, width), BF),
            pltpu.VMEM((width, rows), BF),
            pltpu.VMEM((rows, width), BF),
            pltpu.VMEM((width, rows), BF),
            pltpu.VMEM((rows, units), BF),
            pltpu.VMEM((rows, units), BF),
            pltpu.VMEM((rows, width), F32),
            pltpu.VMEM((rows, width), F32),
            pltpu.VMEM(square, BF),
            pltpu.VMEM(square, BF),
            pltpu.VMEM(square, BF),
            pltpu.VMEM(square, BF),
            pltpu.VMEM((rows, width), BF),
            pltpu.VMEM((4, head_width, rows), BF),
            pltpu.VMEM((2, width, head_width), BF),
            pltpu.VMEM((2, width, head_width), BF),
            pltpu.VMEM(sums, F32),
            pltpu.VMEM((4, sums[0], sums[1] // 4), F32),
            pltpu.VMEM((2, rows, units), F32),
            pltpu.SemaphoreType.DMA((6,)),
            pltpu.SemaphoreType.DMA((slots,)),
            pltpu.SemaphoreType.DMA((slots,)),
        ],
        compiler_params=pltpu.CompilerParams(
            collective_id=2, has_side_effects=True, vmem_limit_bytes=63 * 1024 * 1024
        ),
        cost_estimate=pl.CostEstimate(
            flops=12 * rows * width * units * 4, bytes_accessed=64 << 20, transcendentals=0
        ),
    )(mixed, proj, *weights, x, grad, mod, sel, embed, proj_bias, up_bias, down_bias)


def results_kernel(*refs):
    out_ref, in_grad_ref, tail_ref, time_ref, time_bias_ref, biases_ref = refs[:6]
    up_ref, down_ref, proj_ref, qkv_ref = refs[6:10]
    (
        out,
        in_grad,
        gain,
        bias,
        qkv,
        proj,
        proj_bias,
        up,
        up_bias,
        down,
        down_bias,
        time,
        time_bias,
    ) = refs[10:]
    width = out.shape[1]
    out[...] = out_ref[...]
    in_grad[...] = in_grad_ref[...]
    gain[...] = tail_ref[0, :width]
    bias[...] = tail_ref[0, width:]
    columns = qkv.shape[2]
    for part in range(3):
        qkv[part] = qkv_ref[:, part * columns : (part + 1) * columns]
    proj[...] = proj_ref[...].T
    down[...] = down_ref[...]
    up[...] = up_ref[...]
    proj_bias[...] = biases_ref[0, :width]
    down_bias[...] = biases_ref[0, width:]
    units = up.shape[1]
    for r in range(up_bias.shape[0] // units):
        up_bias[r * units : (r + 1) * units] = biases_ref[1 + r, :units]
    time[...] = time_ref[...]
    time_bias[...] = time_bias_ref[0, :]


def results(residual_out, in_grad, tail, times, grads, tensor_units):
    rows, width = in_grad.shape
    depth, units = grads[0].shape
    columns = grads[2].shape[1]
    shapes = [
        (rows, width),
        (rows, width),
        (width,),
        (width,),
        (3, depth, columns),
        (columns, depth),
        (width,),
        (depth, units),
        (tensor_units,),
        (depth, units),
        (width,),
        times[0].shape,
        (times[0].shape[1],),
    ]
    vmem = pl.BlockSpec(memory_space=pltpu.VMEM)
    return pl.pallas_call(
        results_kernel,
        name="results",
        in_specs=[vmem] * 10,
        out_specs=[vmem] * len(shapes),
        out_shape=[jax.ShapeDtypeStruct(shape, F32) for shape in shapes],
        compiler_params=pltpu.CompilerParams(vmem_limit_bytes=VMEM_LIMIT),
    )(residual_out, in_grad, tail, *times, *grads)


def to_tensor_peer(value, distance):
    size = lax.axis_size("tensor")
    return lax.ppermute(value, "tensor", [(r, r ^ distance) for r in range(size)])


def shards(
    residual_in,
    out_grad,
    seq_lengths,
    timesteps,
    norm_gain,
    norm_bias,
    qkv_weight,
    proj_weight,
    proj_bias,
    up_weight,
    up_bias,
    down_weight,
    down_bias,
    time_weight,
    time_bias,
):
    row_count, width_model = residual_in.shape
    n_dp = lax.axis_size("dp")
    n_tensor = lax.axis_size("tensor")
    tensor_rank = lax.axis_index("tensor")
    total_rows = row_count * n_tensor
    slot_count = seq_lengths.shape[1]
    head_width = qkv_weight.shape[2]
    heads = head_width // HDIM
    units = up_weight.shape[1]
    ranks = [tensor_rank ^ d for d in range(n_tensor)]

    segment, positions = pack_info(seq_lengths[0], total_rows)
    lo, hi = key_ranges(seq_lengths[0], total_rows)
    own_segment = lax.dynamic_slice_in_dim(segment, tensor_rank * row_count, row_count)
    slots = jnp.arange(slot_count, dtype=jnp.int32)
    onehot = (own_segment[:, None] == slots[None, :]).astype(F32)
    embedded = time_embed(timesteps[0], time_weight.shape[0])
    sums_rows = -(-(slot_count + 1 + n_tensor) // 8) * 8
    chosen = (own_segment[None, :] == jnp.arange(sums_rows, dtype=jnp.int32)[:, None]) & (
        own_segment[None, :] < slot_count
    )
    own_embed = jnp.where(tensor_rank == 0, embedded, 0.0)
    up_bias_rel = jnp.stack(
        [lax.dynamic_slice_in_dim(up_bias, ranks[d] * units, units)[None] for d in range(n_tensor)]
    )
    normed_full, modulation, qkv_full, proj_all, up_both, down_own, up_late = opening(
        residual_in,
        norm_gain,
        norm_bias,
        onehot,
        embedded,
        time_weight,
        time_bias,
        (qkv_weight, proj_weight, up_weight, down_weight.T),
        n_dp,
        n_tensor,
    )
    qkv_full = qkv_full.reshape(width_model, -1)
    proj_all = proj_all.reshape(n_tensor, width_model, -1)
    up_both = up_both.reshape(2, width_model, -1)
    down_own = down_own.reshape(width_model, -1)
    up_late = up_late.reshape(width_model, -1)
    up_late_far = to_tensor_peer(up_late, 2)
    down_far = to_tensor_peer(down_own, 2)

    cos, sin = rope_tables(positions)
    seg_row = segment[None, :]
    seg_col = segment[:, None]

    queries, keys, values = project(normed_full, qkv_full, cos, sin, heads)
    mixed, log_totals = attend(queries, keys, values, seg_row, seg_col, lo, hi)

    outs = middle(
        mixed,
        proj_all,
        (up_both, up_late, up_late_far, down_own, down_far),
        residual_in,
        out_grad,
        modulation,
        chosen.astype(F32),
        own_embed,
        proj_bias,
        up_bias_rel,
        down_bias,
        n_dp,
    )
    residual_out, hidden_grad, mixed_grad, sums, down_near, proj_near, down_other, proj_other = outs[:8]
    up_keep, up_away = outs[8:]

    qkv_grad = attend_back(
        queries, keys, values, mixed_grad, mixed, log_totals, seg_row, seg_col, cos, sin, lo, hi
    )

    down_far = to_tensor_peer(down_other, 2)
    up_got = lax.ppermute(up_away, "dp", [(r, r ^ 1) for r in range(n_dp)])

    input_grad, tail, times, grads = closing(
        qkv_grad,
        normed_full,
        qkv_full,
        (up_keep, up_got),
        (down_near, down_far),
        (proj_near, proj_other),
        residual_in,
        hidden_grad,
        norm_gain,
        sums,
        n_dp,
        slot_count,
        time_weight.shape[0],
    )
    done = list(results(residual_out, input_grad, tail, times, grads, up_bias.shape[0]))
    done[9] = done[9].T
    return tuple(done)


def solution(mesh):
    in_specs = (
        P(("dp", "tensor"), None),
        P(("dp", "tensor"), None),
        P("dp", None),
        P("dp", None),
        P(),
        P(),
        P(None, "dp", "tensor"),
        P("tensor", "dp"),
        P(),
        P("dp", "tensor"),
        P(),
        P("tensor", "dp"),
        P(),
        P(),
        P(),
    )
    out_specs = (
        P(("dp", "tensor"), None),
        P(("dp", "tensor"), None),
        P(),
        P(),
        P(None, "dp", "tensor"),
        P("tensor", "dp"),
        P(),
        P("dp", "tensor"),
        P(),
        P("tensor", "dp"),
        P(),
        P(),
        P(),
    )

    return jax.shard_map(shards, mesh=mesh, in_specs=in_specs, out_specs=out_specs, check_vma=False)
```
